32 devices in a mesh: fsdp: 32 (over z, y, x, core).
Axes of the slice: x: 2, y: 2, z: 4, core: 2. Of those that a mesh axis runs over, the one named last changes fastest.
Arguments:
- tokens: bfloat16 [32768, 768], P('fsdp'), may hold values from -6 to 6
- cotangent: bfloat16 [32768, 128], P('fsdp'), may hold values from -6 to 6
- slot_row: int32 [32768], P('fsdp'), may hold values from 0 to 32767, as said below
- lengths: int32 [64], P('fsdp'), may hold values from 256 to 512, as said below
- w_qkv: bfloat16 [768, 2304], P('fsdp'), may hold values from -0.21875 to 0.21875
- b_qv: bfloat16 [1536], P('fsdp'), may hold values from -0.29882812 to 0.29882812
- w_out: bfloat16 [768, 768], P('fsdp'), may hold values from -4 to 4
- b_out: bfloat16 [768], P('fsdp'), may hold values from -1.796875 to 1.796875
- ln1_gain: bfloat16 [768], P('fsdp'), may hold values from 0.099609375 to 1.8984375
- ln1_bias: bfloat16 [768], P('fsdp'), may hold values from -1.796875 to 1.796875
- w_up: bfloat16 [768, 3072], P('fsdp'), may hold values from -0.21875 to 0.21875
- b_up: bfloat16 [3072], P('fsdp'), may hold values from -1.796875 to 1.796875
- w_down: bfloat16 [3072, 768], P('fsdp'), may hold values from -0.109375 to 0.109375
- b_down: bfloat16 [768], P('fsdp'), may hold values from -1.796875 to 1.796875
- ln2_gain: bfloat16 [768], P('fsdp'), may hold values from 0.099609375 to 1.8984375
- ln2_bias: bfloat16 [768], P('fsdp'), may hold values from -1.796875 to 1.796875
- w_proj: bfloat16 [768, 128], P('fsdp'), may hold values from -0.21875 to 0.21875
Outputs:
- embeddings: bfloat16 [32768, 128], P('fsdp')
- input_grad: bfloat16 [32768, 768], P('fsdp')
- grad_w_qkv: float32 [768, 2304], P('fsdp')
- grad_b_qv: float32 [1536], P('fsdp')
- grad_w_out: float32 [768, 768], P('fsdp')
- grad_b_out: float32 [768], P('fsdp')
- grad_ln1_gain: float32 [768], P('fsdp')
- grad_ln1_bias: float32 [768], P('fsdp')
- grad_w_up: float32 [768, 3072], P('fsdp')
- grad_b_up: float32 [3072], P('fsdp')
- grad_w_down: float32 [3072, 768], P('fsdp')
- grad_b_down: float32 [768], P('fsdp')
- grad_ln2_gain: float32 [768], P('fsdp')
- grad_ln2_bias: float32 [768], P('fsdp')
- grad_w_proj: float32 [768, 128], P('fsdp')
The draws below stay inside these ranges and needn't reach their ends.
Inputs may be any that keep to these rules, and one draw needn't show every extreme that they name: slot_row is a permutation of the 32768 input rows. The 1024 slots of device k take exactly 32 rows from each device's shard of tokens, namely those whose position in that shard lies from k * 32 to (k + 1) * 32 - 1. Entries b * 2 to (b + 1) * 2 - 1 are the lengths of the passages laid one after another from the first slot of device b; the slots after them are padding. Some passage has exactly 512 tokens.
All inputs are finite; a program needn't handle non-finite values.
Results may differ from the reference program's by a relative error of at most 0.018.
Values may be sent and summed in bfloat16 or wider, within the bound.
A program may use at most 256 MiB of HBM per device.

```python
from functools import partial
import jax
import jax.numpy as jnp
from jax import lax

D = 768
HEADS = 12
HEAD_DIM = 64
FF = 3072
EMB = 128
TOK_DEV = 1024
PASS_DEV = 2
TOKENS = 32768
PASSAGES = 64
N_FSDP = 32


def draw_slot_row(key, part):
    per_peer = TOK_DEV // N_FSDP

    def one_device(device_index):
        ordering = jax.random.permutation(jax.random.fold_in(key, device_index), TOK_DEV).astype(jnp.int32)
        source = ordering // per_peer
        within = ordering % per_peer
        return source * TOK_DEV + device_index * per_peer + within
    return jax.vmap(one_device)(jnp.arange(N_FSDP, dtype=jnp.int32)).reshape(TOKENS).astype(jnp.int32)


def draw_lengths(key, part):
    least_len = TOK_DEV // 4
    most_len = TOK_DEV // 2
    values = jax.random.randint(jax.random.fold_in(key, 11), (PASSAGES,), least_len, most_len + 1)
    chosen = jax.random.randint(jax.random.fold_in(key, 12), (), 0, PASSAGES)
    return jnp.where(jnp.arange(PASSAGES) == chosen, most_len, values).astype(jnp.int32)


def strengthened(values, stream_key, source, target, blocks, factor):
    owner, partner = [(jnp.arange(values.shape[dim]) // (values.shape[dim] // blocks)).reshape([-1 if axis == dim else 1 for axis in range(values.ndim)]) for dim in (source, target)]
    chosen = jax.random.permutation(stream_key, blocks)[partner]
    strong = (owner == chosen) | (owner == (partner + blocks // 2) % blocks)
    return jnp.where(strong, factor * values, values)


def level_of(own_key, extent, split, least, top_value):
    level = 1.0
    for dim, blocks in split:
        heights = jax.random.uniform(jax.random.fold_in(jax.random.fold_in(own_key, 6), dim), (blocks,), jnp.float32, least / len(split), top_value / len(split))
        level = level * jnp.repeat(jnp.exp(heights), extent[dim] // blocks).reshape((-1,) + (1,) * (len(extent) - 1 - dim))
    return level


def gaussian(rng, shape, width, most, split=(), kind=jnp.bfloat16):
    loudness = level_of(rng, shape, split, -0.22, 0.18) if split else 1.0
    result = jax.random.normal(rng, shape, jnp.float32) * width * loudness
    return jnp.minimum(jnp.maximum(result, -most), most).astype(kind)


def noise_with(own_key, extent, width, limit, split, heavy, held_as=jnp.bfloat16):
    entries = width * jax.random.normal(own_key, extent, jnp.float32)
    if split:
        entries = entries * level_of(own_key, extent, split, -0.22, 0.18)
    return jnp.clip(strengthened(entries, jax.random.fold_in(own_key, 3), *heavy), -limit, limit).astype(held_as)


def setup_inputs(seed: int = 0) -> dict:
    keys = jax.random.split(jax.random.key(seed), 18)
    tokens = gaussian(keys[0], (TOKENS, D), 1.0, 6.0, ((0, 32),))
    cotangent = noise_with(keys[1], (TOKENS, EMB), 1.0, 6.0, ((0, 32),), (0, 1, 32, 2.75))
    slot_row = draw_slot_row(jax.random.fold_in(keys[17], 71), 0)
    lengths = draw_lengths(jax.random.fold_in(keys[17], 71), 0)
    w_qkv = gaussian(keys[4], (D, 3 * D), D ** -0.5, 0.21875, ((0, 32),))
    b_qv = gaussian(keys[5], (2 * D,), 0.05, 0.29882812, ((0, 32),))
    w_out = gaussian(keys[6], (D, D), (max(1, 8 * D // (3 * TOK_DEV))) ** -0.5, 4.0, ((0, 32),))
    b_out = gaussian(keys[7], (D,), 0.3, 1.796875, ((0, 32),))
    ln1_gain = jnp.clip(1.0 + 0.18 * jax.random.normal(keys[8], (D,), jnp.float32), 0.099609375, 1.8984375).astype(jnp.bfloat16)
    ln1_bias = gaussian(keys[9], (D,), 0.3, 1.796875, ((0, 32),))
    w_up = gaussian(keys[10], (D, FF), D ** -0.5, 0.21875, ((0, 32),))
    b_up = gaussian(keys[11], (FF,), 0.3, 1.796875, ((0, 32),))
    w_down = gaussian(keys[12], (FF, D), FF ** -0.5, 0.109375, ((0, 32),))
    b_down = gaussian(keys[13], (D,), 0.3, 1.796875, ((0, 32),))
    ln2_gain = jnp.clip(1.0 + 0.18 * jax.random.normal(keys[14], (D,), jnp.float32), 0.099609375, 1.8984375).astype(jnp.bfloat16)
    ln2_bias = gaussian(keys[15], (D,), 0.3, 1.796875, ((0, 32),))
    w_proj = gaussian(keys[16], (D, EMB), D ** -0.5, 0.21875, ((0, 32),))
    return dict(tokens=tokens, cotangent=cotangent, slot_row=slot_row, lengths=lengths, w_qkv=w_qkv, b_qv=b_qv, w_out=w_out, b_out=b_out, ln1_gain=ln1_gain, ln1_bias=ln1_bias, w_up=w_up, b_up=b_up, w_down=w_down, b_down=b_down, ln2_gain=ln2_gain, ln2_bias=ln2_bias, w_proj=w_proj)


highest = lax.Precision.HIGHEST

@jax.custom_vjp
def low(v):
    return lax.optimization_barrier(v.astype(jnp.bfloat16)).astype(jnp.float32)

@jax.custom_vjp
def low_back(v):
    return v

def low_keep(v):
    return (low(v), None)

def low_pass(kept, grad):
    return (grad,)

def back_keep(v):
    return (v, None)

def back_low(kept, grad):
    return (low(grad),)
low.defvjp(low_keep, low_pass)
low_back.defvjp(back_keep, back_low)

def product(left, right):
    return jnp.dot(left, right, precision=highest, preferred_element_type=jnp.float32)

def passage_ids(length_block, row_count):
    position = jnp.arange(row_count, dtype=jnp.int32)
    bounds = jnp.cumsum(length_block).astype(jnp.int32)
    passage = lax.optimization_barrier(jnp.sum((position[:, None] >= bounds[None, :]).astype(jnp.int32), axis=1)).astype(jnp.int32)
    inside = passage < length_block.shape[0]
    passage = jnp.where(inside, passage, length_block.shape[0] + position)
    return (passage, inside)

def layer_norm(hidden, gain, shift):
    center = hidden - lax.optimization_barrier(jnp.mean(hidden, axis=-1, keepdims=True))
    variance = lax.optimization_barrier(jnp.mean(center * center, axis=-1, keepdims=True))
    return center * lax.rsqrt(variance + 1e-12) * gain + shift

def block_forward(weights, tokens_block, length_block):
    w_qkv, b_qv, w_out, b_out, gain_one, bias_one, w_up, b_up, w_down, b_down, gain_two, bias_two, w_proj = weights
    row_count = tokens_block.shape[0]
    passage, inside = passage_ids(length_block, row_count)
    allowed = passage[:, None] == passage[None, :]
    key_zeros = jnp.zeros((D,), jnp.float32)
    bias_all = jnp.concatenate([b_qv[:D], key_zeros, b_qv[D:]])
    qkv = low(low_back(product(tokens_block, w_qkv)) + bias_all)
    heads_all = qkv.reshape(row_count, 3, HEADS, HEAD_DIM)
    scores = low_back(jnp.einsum('qhd,khd->hqk', heads_all[:, 0], heads_all[:, 1], precision=highest) * 0.125)
    scores = jnp.where(allowed[None], scores, -1e+30)
    attn_probs = jax.nn.softmax(scores, axis=-1)
    context = jnp.einsum('hqk,khd->qhd', low(attn_probs), heads_all[:, 2], precision=highest)
    context = low(low_back(context.reshape(row_count, D)))
    hidden_one = tokens_block + low_back(product(context, w_out)) + b_out
    first = low(layer_norm(hidden_one, gain_one, bias_one))
    up_input = low_back(product(first, w_up)) + b_up
    active = low(jax.nn.gelu(up_input, approximate=False))
    hidden_two = first + low_back(product(active, w_down)) + b_down
    second = low(layer_norm(hidden_two, gain_two, bias_two))
    project = low_back(product(second, w_proj))
    inv_norm = lax.rsqrt(lax.optimization_barrier(jnp.sum(project * project, axis=-1, keepdims=True)) + 1e-06)
    return project * inv_norm * inside[:, None].astype(jnp.float32)

def reference(tokens, cotangent, slot_row, lengths, w_qkv, b_qv, w_out, b_out, ln1_gain, ln1_bias, w_up, b_up, w_down, b_down, ln2_gain, ln2_bias, w_proj):
    weights = tuple((weight_arg.astype(jnp.float32) for weight_arg in (w_qkv, b_qv, w_out, b_out, ln1_gain, ln1_bias, w_up, b_up, w_down, b_down, ln2_gain, ln2_bias, w_proj)))

    def forward(weight_set, inputs):
        dealt = inputs[slot_row].reshape(N_FSDP, TOK_DEV, D)
        length_rows = lengths.reshape(N_FSDP, PASS_DEV)
        block_step = jax.checkpoint(partial(block_forward, weight_set))

        def group_step(group_args):
            return block_step(group_args[0], group_args[1])
        embedded = lax.map(group_step, (dealt, length_rows))
        return jnp.zeros((TOKENS, EMB), jnp.float32).at[slot_row].set(embedded.reshape(TOKENS, EMB))
    embedded, pullback = jax.vjp(forward, weights, tokens.astype(jnp.float32))
    grad_weights, grad_tokens = pullback(cotangent.astype(jnp.float32))
    return (embedded.astype(jnp.bfloat16), grad_tokens.astype(jnp.bfloat16), grad_weights[0], grad_weights[1], grad_weights[2], grad_weights[3], grad_weights[4], grad_weights[5], grad_weights[6], grad_weights[7], grad_weights[8], grad_weights[9], grad_weights[10], grad_weights[11], grad_weights[12])
```

```python
from functools import partial

import jax
import jax.numpy as jnp
from jax import lax
from jax.experimental import pallas as pl
from jax.experimental.pallas import tpu as pltpu
from jax.sharding import PartitionSpec as P

HEADS = 12
HEAD_DIM = 64
AXIS = "fsdp"
MESH_ID = pl.DeviceIdType.MESH
VMEM_SPEC = pl.BlockSpec(memory_space=pltpu.VMEM)
ANY_SPEC = pl.BlockSpec(memory_space=pl.ANY)
VMEM_LIMIT = 60 * 1024 * 1024


def chain_edges(node, ring, lean_up):
    up_count = ring // 2 if lean_up else (ring - 1) // 2
    edges = []
    here = node
    for _ in range(up_count):
        there = ((here[0] + 1) % ring,) + here[1:]
        edges.append((here, there, "up"))
        here = there
    here = node
    for _ in range(ring - 1 - up_count):
        there = ((here[0] - 1) % ring,) + here[1:]
        edges.append((here, there, "down"))
        here = there
    return edges


def plane_edges(node, x_first):
    z = node[0]
    own, by_x, by_y, both = (z, 0, 0, 0), (z, 0, 1, 0), (z, 1, 0, 0), (z, 1, 1, 0)
    edges = [(own, by_x, "x"), (own, by_y, "y")]
    edges.append((by_x, both, "y") if x_first else (by_y, both, "x"))
    return edges


def make_tree(ring, ring_first, flip):
    root = (0, 0, 0, 0)
    edges = []
    if ring_first:
        edges += chain_edges(root, ring, flip)
        nodes = [root] + [edge[1] for edge in edges]
        for place, node in enumerate(nodes):
            edges += plane_edges(node, (place % 2 == 0) != flip)
    else:
        edges += plane_edges(root, flip)
        nodes = [root] + [edge[1] for edge in edges]
        for place, node in enumerate(nodes):
            edges += chain_edges(node, ring, (place % 2 == 0) != flip)
    nodes = [root] + [edge[1] for edge in edges]
    edges += [(node, node[:3] + (1,), "core") for node in nodes]
    depth = {root: 0}
    for parent, child, _ in edges:
        depth[child] = depth[parent] + 1
    order = sorted(range(len(edges)), key=lambda index: depth[edges[index][1]])
    return [edges[index] + (depth[edges[index][1]],) for index in order]


class Place:
    def __init__(self, ring):
        me = lax.axis_index(AXIS)
        self.ring = ring
        self.me = me
        self.core = lax.rem(me, 2)
        self.x = lax.rem(me // 2, 2)
        self.y = lax.rem(me // 4, 2)
        self.z = me // 8

    @staticmethod
    def flip(value, amount):
        return 1 - value if amount else value

    def chip_of(self, offset):
        z = lax.rem(self.z + (self.ring - offset[0]) % self.ring, self.ring)
        return (z * 2 + self.flip(self.y, offset[1])) * 2 + self.flip(self.x, offset[2])

    def unit_of(self, offset):
        return self.chip_of(offset) * 2 + self.flip(self.core, offset[3])

    def neighbour(self, way, back=False):
        step = {"up": (1, 0, 0, 0), "down": (-1, 0, 0, 0), "x": (0, 0, 1, 0)}
        step.update({"y": (0, 1, 0, 0), "core": (0, 0, 0, 1)})
        offset = step[way]
        dz = offset[0] if back else -offset[0]
        return self.unit_of((dz % self.ring,) + offset[1:])


def enter(place):
    barrier = pltpu.get_barrier_semaphore()
    for way in ("up", "down", "x", "y", "core"):
        pl.semaphore_signal(
            barrier, inc=1, device_id=(place.neighbour(way),), device_id_type=MESH_ID
        )
    pl.semaphore_wait(barrier, 5)


def gather_kernel(ring, plan, *refs):
    arrays = len(plan["shapes"])
    shards, outs = refs[:arrays], refs[arrays : 2 * arrays]
    recv_sem, send_sem, local_sem = refs[2 * arrays :]
    place = Place(ring)
    parts = plan["parts"]

    def window(ref, part):
        _, first, count, _ = parts[part]
        return ref if count is None else ref.at[pl.ds(first, count)]

    def copy(part, index):
        array, _, _, tree = parts[part]
        parent, _, way, _ = tree[index]
        unit = place.unit_of(parent)
        source = shards[array] if parent == (0, 0, 0, 0) else outs[array].at[unit]
        return pltpu.make_async_remote_copy(
            src_ref=window(source, part),
            dst_ref=window(outs[array].at[unit], part),
            send_sem=send_sem.at[part],
            recv_sem=recv_sem.at[part, index],
            device_id=(place.neighbour(way),),
            device_id_type=MESH_ID,
        )

    def arrived(part, index):
        array, _, _, tree = parts[part]
        _, child, way, _ = tree[index]
        landed = window(outs[array].at[place.unit_of(child)], part)
        pltpu.make_async_remote_copy(
            src_ref=landed,
            dst_ref=landed,
            send_sem=send_sem.at[part],
            recv_sem=recv_sem.at[part, index],
            device_id=(place.neighbour(way),),
            device_id_type=MESH_ID,
        ).wait_recv()

    def send_from(part, node):
        for index, edge in enumerate(parts[part][3]):
            if edge[0] == node:
                copy(part, index).start()

    own_copies = [
        pltpu.make_async_copy(shards[array], outs[array].at[place.me], local_sem.at[array])
        for array in range(arrays)
    ]
    for own_copy in own_copies:
        own_copy.start()
    enter(place)
    for part in range(len(parts)):
        send_from(part, (0, 0, 0, 0))
    deepest = max(edge[3] for part in parts for edge in part[3])
    for depth in range(1, deepest + 1):
        for part in range(len(parts)):
            for index, edge in enumerate(parts[part][3]):
                if edge[3] == depth and edge[2] != "core":
                    arrived(part, index)
                    send_from(part, edge[1])
    for part in range(len(parts)):
        for index, edge in enumerate(parts[part][3]):
            if edge[2] == "core":
                arrived(part, index)
    for own_copy in own_copies:
        own_copy.wait()
    for part, (array, first, count, tree) in enumerate(parts):
        whole = outs[array].at[pl.ds(0, len(tree))]
        if count is not None:
            whole = whole.at[:, pl.ds(first, count)]
        pltpu.make_async_copy(whole, whole, send_sem.at[part]).wait()


def gather_units(shards, plan, ring):
    devices = ring * 8
    edges = devices - 1
    return pl.pallas_call(
        partial(gather_kernel, ring, plan),
        out_shape=[
            jax.ShapeDtypeStruct((devices,) + shard.shape, shard.dtype) for shard in shards
        ],
        in_specs=[VMEM_SPEC] * len(shards),
        out_specs=[ANY_SPEC] * len(shards),
        scratch_shapes=[
            pltpu.SemaphoreType.DMA((len(plan["parts"]), edges)),
            pltpu.SemaphoreType.DMA((len(plan["parts"]),)),
            pltpu.SemaphoreType.DMA((len(shards),)),
        ],
        compiler_params=pltpu.CompilerParams(collective_id=0, has_side_effects=True),
        name="gather_units",
    )(*shards)


def scatter_kernel(ring, plan, *refs):
    shapes = plan["shapes"]
    arrays = len(shapes)
    parts = plan["parts"]
    grads, outs = refs[:arrays], refs[arrays : 2 * arrays]
    owns = refs[2 * arrays : 3 * arrays]
    lands = refs[3 * arrays : 3 * arrays + len(parts)]
    recv_sem, send_sem, local_sem = refs[3 * arrays + len(parts) :]
    place = Place(ring)

    def window(ref, part):
        _, first, count, _ = parts[part]
        return ref if count is None else ref.at[pl.ds(first, count)]

    def copy(part, index, source):
        way = parts[part][3][index][2]
        return pltpu.make_async_remote_copy(
            src_ref=source,
            dst_ref=lands[part].at[index],
            send_sem=send_sem.at[part],
            recv_sem=recv_sem.at[part, index],
            device_id=(place.neighbour(way, back=True),),
            device_id_type=MESH_ID,
        )

    own_copies = [
        pltpu.make_async_copy(grads[array].at[:, place.core], owns[array], local_sem.at[array])
        for array in range(arrays)
    ]
    for own_copy in own_copies:
        own_copy.start()
    enter(place)
    deepest = max(edge[3] for part in parts for edge in part[3])
    for depth in range(deepest, 0, -1):
        for part, (array, _, _, tree) in enumerate(parts):
            for index, (_, child, way, level) in enumerate(tree):
                if way == "core" and level == depth:
                    chip = place.chip_of(child)
                    source = grads[array].at[chip, place.flip(place.core, 1)]
                    copy(part, index, window(source, part)).start()
    for own_copy in own_copies:
        own_copy.wait()

    def add_up(part, node, target):
        array, first, count, tree = parts[part]
        children = [index for index, edge in enumerate(tree) if edge[0] == node]
        for index in children:
            copy(part, index, lands[part].at[index]).wait_recv()
        chip = place.chip_of(node)
        rows, columns = shapes[array]
        if count is not None:
            rows = count
        row_slice = pl.ds(first, rows)
        step = columns
        while rows * step > 24 * 768 and step % 256 == 0:
            step //= 2
        own = owns[array]

        def body(block, carry):
            where = pl.ds(pl.multiple_of(block * step, 128), step)
            total = own[chip, row_slice, where].astype(jnp.float32)
            for index in children:
                total = total + lands[part][index, :, where].astype(jnp.float32)
            if target is None:
                own[chip, row_slice, where] = total.astype(own.dtype)
            else:
                target[row_slice, where] = total
            return carry

        lax.fori_loop(0, columns // step, body, 0)
        return window(own.at[chip], part)

    waiting = None
    for depth in range(deepest, 0, -1):
        for part in range(len(parts)):
            for index, (_, child, way, level) in enumerate(parts[part][3]):
                if way != "core" and level == depth:
                    ready = copy(part, index, add_up(part, child, None))
                    if waiting is not None:
                        waiting.start()
                    waiting = ready
    waiting.start()
    for part in range(len(parts)):
        add_up(part, (0, 0, 0, 0), outs[parts[part][0]])
    for part in range(len(parts)):
        pltpu.make_async_copy(lands[part], lands[part], send_sem.at[part]).wait()


def scatter_units(grads, plan, ring):
    devices = ring * 8
    edges = devices - 1
    shapes = plan["shapes"]
    lands = []
    for array, _, count, _ in plan["parts"]:
        rows, columns = shapes[array]
        lands.append(
            pltpu.VMEM((edges, rows if count is None else count, columns), jnp.bfloat16)
        )
    return pl.pallas_call(
        partial(scatter_kernel, ring, plan),
        out_shape=[jax.ShapeDtypeStruct(shape, jnp.float32) for shape in shapes],
        in_specs=[ANY_SPEC] * len(shapes),
        out_specs=[VMEM_SPEC] * len(shapes),
        scratch_shapes=[pltpu.VMEM((devices // 2,) + shape, jnp.bfloat16) for shape in shapes]
        + lands
        + [
            pltpu.SemaphoreType.DMA((len(plan["parts"]), edges)),
            pltpu.SemaphoreType.DMA((len(plan["parts"]),)),
            pltpu.SemaphoreType.DMA((len(shapes),)),
        ],
        compiler_params=pltpu.CompilerParams(
            collective_id=1, has_side_effects=True, vmem_limit_bytes=VMEM_LIMIT
        ),
        name="scatter_units",
    )(*[grad.reshape((devices // 2, 2) + shape) for grad, shape in zip(grads, shapes)])


def make_plan(shapes, ring):
    ring_trees = [make_tree(ring, True, flip) for flip in (False, True)]
    plane_trees = [make_tree(ring, False, flip) for flip in (False, True)]
    order = [
        (0, None, plane_trees[0]),
        (1, None, plane_trees[1]),
        (2, None, ring_trees[0]),
        (3, 0, ring_trees[1]),
        (3, 1, plane_trees[1]),
        (4, None, ring_trees[1]),
    ]
    parts = []
    for array, piece, tree in order:
        half = shapes[array][0] // 2
        parts.append((array, (piece or 0) * half, None if piece is None else half, tree))
    return {"shapes": shapes, "parts": parts}


def masked_softmax(scores, inside_rows, inside_columns, diagonal):
    allowed = jnp.logical_or(jnp.logical_and(inside_rows, inside_columns), diagonal)
    scores = jnp.where(allowed, scores * 0.125, -1e30)
    exponent = jnp.exp(scores - jnp.max(scores, axis=-1, keepdims=True))
    return exponent, jnp.sum(exponent, axis=-1, keepdims=True)


def mask_parts(length, rows):
    row = lax.broadcasted_iota(jnp.int32, (rows, rows), 0)
    column = lax.broadcasted_iota(jnp.int32, (rows, rows), 1)
    return row < length, column < length, row == column


def dot_nt(left, right):
    return lax.dot_general(
        left, right, (((1,), (1,)), ((), ())), preferred_element_type=jnp.float32
    )


def dot_tn(left, right):
    return lax.dot_general(
        left, right, (((0,), (0,)), ((), ())), preferred_element_type=jnp.float32
    )


def dot_nn(left, right):
    return jnp.dot(left, right, preferred_element_type=jnp.float32)


def attend_kernel(lengths_ref, q_ref, k_ref, v_ref, context_ref):
    rows, width = q_ref.shape
    masks = mask_parts(lengths_ref[pl.program_id(0)], rows)
    lane = lax.broadcasted_iota(jnp.int32, (rows, width), 1)
    queries, keys, values = q_ref[...], k_ref[...], v_ref[...]
    context = jnp.zeros((rows, width), jnp.float32)
    for head in range(width // HEAD_DIM):
        mine = lane // HEAD_DIM == head
        scores = dot_nt(jnp.where(mine, queries, jnp.zeros_like(queries)), keys)
        exponent, total = masked_softmax(scores, *masks)
        probs = (exponent / total).astype(jnp.bfloat16)
        context = jnp.where(mine, dot_nn(probs, values), context)
    context_ref[...] = context.astype(context_ref.dtype)


def attend(qkv, lengths):
    rows, width3 = qkv.shape
    width = width3 // 3
    halves = lengths.shape[0]
    half = rows // halves
    pairs = width // 128

    def columns(which):
        return pl.BlockSpec((half, 128), lambda i, j, l: (i, which * pairs + j))

    return pl.pallas_call(
        attend_kernel,
        out_shape=jax.ShapeDtypeStruct((rows, width), jnp.bfloat16),
        grid_spec=pltpu.PrefetchScalarGridSpec(
            num_scalar_prefetch=1,
            grid=(halves, pairs),
            in_specs=[columns(0), columns(1), columns(2)],
            out_specs=columns(0),
        ),
        compiler_params=pltpu.CompilerParams(vmem_limit_bytes=VMEM_LIMIT),
        name="attend",
    )(lengths, qkv, qkv, qkv)


def attend_back_kernel(lengths_ref, q_ref, k_ref, v_ref, g_ref, grad_ref, sums_ref):
    rows, width = q_ref.shape
    masks = mask_parts(lengths_ref[pl.program_id(0)], rows)
    lane = lax.broadcasted_iota(jnp.int32, (rows, width), 1)
    queries, keys, values, grads = q_ref[...], k_ref[...], v_ref[...], g_ref[...]
    zero = jnp.zeros_like(queries)
    grad_q = jnp.zeros((rows, width), jnp.float32)
    grad_k, grad_v = grad_q, grad_q
    for head in range(width // HEAD_DIM):
        mine = lane // HEAD_DIM == head
        scores = dot_nt(jnp.where(mine, queries, zero), keys)
        exponent, total = masked_softmax(scores, *masks)
        probs = exponent / total
        grad_v = jnp.where(mine, dot_tn(probs.astype(jnp.bfloat16), grads), grad_v)
        grad_probs = dot_nt(jnp.where(mine, grads, zero), values)
        along = jnp.sum(probs * grad_probs, axis=-1, keepdims=True)
        grad_scores = (probs * (grad_probs - along)).astype(jnp.bfloat16)
        grad_q = jnp.where(mine, dot_nn(grad_scores, keys) * 0.125, grad_q)
        grad_k = jnp.where(mine, dot_tn(grad_scores, queries) * 0.125, grad_k)
    for place, grad in enumerate((grad_q, grad_k, grad_v)):
        grad_ref[place] = grad.astype(grad_ref.dtype)
        sums_ref[0, place] = jnp.sum(grad, axis=0, keepdims=True)


def attend_back(qkv, grad_context, lengths):
    rows, width3 = qkv.shape
    width = width3 // 3
    halves = lengths.shape[0]
    half = rows // halves
    pairs = width // 128

    def columns(which):
        return pl.BlockSpec((half, 128), lambda i, j, l: (i, which * pairs + j))

    return pl.pallas_call(
        attend_back_kernel,
        out_shape=[
            jax.ShapeDtypeStruct((3, rows, width), jnp.bfloat16),
            jax.ShapeDtypeStruct((halves, 3, 1, width), jnp.float32),
        ],
        grid_spec=pltpu.PrefetchScalarGridSpec(
            num_scalar_prefetch=1,
            grid=(halves, pairs),
            in_specs=[columns(0), columns(1), columns(2), columns(0)],
            out_specs=[
                pl.BlockSpec((3, half, 128), lambda i, j, l: (0, i, j)),
                pl.BlockSpec((1, 3, 1, 128), lambda i, j, l: (i, 0, 0, j)),
            ],
        ),
        compiler_params=pltpu.CompilerParams(vmem_limit_bytes=VMEM_LIMIT),
        name="attend_back",
    )(lengths, qkv, qkv, qkv, grad_context)


ERFC_TERMS = (
    0.17087277,
    -0.82215223,
    1.48851587,
    -1.13520398,
    0.27886807,
    -0.18628806,
    0.09678418,
    0.37409196,
    1.00002368,
    -1.26551223,
)


def gelu_parts(u):
    x = jnp.abs(u) * 0.7071067811865476
    square = -0.5 * u * u
    t = 1.0 / (1.0 + 0.5 * x)
    poly = ERFC_TERMS[0]
    for term in ERFC_TERMS[1:]:
        poly = poly * t + term
    tail = 0.5 * t * jnp.exp(poly + square)
    cdf = jnp.where(u < 0, tail, 1.0 - tail)
    return u * cdf, cdf + u * jnp.exp(square) * 0.3989422804014327


def up_kernel(first_ref, w_ref, b_ref, active_ref, slope_ref):
    rows = first_ref.shape[0]
    step = 128
    for start in range(0, rows, step):
        where = pl.ds(start, step)
        u = dot_nn(first_ref[where, :], w_ref[...]) + b_ref[...]
        value, slope = gelu_parts(u)
        active_ref[where, :] = value.astype(active_ref.dtype)
        slope_ref[where, :] = slope.astype(slope_ref.dtype)


def up_project(first_low, w_up, b_up):
    rows, width = first_low.shape
    hidden = w_up.shape[1]
    block = 512
    return pl.pallas_call(
        up_kernel,
        out_shape=[jax.ShapeDtypeStruct((rows, hidden), jnp.bfloat16)] * 2,
        grid=(hidden // block,),
        in_specs=[
            pl.BlockSpec((rows, width), lambda j: (0, 0)),
            pl.BlockSpec((width, block), lambda j: (0, j)),
            pl.BlockSpec((1, block), lambda j: (0, j)),
        ],
        out_specs=[pl.BlockSpec((rows, block), lambda j: (0, j))] * 2,
        compiler_params=pltpu.CompilerParams(vmem_limit_bytes=VMEM_LIMIT),
        name="up_project",
    )(first_low, w_up, b_up.reshape(1, hidden))


def norm_parts(hidden):
    center = hidden - jnp.mean(hidden, axis=-1, keepdims=True)
    inverse = lax.rsqrt(jnp.mean(center * center, axis=-1, keepdims=True) + 1e-12)
    return (center * inverse, inverse)


def norm_back(grad_out, normed, inverse, gain):
    scaled = grad_out * gain
    centered = scaled - jnp.mean(scaled, axis=-1, keepdims=True)
    return inverse * (centered - normed * jnp.mean(scaled * normed, axis=-1, keepdims=True))


def block_slots(lengths, row_count):
    half = row_count // 2
    row = jnp.arange(row_count, dtype=jnp.int32)
    first, second = lengths[0], lengths[1]
    slot = jnp.where(
        row < half,
        jnp.where(row < first, row, row + second),
        jnp.where(row - half < second, row - half + first, row),
    )
    return slot, jnp.where(row < half, row < first, row - half < second)


def gather_params(params, ring):
    (w_qkv, b_qv, w_out, b_out, g1, c1, w_up, b_up, w_down, b_down, g2, c2, w_proj) = params
    small = [b_qv, b_out, g1, c1, b_up, b_down, g2, c2]
    sizes = [entry.shape[0] for entry in small]
    if ring is None:
        whole = [lax.all_gather(w, AXIS, axis=0, tiled=True) for w in (w_qkv, w_out, w_up, w_down)]
        proj = lax.all_gather(w_proj, AXIS, axis=0, tiled=True)
        few = lax.all_gather(jnp.concatenate(small), AXIS, axis=0)
    else:
        packed = jnp.concatenate(small)
        packed = jnp.pad(packed, (0, 1024 - packed.shape[0])).reshape(8, 128)
        shards = [w_qkv, w_out, w_up, w_down, jnp.concatenate([w_proj, packed], axis=0)]
        plan = make_plan([shard.shape for shard in shards], ring)
        units = gather_units(shards, plan, ring)
        whole = [unit.reshape(-1, unit.shape[2]) for unit in units[:4]]
        rows = w_proj.shape[0]
        proj = units[4][:, :rows].reshape(-1, w_proj.shape[1])
        few = units[4][:, rows:].reshape(units[4].shape[0], -1)
    vectors = []
    start = 0
    for size in sizes:
        vectors.append(few[:, start : start + size].reshape(-1).astype(jnp.float32))
        start += size
    return whole + [proj], vectors


def scatter_grads(weights, vectors, ring, devices):
    few = [vector.reshape(devices, -1) for vector in vectors]
    sizes = [entry.shape[1] for entry in few]
    few = jnp.concatenate(few, axis=1)
    if ring is None:
        shards = [
            lax.psum_scatter(w, AXIS, scatter_dimension=0, tiled=True).astype(jnp.float32)
            for w in weights
        ]
        small = lax.psum_scatter(few.reshape(-1), AXIS, scatter_dimension=0, tiled=True)
    else:
        few = jnp.pad(few, ((0, 0), (0, 1024 - few.shape[1]))).astype(jnp.bfloat16)
        units = [w.reshape(devices, -1, w.shape[1]) for w in weights]
        rows = units[4].shape[1]
        units[4] = jnp.concatenate([units[4], few.reshape(devices, 8, 128)], axis=1)
        plan = make_plan([unit.shape[1:] for unit in units], ring)
        shards = list(scatter_units(units, plan, ring))
        small = shards[4][rows:].reshape(-1)
        shards[4] = shards[4][:rows]
    pieces = []
    start = 0
    for size in sizes:
        pieces.append(small[start : start + size])
        start += size
    return shards, pieces


def local(tokens, cotangent, slot_row, lengths, *params):
    devices = lax.axis_size(AXIS)
    row_count, model_width = tokens.shape
    peer_rows = row_count // devices
    ring = devices // 8 if params[0].shape[0] % 8 == 0 and devices % 8 == 0 else None
    (w_qkv, w_out, w_up, w_down, w_proj), vectors = gather_params(params, ring)
    b_qv, b_out, gain_one, bias_one, b_up, b_down, gain_two, bias_two = vectors

    slot, inside = block_slots(lengths, row_count)
    local_row = (slot_row // row_count * peer_rows + slot_row % peer_rows)[slot]
    both = jnp.concatenate([tokens, cotangent], axis=1)
    arrived = lax.all_to_all(both, AXIS, split_axis=0, concat_axis=0, tiled=True)[local_row]
    dealt, dealt_cot = arrived[:, :model_width], arrived[:, model_width:]
    valid = inside[:, None].astype(jnp.float32)

    bias_all = jnp.concatenate(
        [b_qv[:model_width], jnp.zeros((model_width,), jnp.float32), b_qv[model_width:]]
    )
    qkv = (dot_nn(dealt, w_qkv) + bias_all).astype(jnp.bfloat16)
    context = attend(qkv, lengths)
    hidden_one = dealt.astype(jnp.float32) + dot_nn(context, w_out) + b_out
    normed_one, inverse_one = norm_parts(hidden_one)
    first_low = (normed_one * gain_one + bias_one).astype(jnp.bfloat16)
    active, slope = up_project(first_low, w_up, b_up)
    hidden_two = first_low.astype(jnp.float32) + dot_nn(active, w_down) + b_down
    normed_two, inverse_two = norm_parts(hidden_two)
    second_low = (normed_two * gain_two + bias_two).astype(jnp.bfloat16)
    project = dot_nn(second_low, w_proj)
    inv_norm = lax.rsqrt(jnp.sum(project * project, axis=-1, keepdims=True) + 1e-06)
    embedded = (project * inv_norm * valid).astype(jnp.bfloat16)

    grad_emb = dealt_cot.astype(jnp.float32) * valid
    along = jnp.sum(project * grad_emb, axis=-1, keepdims=True)
    grad_project = (inv_norm * grad_emb - inv_norm * inv_norm * inv_norm * along * project).astype(
        jnp.bfloat16
    )
    grad_w_proj = dot_tn(second_low, grad_project).astype(jnp.bfloat16)
    grad_second = dot_nt(grad_project, w_proj)
    grad_gain_two = jnp.sum(grad_second * normed_two, axis=0)
    grad_bias_two = jnp.sum(grad_second, axis=0)
    grad_hidden_two = norm_back(grad_second, normed_two, inverse_two, gain_two)
    grad_b_down = jnp.sum(grad_hidden_two, axis=0)
    down_low = grad_hidden_two.astype(jnp.bfloat16)
    grad_w_down = dot_tn(active, down_low).astype(jnp.bfloat16)
    grad_up = dot_nt(down_low, w_down) * slope.astype(jnp.float32)
    grad_b_up = jnp.sum(grad_up, axis=0)
    up_low = grad_up.astype(jnp.bfloat16)
    grad_w_up = dot_tn(first_low, up_low).astype(jnp.bfloat16)
    grad_first = grad_hidden_two + dot_nt(up_low, w_up)
    grad_gain_one = jnp.sum(grad_first * normed_one, axis=0)
    grad_bias_one = jnp.sum(grad_first, axis=0)
    grad_hidden_one = norm_back(grad_first, normed_one, inverse_one, gain_one)
    grad_b_out = jnp.sum(grad_hidden_one, axis=0)
    out_low = grad_hidden_one.astype(jnp.bfloat16)
    grad_w_out = dot_tn(context, out_low).astype(jnp.bfloat16)
    grad_context = dot_nt(out_low, w_out).astype(jnp.bfloat16)
    grad_three, sums = attend_back(qkv, grad_context, lengths)
    sums = jnp.sum(sums, axis=0)[:, 0]
    grad_b_qv = jnp.concatenate([sums[0], sums[2]])
    grad_qkv = jnp.concatenate([grad_three[0], grad_three[1], grad_three[2]], axis=1)
    grad_w_qkv = dot_tn(dealt, grad_qkv).astype(jnp.bfloat16)
    grad_dealt = (dot_nt(grad_qkv, w_qkv) + grad_hidden_one).astype(jnp.bfloat16)

    inverse_row = (
        jnp.zeros((row_count,), jnp.int32).at[local_row].set(jnp.arange(row_count, dtype=jnp.int32))
    )
    back = jnp.concatenate([grad_dealt, embedded], axis=1)[inverse_row]
    returned = lax.all_to_all(back, AXIS, split_axis=0, concat_axis=0, tiled=True)
    shards, small = scatter_grads(
        [grad_w_qkv, grad_w_out, grad_w_up, grad_w_down, grad_w_proj],
        [
            grad_b_qv,
            grad_b_out,
            grad_gain_one,
            grad_bias_one,
            grad_b_up,
            grad_b_down,
            grad_gain_two,
            grad_bias_two,
        ],
        ring,
        devices,
    )
    return (
        returned[:, model_width:],
        returned[:, :model_width],
        shards[0],
        small[0],
        shards[1],
        small[1],
        small[2],
        small[3],
        shards[2],
        small[4],
        shards[3],
        small[5],
        small[6],
        small[7],
        shards[4],
    )


def solution(mesh):
    matrix, vector = P(AXIS, None), P(AXIS)
    params = "mvmvvvmvmvvvm"
    in_kinds = "mmvv" + params
    out_kinds = "mm" + params
    specs = {"m": matrix, "v": vector}
    return jax.shard_map(
        local,
        mesh=mesh,
        in_specs=tuple(specs[kind] for kind in in_kinds),
        out_specs=tuple(specs[kind] for kind in out_kinds),
        check_vma=False,
    )
```

```python
from functools import partial

import jax
import jax.numpy as jnp
from jax import lax
from jax.experimental import pallas as pl
from jax.experimental.pallas import tpu as pltpu
from jax.sharding import PartitionSpec as P

HEADS = 12
HEAD_DIM = 64
AXIS = "fsdp"
MESH_ID = pl.DeviceIdType.MESH
VMEM_SPEC = pl.BlockSpec(memory_space=pltpu.VMEM)
ANY_SPEC = pl.BlockSpec(memory_space=pl.ANY)
VMEM_LIMIT = 60 * 1024 * 1024


def chain_edges(node, ring, lean_up):
    up_count = ring // 2 if lean_up else (ring - 1) // 2
    edges = []
    here = node
    for _ in range(up_count):
        there = ((here[0] + 1) % ring,) + here[1:]
        edges.append((here, there, "up"))
        here = there
    here = node
    for _ in range(ring - 1 - up_count):
        there = ((here[0] - 1) % ring,) + here[1:]
        edges.append((here, there, "down"))
        here = there
    return edges


def plane_edges(node, x_first):
    z = node[0]
    own, by_x, by_y, both = (z, 0, 0, 0), (z, 0, 1, 0), (z, 1, 0, 0), (z, 1, 1, 0)
    edges = [(own, by_x, "x"), (own, by_y, "y")]
    edges.append((by_x, both, "y") if x_first else (by_y, both, "x"))
    return edges


def make_tree(ring, ring_first, flip):
    root = (0, 0, 0, 0)
    edges = []
    if ring_first:
        edges += chain_edges(root, ring, flip)
        nodes = [root] + [edge[1] for edge in edges]
        for place, node in enumerate(nodes):
            edges += plane_edges(node, (place % 2 == 0) != flip)
    else:
        edges += plane_edges(root, flip)
        nodes = [root] + [edge[1] for edge in edges]
        for place, node in enumerate(nodes):
            edges += chain_edges(node, ring, (place % 2 == 0) != flip)
    nodes = [root] + [edge[1] for edge in edges]
    edges += [(node, node[:3] + (1,), "core") for node in nodes]
    depth = {root: 0}
    for parent, child, _ in edges:
        depth[child] = depth[parent] + 1
    order = sorted(range(len(edges)), key=lambda index: depth[edges[index][1]])
    return [edges[index] + (depth[edges[index][1]],) for index in order]


class Place:
    def __init__(self, ring):
        me = lax.axis_index(AXIS)
        self.ring = ring
        self.me = me
        self.core = lax.rem(me, 2)
        self.x = lax.rem(me // 2, 2)
        self.y = lax.rem(me // 4, 2)
        self.z = me // 8

    @staticmethod
    def flip(value, amount):
        return 1 - value if amount else value

    def chip_of(self, offset):
        z = lax.rem(self.z + (self.ring - offset[0]) % self.ring, self.ring)
        return (z * 2 + self.flip(self.y, offset[1])) * 2 + self.flip(self.x, offset[2])

    def unit_of(self, offset):
        return self.chip_of(offset) * 2 + self.flip(self.core, offset[3])

    def neighbour(self, way, back=False):
        step = {"up": (1, 0, 0, 0), "down": (-1, 0, 0, 0), "x": (0, 0, 1, 0)}
        step.update({"y": (0, 1, 0, 0), "core": (0, 0, 0, 1)})
        offset = step[way]
        dz = offset[0] if back else -offset[0]
        return self.unit_of((dz % self.ring,) + offset[1:])


def enter(place):
    barrier = pltpu.get_barrier_semaphore()
    for way in ("up", "down", "x", "y", "core"):
        pl.semaphore_signal(
            barrier, inc=1, device_id=(place.neighbour(way),), device_id_type=MESH_ID
        )
    pl.semaphore_wait(barrier, 5)


def gather_kernel(ring, plan, *refs):
    arrays = len(plan["shapes"])
    shards, outs = refs[:arrays], refs[arrays : 2 * arrays]
    recv_sem, send_sem, local_sem = refs[2 * arrays :]
    place = Place(ring)
    parts = plan["parts"]

    def window(ref, part):
        _, first, count, _ = parts[part]
        return ref if count is None else ref.at[:, pl.ds(first, count)]

    def copy(part, index):
        array, _, _, tree = parts[part]
        parent, _, way, _ = tree[index]
        unit = place.unit_of(parent)
        source = shards[array] if parent == (0, 0, 0, 0) else outs[array].at[unit]
        return pltpu.make_async_remote_copy(
            src_ref=window(source, part),
            dst_ref=window(outs[array].at[unit], part),
            send_sem=send_sem.at[part],
            recv_sem=recv_sem.at[part, index],
            device_id=(place.neighbour(way),),
            device_id_type=MESH_ID,
        )

    def arrived(part, index):
        array, _, _, tree = parts[part]
        _, child, way, _ = tree[index]
        landed = window(outs[array].at[place.unit_of(child)], part)
        pltpu.make_async_remote_copy(
            src_ref=landed,
            dst_ref=landed,
            send_sem=send_sem.at[part],
            recv_sem=recv_sem.at[part, index],
            device_id=(place.neighbour(way),),
            device_id_type=MESH_ID,
        ).wait_recv()

    def send_from(part, node):
        for index, edge in enumerate(parts[part][3]):
            if edge[0] == node:
                copy(part, index).start()

    own_copies = [
        pltpu.make_async_copy(shards[array], outs[array].at[place.me], local_sem.at[array])
        for array in range(arrays)
    ]
    for own_copy in own_copies:
        own_copy.start()
    enter(place)
    for part in range(len(parts)):
        send_from(part, (0, 0, 0, 0))
    deepest = max(edge[3] for part in parts for edge in part[3])
    for depth in range(1, deepest + 1):
        for part in range(len(parts)):
            for index, edge in enumerate(parts[part][3]):
                if edge[3] == depth and edge[2] != "core":
                    arrived(part, index)
                    send_from(part, edge[1])
    for part in range(len(parts)):
        for index, edge in enumerate(parts[part][3]):
            if edge[2] == "core":
                arrived(part, index)
    for own_copy in own_copies:
        own_copy.wait()
    for part, (array, first, count, tree) in enumerate(parts):
        whole = outs[array].at[pl.ds(0, len(tree))]
        if count is not None:
            whole = whole.at[:, :, pl.ds(first, count)]
        pltpu.make_async_copy(whole, whole, send_sem.at[part]).wait()


def gather_units(shards, plan, ring):
    devices = ring * 8
    edges = devices - 1
    return pl.pallas_call(
        partial(gather_kernel, ring, plan),
        out_shape=[
            jax.ShapeDtypeStruct((devices,) + shard.shape, shard.dtype) for shard in shards
        ],
        in_specs=[VMEM_SPEC] * len(shards),
        out_specs=[ANY_SPEC] * len(shards),
        scratch_shapes=[
            pltpu.SemaphoreType.DMA((len(plan["parts"]), edges)),
            pltpu.SemaphoreType.DMA((len(plan["parts"]),)),
            pltpu.SemaphoreType.DMA((len(shards),)),
        ],
        compiler_params=pltpu.CompilerParams(collective_id=0, has_side_effects=True),
        name="gather_units",
    )(*shards)


def scatter_kernel(ring, plan, *refs):
    shapes = plan["shapes"]
    arrays = len(shapes)
    parts = plan["parts"]
    grads, outs = refs[:arrays], refs[arrays : 2 * arrays]
    owns = refs[2 * arrays : 3 * arrays]
    lands = refs[3 * arrays : 3 * arrays + len(parts)]
    recv_sem, send_sem, local_sem = refs[3 * arrays + len(parts) :]
    place = Place(ring)

    def window(ref, part):
        _, first, count, _ = parts[part]
        return ref if count is None else ref.at[:, pl.ds(first, count)]

    def copy(part, index, source):
        way = parts[part][3][index][2]
        return pltpu.make_async_remote_copy(
            src_ref=source,
            dst_ref=lands[part].at[index],
            send_sem=send_sem.at[part],
            recv_sem=recv_sem.at[part, index],
            device_id=(place.neighbour(way, back=True),),
            device_id_type=MESH_ID,
        )

    own_copies = [
        pltpu.make_async_copy(grads[array].at[:, place.core], owns[array], local_sem.at[array])
        for array in range(arrays)
    ]
    for own_copy in own_copies:
        own_copy.start()
    enter(place)
    deepest = max(edge[3] for part in parts for edge in part[3])
    for depth in range(deepest, 0, -1):
        for part, (array, _, _, tree) in enumerate(parts):
            for index, (_, child, way, level) in enumerate(tree):
                if way == "core" and level == depth:
                    chip = place.chip_of(child)
                    source = grads[array].at[chip, place.flip(place.core, 1)]
                    copy(part, index, window(source, part)).start()
    for own_copy in own_copies:
        own_copy.wait()

    def add_up(part, node, target):
        array, first, count, tree = parts[part]
        children = [index for index, edge in enumerate(tree) if edge[0] == node]
        for index in children:
            copy(part, index, lands[part].at[index]).wait_recv()
        chip = place.chip_of(node)
        rows, columns = shapes[array]
        if count is not None:
            columns = count
        step = columns
        while rows * step > 24 * 768 and step % 256 == 0:
            step //= 2
        own = owns[array]

        def body(block, carry):
            here = pl.ds(pl.multiple_of(block * step, 128), step)
            where = pl.ds(pl.multiple_of(first + block * step, 128), step)
            total = own[chip, :, where].astype(jnp.float32)
            for index in children:
                total = total + lands[part][index, :, here].astype(jnp.float32)
            if target is None:
                own[chip, :, where] = total.astype(own.dtype)
            else:
                target[:, where] = total
            return carry

        lax.fori_loop(0, columns // step, body, 0)
        return window(own.at[chip], part)

    waiting = None
    for depth in range(deepest, 0, -1):
        for part in range(len(parts)):
            for index, (_, child, way, level) in enumerate(parts[part][3]):
                if way != "core" and level == depth:
                    ready = copy(part, index, add_up(part, child, None))
                    if waiting is not None:
                        waiting.start()
                    waiting = ready
    waiting.start()
    for part in range(len(parts)):
        add_up(part, (0, 0, 0, 0), outs[parts[part][0]])
    for part in range(len(parts)):
        pltpu.make_async_copy(lands[part], lands[part], send_sem.at[part]).wait()


def scatter_units(grads, plan, ring):
    devices = ring * 8
    edges = devices - 1
    shapes = plan["shapes"]
    lands = []
    for array, _, count, _ in plan["parts"]:
        rows, columns = shapes[array]
        lands.append(
            pltpu.VMEM((edges, rows, columns if count is None else count), jnp.bfloat16)
        )
    return pl.pallas_call(
        partial(scatter_kernel, ring, plan),
        out_shape=[jax.ShapeDtypeStruct(shape, jnp.float32) for shape in shapes],
        in_specs=[ANY_SPEC] * len(shapes),
        out_specs=[VMEM_SPEC] * len(shapes),
        scratch_shapes=[pltpu.VMEM((devices // 2,) + shape, jnp.bfloat16) for shape in shapes]
        + lands
        + [
            pltpu.SemaphoreType.DMA((len(plan["parts"]), edges)),
            pltpu.SemaphoreType.DMA((len(plan["parts"]),)),
            pltpu.SemaphoreType.DMA((len(shapes),)),
        ],
        compiler_params=pltpu.CompilerParams(
            collective_id=1, has_side_effects=True, vmem_limit_bytes=VMEM_LIMIT
        ),
        name="scatter_units",
    )(*[grad.reshape((devices // 2, 2) + shape) for grad, shape in zip(grads, shapes)])


def make_plan(shapes, ring):
    trees = [make_tree(ring, first, flip) for first in (True, False) for flip in (False, True)]
    parts = []
    for array, (_, columns) in enumerate(shapes):
        flip = array % 2
        if columns % 256 == 0:
            half = columns // 2
            parts.append((array, 0, half, trees[flip]))
            parts.append((array, half, half, trees[2 + flip]))
        else:
            parts.append((array, 0, None, trees[flip]))
    return {"shapes": shapes, "parts": parts}


def masked_softmax(scores, inside_rows, inside_columns, diagonal):
    allowed = jnp.logical_or(jnp.logical_and(inside_rows, inside_columns), diagonal)
    scores = jnp.where(allowed, scores * 0.125, -1e30)
    exponent = jnp.exp(scores - jnp.max(scores, axis=-1, keepdims=True))
    return exponent, jnp.sum(exponent, axis=-1, keepdims=True)


def mask_parts(length, rows):
    row = lax.broadcasted_iota(jnp.int32, (rows, rows), 0)
    column = lax.broadcasted_iota(jnp.int32, (rows, rows), 1)
    return row < length, column < length, row == column


def dot_nt(left, right):
    return lax.dot_general(
        left, right, (((1,), (1,)), ((), ())), preferred_element_type=jnp.float32
    )


def dot_tn(left, right):
    return lax.dot_general(
        left, right, (((0,), (0,)), ((), ())), preferred_element_type=jnp.float32
    )


def dot_nn(left, right):
    return jnp.dot(left, right, preferred_element_type=jnp.float32)


def attend_kernel(lengths_ref, q_ref, k_ref, v_ref, context_ref):
    rows, width = q_ref.shape
    masks = mask_parts(lengths_ref[pl.program_id(0)], rows)
    lane = lax.broadcasted_iota(jnp.int32, (rows, width), 1)
    queries, keys, values = q_ref[...], k_ref[...], v_ref[...]
    context = jnp.zeros((rows, width), jnp.float32)
    for head in range(width // HEAD_DIM):
        mine = lane // HEAD_DIM == head
        scores = dot_nt(jnp.where(mine, queries, jnp.zeros_like(queries)), keys)
        exponent, total = masked_softmax(scores, *masks)
        probs = (exponent / total).astype(jnp.bfloat16)
        context = jnp.where(mine, dot_nn(probs, values), context)
    context_ref[...] = context.astype(context_ref.dtype)


def attend(qkv, lengths):
    rows, width3 = qkv.shape
    width = width3 // 3
    halves = lengths.shape[0]
    half = rows // halves
    pairs = width // 128

    def columns(which):
        return pl.BlockSpec((half, 128), lambda i, j, l: (i, which * pairs + j))

    return pl.pallas_call(
        attend_kernel,
        out_shape=jax.ShapeDtypeStruct((rows, width), jnp.bfloat16),
        grid_spec=pltpu.PrefetchScalarGridSpec(
            num_scalar_prefetch=1,
            grid=(halves, pairs),
            in_specs=[columns(0), columns(1), columns(2)],
            out_specs=columns(0),
        ),
        compiler_params=pltpu.CompilerParams(vmem_limit_bytes=VMEM_LIMIT),
        name="attend",
    )(lengths, qkv, qkv, qkv)


def attend_back_kernel(lengths_ref, q_ref, k_ref, v_ref, g_ref, grad_ref, sums_ref):
    rows, width = q_ref.shape
    masks = mask_parts(lengths_ref[pl.program_id(0)], rows)
    lane = lax.broadcasted_iota(jnp.int32, (rows, width), 1)
    queries, keys, values, grads = q_ref[...], k_ref[...], v_ref[...], g_ref[...]
    zero = jnp.zeros_like(queries)
    grad_q = jnp.zeros((rows, width), jnp.float32)
    grad_k, grad_v = grad_q, grad_q
    for head in range(width // HEAD_DIM):
        mine = lane // HEAD_DIM == head
        scores = dot_nt(jnp.where(mine, queries, zero), keys)
        exponent, total = masked_softmax(scores, *masks)
        probs = exponent / total
        grad_v = jnp.where(mine, dot_tn(probs.astype(jnp.bfloat16), grads), grad_v)
        grad_probs = dot_nt(jnp.where(mine, grads, zero), values)
        along = jnp.sum(probs * grad_probs, axis=-1, keepdims=True)
        grad_scores = (probs * (grad_probs - along)).astype(jnp.bfloat16)
        grad_q = jnp.where(mine, dot_nn(grad_scores, keys) * 0.125, grad_q)
        grad_k = jnp.where(mine, dot_tn(grad_scores, queries) * 0.125, grad_k)
    for place, grad in enumerate((grad_q, grad_k, grad_v)):
        grad_ref[place] = grad.astype(grad_ref.dtype)
        sums_ref[0, place] = jnp.sum(grad, axis=0, keepdims=True)


def attend_back(qkv, grad_context, lengths):
    rows, width3 = qkv.shape
    width = width3 // 3
    halves = lengths.shape[0]
    half = rows // halves
    pairs = width // 128

    def columns(which):
        return pl.BlockSpec((half, 128), lambda i, j, l: (i, which * pairs + j))

    return pl.pallas_call(
        attend_back_kernel,
        out_shape=[
            jax.ShapeDtypeStruct((3, rows, width), jnp.bfloat16),
            jax.ShapeDtypeStruct((halves, 3, 1, width), jnp.float32),
        ],
        grid_spec=pltpu.PrefetchScalarGridSpec(
            num_scalar_prefetch=1,
            grid=(halves, pairs),
            in_specs=[columns(0), columns(1), columns(2), columns(0)],
            out_specs=[
                pl.BlockSpec((3, half, 128), lambda i, j, l: (0, i, j)),
                pl.BlockSpec((1, 3, 1, 128), lambda i, j, l: (i, 0, 0, j)),
            ],
        ),
        compiler_params=pltpu.CompilerParams(vmem_limit_bytes=VMEM_LIMIT),
        name="attend_back",
    )(lengths, qkv, qkv, qkv, grad_context)


ERFC_TERMS = (
    0.17087277,
    -0.82215223,
    1.48851587,
    -1.13520398,
    0.27886807,
    -0.18628806,
    0.09678418,
    0.37409196,
    1.00002368,
    -1.26551223,
)


def gelu_parts(u):
    x = jnp.abs(u) * 0.7071067811865476
    square = -0.5 * u * u
    t = 1.0 / (1.0 + 0.5 * x)
    poly = ERFC_TERMS[0]
    for term in ERFC_TERMS[1:]:
        poly = poly * t + term
    tail = 0.5 * t * jnp.exp(poly + square)
    cdf = jnp.where(u < 0, tail, 1.0 - tail)
    return u * cdf, cdf + u * jnp.exp(square) * 0.3989422804014327


def up_kernel(first_ref, w_ref, b_ref, active_ref, slope_ref):
    rows = first_ref.shape[0]
    step = 128
    for start in range(0, rows, step):
        where = pl.ds(start, step)
        u = dot_nn(first_ref[where, :], w_ref[...]) + b_ref[...]
        value, slope = gelu_parts(u)
        active_ref[where, :] = value.astype(active_ref.dtype)
        slope_ref[where, :] = slope.astype(slope_ref.dtype)


def up_project(first_low, w_up, b_up):
    rows, width = first_low.shape
    hidden = w_up.shape[1]
    block = 512
    return pl.pallas_call(
        up_kernel,
        out_shape=[jax.ShapeDtypeStruct((rows, hidden), jnp.bfloat16)] * 2,
        grid=(hidden // block,),
        in_specs=[
            pl.BlockSpec((rows, width), lambda j: (0, 0)),
            pl.BlockSpec((width, block), lambda j: (0, j)),
            pl.BlockSpec((1, block), lambda j: (0, j)),
        ],
        out_specs=[pl.BlockSpec((rows, block), lambda j: (0, j))] * 2,
        compiler_params=pltpu.CompilerParams(vmem_limit_bytes=VMEM_LIMIT),
        name="up_project",
    )(first_low, w_up, b_up.reshape(1, hidden))


def norm_parts(hidden):
    center = hidden - jnp.mean(hidden, axis=-1, keepdims=True)
    inverse = lax.rsqrt(jnp.mean(center * center, axis=-1, keepdims=True) + 1e-12)
    return (center * inverse, inverse)


def norm_back(grad_out, normed, inverse, gain):
    scaled = grad_out * gain
    centered = scaled - jnp.mean(scaled, axis=-1, keepdims=True)
    return inverse * (centered - normed * jnp.mean(scaled * normed, axis=-1, keepdims=True))


def block_slots(lengths, row_count):
    half = row_count // 2
    row = jnp.arange(row_count, dtype=jnp.int32)
    first, second = lengths[0], lengths[1]
    slot = jnp.where(
        row < half,
        jnp.where(row < first, row, row + second),
        jnp.where(row - half < second, row - half + first, row),
    )
    return slot, jnp.where(row < half, row < first, row - half < second)


def gather_params(params, ring):
    (w_qkv, b_qv, w_out, b_out, g1, c1, w_up, b_up, w_down, b_down, g2, c2, w_proj) = params
    small = [b_qv, b_out, g1, c1, b_up, b_down, g2, c2]
    sizes = [entry.shape[0] for entry in small]
    if ring is None:
        whole = [lax.all_gather(w, AXIS, axis=0, tiled=True) for w in (w_qkv, w_out, w_up, w_down)]
        proj = lax.all_gather(w_proj, AXIS, axis=0, tiled=True)
        few = lax.all_gather(jnp.concatenate(small), AXIS, axis=0)
    else:
        packed = jnp.concatenate(small)
        packed = jnp.pad(packed, (0, 1024 - packed.shape[0])).reshape(8, 128)
        large = [lax.all_gather(w, AXIS, axis=0, tiled=True) for w in (w_up, w_down)]
        shards = [w_qkv, w_out, jnp.concatenate([w_proj, packed], axis=0)]
        plan = make_plan([shard.shape for shard in shards], ring)
        units = gather_units(shards, plan, ring)
        whole = [unit.reshape(-1, unit.shape[2]) for unit in units[:2]] + large
        rows = w_proj.shape[0]
        proj = units[2][:, :rows].reshape(-1, w_proj.shape[1])
        few = units[2][:, rows:].reshape(units[2].shape[0], -1)
    vectors = []
    start = 0
    for size in sizes:
        vectors.append(few[:, start : start + size].reshape(-1).astype(jnp.float32))
        start += size
    return whole + [proj], vectors


def scatter_grads(weights, vectors, ring, devices):
    few = [vector.reshape(devices, -1) for vector in vectors]
    sizes = [entry.shape[1] for entry in few]
    few = jnp.concatenate(few, axis=1)
    if ring is None:
        shards = [
            lax.psum_scatter(w, AXIS, scatter_dimension=0, tiled=True).astype(jnp.float32)
            for w in weights
        ]
        small = lax.psum_scatter(few.reshape(-1), AXIS, scatter_dimension=0, tiled=True)
    else:
        few = jnp.pad(few, ((0, 0), (0, 1024 - few.shape[1]))).astype(jnp.bfloat16)
        large = [
            lax.psum_scatter(w, AXIS, scatter_dimension=0, tiled=True).astype(jnp.float32)
            for w in weights[2:4]
        ]
        units = [w.reshape(devices, -1, w.shape[1]) for w in weights[:2] + weights[4:]]
        rows = units[2].shape[1]
        units[2] = jnp.concatenate([units[2], few.reshape(devices, 8, 128)], axis=1)
        plan = make_plan([unit.shape[1:] for unit in units], ring)
        shards = list(scatter_units(units, plan, ring))
        small = shards[2][rows:].reshape(-1)
        shards = shards[:2] + large + [shards[2][:rows]]
    pieces = []
    start = 0
    for size in sizes:
        pieces.append(small[start : start + size])
        start += size
    return shards, pieces


def local(tokens, cotangent, slot_row, lengths, *params):
    devices = lax.axis_size(AXIS)
    row_count, model_width = tokens.shape
    peer_rows = row_count // devices
    ring = devices // 8 if params[0].shape[0] % 8 == 0 and devices % 8 == 0 else None
    (w_qkv, w_out, w_up, w_down, w_proj), vectors = gather_params(params, ring)
    b_qv, b_out, gain_one, bias_one, b_up, b_down, gain_two, bias_two = vectors

    slot, inside = block_slots(lengths, row_count)
    local_row = (slot_row // row_count * peer_rows + slot_row % peer_rows)[slot]
    both = jnp.concatenate([tokens, cotangent], axis=1)
    arrived = lax.all_to_all(both, AXIS, split_axis=0, concat_axis=0, tiled=True)[local_row]
    dealt, dealt_cot = arrived[:, :model_width], arrived[:, model_width:]
    valid = inside[:, None].astype(jnp.float32)

    bias_all = jnp.concatenate(
        [b_qv[:model_width], jnp.zeros((model_width,), jnp.float32), b_qv[model_width:]]
    )
    qkv = (dot_nn(dealt, w_qkv) + bias_all).astype(jnp.bfloat16)
    context = attend(qkv, lengths)
    hidden_one = dealt.astype(jnp.float32) + dot_nn(context, w_out) + b_out
    normed_one, inverse_one = norm_parts(hidden_one)
    first_low = (normed_one * gain_one + bias_one).astype(jnp.bfloat16)
    active, slope = up_project(first_low, w_up, b_up)
    hidden_two = first_low.astype(jnp.float32) + dot_nn(active, w_down) + b_down
    normed_two, inverse_two = norm_parts(hidden_two)
    second_low = (normed_two * gain_two + bias_two).astype(jnp.bfloat16)
    project = dot_nn(second_low, w_proj)
    inv_norm = lax.rsqrt(jnp.sum(project * project, axis=-1, keepdims=True) + 1e-06)
    embedded = (project * inv_norm * valid).astype(jnp.bfloat16)

    grad_emb = dealt_cot.astype(jnp.float32) * valid
    along = jnp.sum(project * grad_emb, axis=-1, keepdims=True)
    grad_project = (inv_norm * grad_emb - inv_norm * inv_norm * inv_norm * along * project).astype(
        jnp.bfloat16
    )
    grad_w_proj = dot_tn(second_low, grad_project).astype(jnp.bfloat16)
    grad_second = dot_nt(grad_project, w_proj)
    grad_gain_two = jnp.sum(grad_second * normed_two, axis=0)
    grad_bias_two = jnp.sum(grad_second, axis=0)
    grad_hidden_two = norm_back(grad_second, normed_two, inverse_two, gain_two)
    grad_b_down = jnp.sum(grad_hidden_two, axis=0)
    down_low = grad_hidden_two.astype(jnp.bfloat16)
    grad_w_down = dot_tn(active, down_low).astype(jnp.bfloat16)
    grad_up = dot_nt(down_low, w_down) * slope.astype(jnp.float32)
    grad_b_up = jnp.sum(grad_up, axis=0)
    up_low = grad_up.astype(jnp.bfloat16)
    grad_w_up = dot_tn(first_low, up_low).astype(jnp.bfloat16)
    grad_first = grad_hidden_two + dot_nt(up_low, w_up)
    grad_gain_one = jnp.sum(grad_first * normed_one, axis=0)
    grad_bias_one = jnp.sum(grad_first, axis=0)
    grad_hidden_one = norm_back(grad_first, normed_one, inverse_one, gain_one)
    grad_b_out = jnp.sum(grad_hidden_one, axis=0)
    out_low = grad_hidden_one.astype(jnp.bfloat16)
    grad_w_out = dot_tn(context, out_low).astype(jnp.bfloat16)
    grad_context = dot_nt(out_low, w_out).astype(jnp.bfloat16)
    grad_three, sums = attend_back(qkv, grad_context, lengths)
    sums = jnp.sum(sums, axis=0)[:, 0]
    grad_b_qv = jnp.concatenate([sums[0], sums[2]])
    grad_qkv = jnp.concatenate([grad_three[0], grad_three[1], grad_three[2]], axis=1)
    grad_w_qkv = dot_tn(dealt, grad_qkv).astype(jnp.bfloat16)
    grad_dealt = (dot_nt(grad_qkv, w_qkv) + grad_hidden_one).astype(jnp.bfloat16)

    inverse_row = (
        jnp.zeros((row_count,), jnp.int32).at[local_row].set(jnp.arange(row_count, dtype=jnp.int32))
    )
    back = jnp.concatenate([grad_dealt, embedded], axis=1)[inverse_row]
    returned = lax.all_to_all(back, AXIS, split_axis=0, concat_axis=0, tiled=True)
    shards, small = scatter_grads(
        [grad_w_qkv, grad_w_out, grad_w_up, grad_w_down, grad_w_proj],
        [
            grad_b_qv,
            grad_b_out,
            grad_gain_one,
            grad_bias_one,
            grad_b_up,
            grad_b_down,
            grad_gain_two,
            grad_bias_two,
        ],
        ring,
        devices,
    )
    return (
        returned[:, model_width:],
        returned[:, :model_width],
        shards[0],
        small[0],
        shards[1],
        small[1],
        small[2],
        small[3],
        shards[2],
        small[4],
        shards[3],
        small[5],
        small[6],
        small[7],
        shards[4],
    )


def solution(mesh):
    matrix, vector = P(AXIS, None), P(AXIS)
    params = "mvmvvvmvmvvvm"
    in_kinds = "mmvv" + params
    out_kinds = "mm" + params
    specs = {"m": matrix, "v": vector}
    return jax.shard_map(
        local,
        mesh=mesh,
        in_specs=tuple(specs[kind] for kind in in_kinds),
        out_specs=tuple(specs[kind] for kind in out_kinds),
        check_vma=False,
    )
```

```python
from functools import partial

import jax
import jax.numpy as jnp
from jax import lax
from jax.experimental import pallas as pl
from jax.experimental.pallas import tpu as pltpu
from jax.sharding import PartitionSpec as P

HEADS = 12
HEAD_DIM = 64
AXIS = "fsdp"
MESH_ID = pl.DeviceIdType.MESH
VMEM_SPEC = pl.BlockSpec(memory_space=pltpu.VMEM)
ANY_SPEC = pl.BlockSpec(memory_space=pl.ANY)
VMEM_LIMIT = 60 * 1024 * 1024


def chain_edges(node, ring, lean_up):
    up_count = ring // 2 if lean_up else (ring - 1) // 2
    edges = []
    here = node
    for _ in range(up_count):
        there = ((here[0] + 1) % ring,) + here[1:]
        edges.append((here, there, "up"))
        here = there
    here = node
    for _ in range(ring - 1 - up_count):
        there = ((here[0] - 1) % ring,) + here[1:]
        edges.append((here, there, "down"))
        here = there
    return edges


def plane_edges(node, x_first):
    z = node[0]
    own, by_x, by_y, both = (z, 0, 0, 0), (z, 0, 1, 0), (z, 1, 0, 0), (z, 1, 1, 0)
    edges = [(own, by_x, "x"), (own, by_y, "y")]
    edges.append((by_x, both, "y") if x_first else (by_y, both, "x"))
    return edges


def make_tree(ring, ring_first, flip):
    root = (0, 0, 0, 0)
    edges = []
    if ring_first:
        edges += chain_edges(root, ring, flip)
        nodes = [root] + [edge[1] for edge in edges]
        for place, node in enumerate(nodes):
            edges += plane_edges(node, (place % 2 == 0) != flip)
    else:
        edges += plane_edges(root, flip)
        nodes = [root] + [edge[1] for edge in edges]
        for place, node in enumerate(nodes):
            edges += chain_edges(node, ring, (place % 2 == 0) != flip)
    nodes = [root] + [edge[1] for edge in edges]
    edges += [(node, node[:3] + (1,), "core") for node in nodes]
    depth = {root: 0}
    for parent, child, _ in edges:
        depth[child] = depth[parent] + 1
    order = sorted(range(len(edges)), key=lambda index: depth[edges[index][1]])
    return [edges[index] + (depth[edges[index][1]],) for index in order]


class Place:
    def __init__(self, ring):
        me = lax.axis_index(AXIS)
        self.ring = ring
        self.me = me
        self.core = lax.rem(me, 2)
        self.x = lax.rem(me // 2, 2)
        self.y = lax.rem(me // 4, 2)
        self.z = me // 8

    @staticmethod
    def flip(value, amount):
        return 1 - value if amount else value

    def chip_of(self, offset):
        z = lax.rem(self.z + (self.ring - offset[0]) % self.ring, self.ring)
        return (z * 2 + self.flip(self.y, offset[1])) * 2 + self.flip(self.x, offset[2])

    def unit_of(self, offset):
        return self.chip_of(offset) * 2 + self.flip(self.core, offset[3])

    def neighbour(self, way, back=False):
        step = {"up": (1, 0, 0, 0), "down": (-1, 0, 0, 0), "x": (0, 0, 1, 0)}
        step.update({"y": (0, 1, 0, 0), "core": (0, 0, 0, 1)})
        offset = step[way]
        dz = offset[0] if back else -offset[0]
        return self.unit_of((dz % self.ring,) + offset[1:])


def enter(place):
    barrier = pltpu.get_barrier_semaphore()
    for way in ("up", "down", "x", "y", "core"):
        pl.semaphore_signal(
            barrier, inc=1, device_id=(place.neighbour(way),), device_id_type=MESH_ID
        )
    pl.semaphore_wait(barrier, 5)


def gather_kernel(ring, plan, *refs):
    arrays = len(plan["shapes"])
    shards, outs = refs[:arrays], refs[arrays : 2 * arrays]
    recv_sem, send_sem, local_sem = refs[2 * arrays :]
    place = Place(ring)
    parts = plan["parts"]

    def window(ref, part):
        _, first, count, _ = parts[part]
        return ref if count is None else ref.at[:, pl.ds(first, count)]

    def copy(part, index):
        array, _, _, tree = parts[part]
        parent, _, way, _ = tree[index]
        unit = place.unit_of(parent)
        source = shards[array] if parent == (0, 0, 0, 0) else outs[array].at[unit]
        return pltpu.make_async_remote_copy(
            src_ref=window(source, part),
            dst_ref=window(outs[array].at[unit], part),
            send_sem=send_sem.at[part],
            recv_sem=recv_sem.at[part, index],
            device_id=(place.neighbour(way),),
            device_id_type=MESH_ID,
        )

    def arrived(part, index):
        array, _, _, tree = parts[part]
        _, child, way, _ = tree[index]
        landed = window(outs[array].at[place.unit_of(child)], part)
        pltpu.make_async_remote_copy(
            src_ref=landed,
            dst_ref=landed,
            send_sem=send_sem.at[part],
            recv_sem=recv_sem.at[part, index],
            device_id=(place.neighbour(way),),
            device_id_type=MESH_ID,
        ).wait_recv()

    def send_from(part, node):
        for index, edge in enumerate(parts[part][3]):
            if edge[0] == node:
                copy(part, index).start()

    own_copies = [
        pltpu.make_async_copy(shards[array], outs[array].at[place.me], local_sem.at[array])
        for array in range(arrays)
    ]
    for own_copy in own_copies:
        own_copy.start()
    enter(place)
    for part in range(len(parts)):
        send_from(part, (0, 0, 0, 0))
    deepest = max(edge[3] for part in parts for edge in part[3])
    for depth in range(1, deepest + 1):
        for part in range(len(parts)):
            for index, edge in enumerate(parts[part][3]):
                if edge[3] == depth and edge[2] != "core":
                    arrived(part, index)
                    send_from(part, edge[1])
    for part in range(len(parts)):
        for index, edge in enumerate(parts[part][3]):
            if edge[2] == "core":
                arrived(part, index)
    for own_copy in own_copies:
        own_copy.wait()
    for part, (array, first, count, tree) in enumerate(parts):
        whole = outs[array].at[pl.ds(0, len(tree))]
        if count is not None:
            whole = whole.at[:, :, pl.ds(first, count)]
        pltpu.make_async_copy(whole, whole, send_sem.at[part]).wait()


def gather_units(shards, plan, ring):
    devices = ring * 8
    edges = devices - 1
    return pl.pallas_call(
        partial(gather_kernel, ring, plan),
        out_shape=[
            jax.ShapeDtypeStruct((devices,) + shard.shape, shard.dtype) for shard in shards
        ],
        in_specs=[VMEM_SPEC] * len(shards),
        out_specs=[ANY_SPEC] * len(shards),
        scratch_shapes=[
            pltpu.SemaphoreType.DMA((len(plan["parts"]), edges)),
            pltpu.SemaphoreType.DMA((len(plan["parts"]),)),
            pltpu.SemaphoreType.DMA((len(shards),)),
        ],
        compiler_params=pltpu.CompilerParams(collective_id=0, has_side_effects=True),
        name="gather_units",
    )(*shards)


def scatter_kernel(ring, plan, *refs):
    shapes = plan["shapes"]
    arrays = len(shapes)
    parts = plan["parts"]
    grads, outs = refs[:arrays], refs[arrays : 2 * arrays]
    owns = refs[2 * arrays : 3 * arrays]
    lands = refs[3 * arrays : 3 * arrays + len(parts)]
    recv_sem, send_sem, local_sem = refs[3 * arrays + len(parts) :]
    place = Place(ring)

    def window(ref, part):
        _, first, count, _ = parts[part]
        return ref if count is None else ref.at[:, pl.ds(first, count)]

    def copy(part, index, source):
        way = parts[part][3][index][2]
        return pltpu.make_async_remote_copy(
            src_ref=source,
            dst_ref=lands[part].at[index],
            send_sem=send_sem.at[part],
            recv_sem=recv_sem.at[part, index],
            device_id=(place.neighbour(way, back=True),),
            device_id_type=MESH_ID,
        )

    own_copies = [
        pltpu.make_async_copy(grads[array].at[:, place.core], owns[array], local_sem.at[array])
        for array in range(arrays)
    ]
    for own_copy in own_copies:
        own_copy.start()
    enter(place)
    deepest = max(edge[3] for part in parts for edge in part[3])
    for depth in range(deepest, 0, -1):
        for part, (array, _, _, tree) in enumerate(parts):
            for index, (_, child, way, level) in enumerate(tree):
                if way == "core" and level == depth:
                    chip = place.chip_of(child)
                    source = grads[array].at[chip, place.flip(place.core, 1)]
                    copy(part, index, window(source, part)).start()
    for own_copy in own_copies:
        own_copy.wait()

    def add_up(part, node, target):
        array, first, count, tree = parts[part]
        children = [index for index, edge in enumerate(tree) if edge[0] == node]
        for index in children:
            copy(part, index, lands[part].at[index]).wait_recv()
        chip = place.chip_of(node)
        rows, columns = shapes[array]
        if count is not None:
            columns = count
        step = columns
        while rows * step > 24 * 768 and step % 256 == 0:
            step //= 2
        own = owns[array]

        def body(block, carry):
            here = pl.ds(pl.multiple_of(block * step, 128), step)
            where = pl.ds(pl.multiple_of(first + block * step, 128), step)
            total = own[chip, :, where].astype(jnp.float32)
            for index in children:
                total = total + lands[part][index, :, here].astype(jnp.float32)
            if target is None:
                own[chip, :, where] = total.astype(own.dtype)
            else:
                target[:, where] = total
            return carry

        lax.fori_loop(0, columns // step, body, 0)
        return window(own.at[chip], part)

    waiting = None
    for depth in range(deepest, 0, -1):
        for part in range(len(parts)):
            for index, (_, child, way, level) in enumerate(parts[part][3]):
                if way != "core" and level == depth:
                    ready = copy(part, index, add_up(part, child, None))
                    if waiting is not None:
                        waiting.start()
                    waiting = ready
    waiting.start()
    for part in range(len(parts)):
        add_up(part, (0, 0, 0, 0), outs[parts[part][0]])
    for part in range(len(parts)):
        pltpu.make_async_copy(lands[part], lands[part], send_sem.at[part]).wait()


def scatter_units(grads, plan, ring):
    devices = ring * 8
    edges = devices - 1
    shapes = plan["shapes"]
    lands = []
    for array, _, count, _ in plan["parts"]:
        rows, columns = shapes[array]
        lands.append(
            pltpu.VMEM((edges, rows, columns if count is None else count), jnp.bfloat16)
        )
    return pl.pallas_call(
        partial(scatter_kernel, ring, plan),
        out_shape=[jax.ShapeDtypeStruct(shape, jnp.float32) for shape in shapes],
        in_specs=[ANY_SPEC] * len(shapes),
        out_specs=[VMEM_SPEC] * len(shapes),
        scratch_shapes=[pltpu.VMEM((devices // 2,) + shape, jnp.bfloat16) for shape in shapes]
        + lands
        + [
            pltpu.SemaphoreType.DMA((len(plan["parts"]), edges)),
            pltpu.SemaphoreType.DMA((len(plan["parts"]),)),
            pltpu.SemaphoreType.DMA((len(shapes),)),
        ],
        compiler_params=pltpu.CompilerParams(
            collective_id=1, has_side_effects=True, vmem_limit_bytes=VMEM_LIMIT
        ),
        name="scatter_units",
    )(*[grad.reshape((devices // 2, 2) + shape) for grad, shape in zip(grads, shapes)])


def make_plan(shapes, ring):
    trees = [make_tree(ring, first, flip) for first in (True, False) for flip in (False, True)]
    parts = []
    for array, (_, columns) in enumerate(shapes):
        flip = array % 2
        late = columns // 512 * 128 if columns > 768 else 0
        if shapes[array][0] > 32:
            late = columns // 3
        if late:
            parts.append((array, 0, columns - late, trees[flip]))
            parts.append((array, columns - late, late, trees[2 + flip]))
        else:
            parts.append((array, 0, None, trees[flip]))
    return {"shapes": shapes, "parts": parts}


def dot_nt(left, right):
    return lax.dot_general(
        left, right, (((1,), (1,)), ((), ())), preferred_element_type=jnp.float32
    )


def dot_tn(left, right):
    return lax.dot_general(
        left, right, (((0,), (0,)), ((), ())), preferred_element_type=jnp.float32
    )


def dot_nn(left, right):
    return jnp.dot(left, right, preferred_element_type=jnp.float32)


def attend_kernel(lengths_ref, q_ref, k_ref, v_ref, context_ref, log_ref):
    rows, width = q_ref.shape
    length = lengths_ref[pl.program_id(0)]
    lane = lax.broadcasted_iota(jnp.int32, (rows, width), 1)
    inside = lax.broadcasted_iota(jnp.int32, (rows, width), 0) < length
    bias = jnp.where(lax.broadcasted_iota(jnp.int32, (1, rows), 1) < length, 0.0, -1e30)
    queries, keys, values = q_ref[...] * 0.125, k_ref[...], v_ref[...]
    context = jnp.zeros((rows, width), jnp.float32)
    logs = context
    for head in range(width // HEAD_DIM):
        mine = lane // HEAD_DIM == head
        scores = dot_nt(jnp.where(mine, queries, jnp.zeros_like(queries)), keys) + bias
        top = jnp.max(scores, axis=-1, keepdims=True)
        weights = jnp.exp(scores - top).astype(jnp.bfloat16)
        sums = dot_nn(weights, jnp.where(mine, values, jnp.ones_like(values)))
        other = (width - 1) if head == 0 else 0
        total = sums[:, other : other + 1]
        context = jnp.where(mine, sums * (1.0 / total), context)
        logs = jnp.where(mine, top + jnp.log(total), logs)
    context_ref[...] = jnp.where(inside, context, values.astype(jnp.float32)).astype(
        context_ref.dtype
    )
    log_ref[...] = logs


def attend(qkv, lengths):
    rows, width3 = qkv.shape
    width = width3 // 3
    halves = lengths.shape[0]
    half = rows // halves
    pairs = width // 128

    def columns(which):
        return pl.BlockSpec((half, 128), lambda i, j, l: (i, which * pairs + j))

    return pl.pallas_call(
        attend_kernel,
        out_shape=[
            jax.ShapeDtypeStruct((rows, width), jnp.bfloat16),
            jax.ShapeDtypeStruct((rows, width), jnp.float32),
        ],
        grid_spec=pltpu.PrefetchScalarGridSpec(
            num_scalar_prefetch=1,
            grid=(halves, pairs),
            in_specs=[columns(0), columns(1), columns(2)],
            out_specs=[columns(0), columns(0)],
        ),
        compiler_params=pltpu.CompilerParams(vmem_limit_bytes=VMEM_LIMIT),
        name="attend",
    )(lengths, qkv, qkv, qkv)


def attend_back_kernel(
    lengths_ref, q_ref, k_ref, v_ref, context_ref, log_ref, g_ref, grad_ref, sums_ref
):
    rows, width = q_ref.shape
    heads = width // HEAD_DIM
    length = lengths_ref[pl.program_id(0)]
    lane = lax.broadcasted_iota(jnp.int32, (rows, width), 1)
    inside = lax.broadcasted_iota(jnp.int32, (rows, width), 0) < length
    bias = jnp.where(lax.broadcasted_iota(jnp.int32, (rows, 1), 0) < length, 0.0, -1e30)
    queries, keys, values = q_ref[...] * 0.125, k_ref[...], v_ref[...]
    keys_scaled = keys * 0.125
    zero = jnp.zeros_like(queries)
    grads = jnp.where(inside, g_ref[...], zero)
    product = grads.astype(jnp.float32) * context_ref[...].astype(jnp.float32)
    table = jnp.zeros((rows, width), jnp.float32)
    for head in range(heads):
        mine = lane // HEAD_DIM == head
        along = jnp.sum(jnp.where(mine, product, 0.0), axis=-1, keepdims=True)
        first = head * HEAD_DIM
        table = jnp.where(lane == head, log_ref[:, first : first + 1], table)
        table = jnp.where(lane == heads + head, along, table)
    table = jnp.transpose(table)
    grad_q = jnp.zeros((rows, width), jnp.float32)
    grad_k = grad_q
    grad_v = jnp.where(inside, 0.0, g_ref[...].astype(jnp.float32))
    for head in range(heads):
        mine = lane // HEAD_DIM == head
        queries_head = jnp.where(mine, queries, zero)
        grads_head = jnp.where(mine, grads, zero)
        scores = dot_nt(keys, queries_head) + bias
        probs = jnp.exp(scores - table[head : head + 1])
        grad_v = grad_v + dot_nn(probs.astype(jnp.bfloat16), grads_head)
        grad_probs = dot_nt(values, grads_head)
        grad_scores = (probs * (grad_probs - table[heads + head : heads + head + 1])).astype(
            jnp.bfloat16
        )
        grad_k = grad_k + dot_nn(grad_scores, queries_head)
        grad_q = grad_q + dot_tn(grad_scores, jnp.where(mine, keys_scaled, zero))
    for place, grad in enumerate((grad_q, grad_k, grad_v)):
        grad_ref[place] = grad.astype(grad_ref.dtype)
        sums_ref[0, place] = jnp.sum(grad, axis=0, keepdims=True)


def attend_back(qkv, context, logs, grad_context, lengths):
    rows, width3 = qkv.shape
    width = width3 // 3
    halves = lengths.shape[0]
    half = rows // halves
    pairs = width // 128

    def columns(which):
        return pl.BlockSpec((half, 128), lambda i, j, l: (i, which * pairs + j))

    return pl.pallas_call(
        attend_back_kernel,
        out_shape=[
            jax.ShapeDtypeStruct((3, rows, width), jnp.bfloat16),
            jax.ShapeDtypeStruct((halves, 3, 1, width), jnp.float32),
        ],
        grid_spec=pltpu.PrefetchScalarGridSpec(
            num_scalar_prefetch=1,
            grid=(halves, pairs),
            in_specs=[columns(0), columns(1), columns(2)] + [columns(0)] * 3,
            out_specs=[
                pl.BlockSpec((3, half, 128), lambda i, j, l: (0, i, j)),
                pl.BlockSpec((1, 3, 1, 128), lambda i, j, l: (i, 0, 0, j)),
            ],
        ),
        compiler_params=pltpu.CompilerParams(vmem_limit_bytes=VMEM_LIMIT),
        name="attend_back",
    )(lengths, qkv, qkv, qkv, context, logs, grad_context)


ERFC_TERMS = (
    0.17087277,
    -0.82215223,
    1.48851587,
    -1.13520398,
    0.27886807,
    -0.18628806,
    0.09678418,
    0.37409196,
    1.00002368,
    -1.26551223,
)


LOG2_E = 1.4426950408889634


def gelu_parts(u):
    under = 1.0 + jnp.abs(u) * (0.5 * 0.7071067811865476)
    t = pl.reciprocal(under, approx=True)
    t = t * (2.0 - under * t)
    square = u * u * (-0.5 * LOG2_E)
    poly = ERFC_TERMS[0] * LOG2_E
    for term in ERFC_TERMS[1:-1]:
        poly = poly * t + term * LOG2_E
    poly = poly * t + (ERFC_TERMS[-1] - 0.6931471805599453) * LOG2_E
    tail = t * jnp.exp2(poly + square)
    cdf = jnp.where(u < 0, tail, 1.0 - tail)
    return u * cdf, cdf + u * (jnp.exp2(square) * 0.3989422804014327)


def up_kernel(first_ref, w_ref, b_ref, active_ref, slope_ref):
    rows = first_ref.shape[0]
    step = 128
    for start in range(0, rows, step):
        where = pl.ds(start, step)
        u = dot_nn(first_ref[where, :], w_ref[...]) + b_ref[...]
        value, slope = gelu_parts(u)
        active_ref[where, :] = value.astype(active_ref.dtype)
        slope_ref[where, :] = slope.astype(slope_ref.dtype)


def up_project(first_low, w_up, b_up):
    rows, width = first_low.shape
    hidden = w_up.shape[1]
    block = 512
    return pl.pallas_call(
        up_kernel,
        out_shape=[jax.ShapeDtypeStruct((rows, hidden), jnp.bfloat16)] * 2,
        grid=(hidden // block,),
        in_specs=[
            pl.BlockSpec((rows, width), lambda j: (0, 0)),
            pl.BlockSpec((width, block), lambda j: (0, j)),
            pl.BlockSpec((1, block), lambda j: (0, j)),
        ],
        out_specs=[pl.BlockSpec((rows, block), lambda j: (0, j))] * 2,
        compiler_params=pltpu.CompilerParams(vmem_limit_bytes=VMEM_LIMIT),
        name="up_project",
    )(first_low, w_up, b_up.reshape(1, hidden))


def norm_parts(hidden):
    center = hidden - jnp.mean(hidden, axis=-1, keepdims=True)
    inverse = lax.rsqrt(jnp.mean(center * center, axis=-1, keepdims=True) + 1e-12)
    return (center * inverse, inverse)


def norm_back(grad_out, normed, inverse, gain):
    scaled = grad_out * gain
    centered = scaled - jnp.mean(scaled, axis=-1, keepdims=True)
    return inverse * (centered - normed * jnp.mean(scaled * normed, axis=-1, keepdims=True))


def order_rows(slots, lengths):
    count = slots.shape[0]
    half = count // 2
    row = jnp.arange(count, dtype=jnp.int32)
    first, second = lengths[0], lengths[1]
    twice = jnp.concatenate([slots, slots])
    hole = lax.dynamic_slice_in_dim(twice, second, count)
    later = lax.dynamic_slice_in_dim(twice, first + half, count)
    in_first, in_second = row < first, row - half < second
    inside = jnp.where(row < half, in_first, in_second)
    placed = jnp.where(
        row < half, jnp.where(in_first, slots, hole), jnp.where(in_second, later, slots)
    )
    return placed, inside


def gather_params(params, ring):
    (w_qkv, b_qv, w_out, b_out, g1, c1, w_up, b_up, w_down, b_down, g2, c2, w_proj) = params
    small = [b_qv, b_out, g1, c1, b_up, b_down, g2, c2]
    sizes = [entry.shape[0] for entry in small]
    if ring is None:
        whole = [lax.all_gather(w, AXIS, axis=0, tiled=True) for w in (w_qkv, w_out, w_up, w_down)]
        proj = lax.all_gather(w_proj, AXIS, axis=0, tiled=True)
        few = lax.all_gather(jnp.concatenate(small), AXIS, axis=0)
    else:
        packed = jnp.concatenate(small)
        packed = jnp.pad(packed, (0, 1024 - packed.shape[0])).reshape(8, 128)
        shards = [w_qkv, w_out, w_up, w_down, jnp.concatenate([w_proj, packed], axis=0)]
        plan = make_plan([shard.shape for shard in shards], ring)
        units = gather_units(shards, plan, ring)
        whole = [unit.reshape(-1, unit.shape[2]) for unit in units[:4]]
        rows = w_proj.shape[0]
        proj = units[4][:, :rows].reshape(-1, w_proj.shape[1])
        few = units[4][:, rows:].reshape(units[4].shape[0], -1)
    vectors = []
    start = 0
    for size in sizes:
        vectors.append(few[:, start : start + size].reshape(-1).astype(jnp.float32))
        start += size
    return whole + [proj], vectors


def scatter_grads(weights, vectors, ring, devices):
    few = [vector.reshape(devices, -1) for vector in vectors]
    sizes = [entry.shape[1] for entry in few]
    few = jnp.concatenate(few, axis=1)
    if ring is None:
        shards = [
            lax.psum_scatter(w, AXIS, scatter_dimension=0, tiled=True).astype(jnp.float32)
            for w in weights
        ]
        small = lax.psum_scatter(few.reshape(-1), AXIS, scatter_dimension=0, tiled=True)
    else:
        few = jnp.pad(few, ((0, 0), (0, 1024 - few.shape[1]))).astype(jnp.bfloat16)
        units = [w.reshape(devices, -1, w.shape[1]) for w in weights]
        rows = units[4].shape[1]
        units[4] = jnp.concatenate([units[4], few.reshape(devices, 8, 128)], axis=1)
        plan = make_plan([unit.shape[1:] for unit in units], ring)
        shards = list(scatter_units(units, plan, ring))
        small = shards[4][rows:].reshape(-1)
        shards[4] = shards[4][:rows]
    pieces = []
    start = 0
    for size in sizes:
        pieces.append(small[start : start + size])
        start += size
    return shards, pieces


def local(tokens, cotangent, slot_row, lengths, *params):
    devices = lax.axis_size(AXIS)
    row_count, model_width = tokens.shape
    peer_rows = row_count // devices
    ring = devices // 8 if params[0].shape[0] % 8 == 0 and devices % 8 == 0 else None
    (w_qkv, w_out, w_up, w_down, w_proj), vectors = gather_params(params, ring)
    b_qv, b_out, gain_one, bias_one, b_up, b_down, gain_two, bias_two = vectors

    local_row, inside = order_rows(
        slot_row // row_count * peer_rows + slot_row % peer_rows, lengths
    )
    both = jnp.concatenate([tokens, cotangent], axis=1)
    arrived = lax.all_to_all(both, AXIS, split_axis=0, concat_axis=0, tiled=True)
    chosen = local_row[:, None] == jnp.arange(row_count, dtype=jnp.int32)[None, :]
    chosen = chosen.astype(jnp.bfloat16)
    dealt = dot_nn(chosen, arrived[:, :model_width]).astype(jnp.bfloat16)
    dealt_cot = dot_nn(chosen, arrived[:, model_width:]).astype(jnp.bfloat16)
    valid = inside[:, None].astype(jnp.float32)

    bias_all = jnp.concatenate(
        [b_qv[:model_width], jnp.zeros((model_width,), jnp.float32), b_qv[model_width:]]
    )
    qkv = (dot_nn(dealt, w_qkv) + bias_all).astype(jnp.bfloat16)
    context, logs = attend(qkv, lengths)
    hidden_one = dealt.astype(jnp.float32) + dot_nn(context, w_out) + b_out
    normed_one, inverse_one = norm_parts(hidden_one)
    first_low = (normed_one * gain_one + bias_one).astype(jnp.bfloat16)
    active, slope = up_project(first_low, w_up, b_up)
    hidden_two = first_low.astype(jnp.float32) + dot_nn(active, w_down) + b_down
    normed_two, inverse_two = norm_parts(hidden_two)
    second_low = (normed_two * gain_two + bias_two).astype(jnp.bfloat16)
    project = dot_nn(second_low, w_proj)
    inv_norm = lax.rsqrt(jnp.sum(project * project, axis=-1, keepdims=True) + 1e-06)
    embedded = (project * inv_norm * valid).astype(jnp.bfloat16)

    grad_emb = dealt_cot.astype(jnp.float32) * valid
    along = jnp.sum(project * grad_emb, axis=-1, keepdims=True)
    grad_project = (inv_norm * grad_emb - inv_norm * inv_norm * inv_norm * along * project).astype(
        jnp.bfloat16
    )
    grad_w_proj = dot_tn(second_low, grad_project).astype(jnp.bfloat16)
    grad_second = dot_nt(grad_project, w_proj)
    grad_gain_two = jnp.sum(grad_second * normed_two, axis=0)
    grad_bias_two = jnp.sum(grad_second, axis=0)
    grad_hidden_two = norm_back(grad_second, normed_two, inverse_two, gain_two)
    grad_b_down = jnp.sum(grad_hidden_two, axis=0)
    down_low = grad_hidden_two.astype(jnp.bfloat16)
    grad_w_down = dot_tn(active, down_low).astype(jnp.bfloat16)
    grad_up = dot_nt(down_low, w_down) * slope.astype(jnp.float32)
    grad_b_up = jnp.sum(grad_up, axis=0)
    up_low = grad_up.astype(jnp.bfloat16)
    grad_w_up = dot_tn(first_low, up_low).astype(jnp.bfloat16)
    grad_first = grad_hidden_two + dot_nt(up_low, w_up)
    grad_gain_one = jnp.sum(grad_first * normed_one, axis=0)
    grad_bias_one = jnp.sum(grad_first, axis=0)
    grad_hidden_one = norm_back(grad_first, normed_one, inverse_one, gain_one)
    grad_b_out = jnp.sum(grad_hidden_one, axis=0)
    out_low = grad_hidden_one.astype(jnp.bfloat16)
    grad_w_out = dot_tn(context, out_low).astype(jnp.bfloat16)
    grad_context = dot_nt(out_low, w_out).astype(jnp.bfloat16)
    grad_three, sums = attend_back(qkv, context, logs, grad_context, lengths)
    sums = jnp.sum(sums, axis=0)[:, 0]
    grad_b_qv = jnp.concatenate([sums[0], sums[2]])
    grad_qkv = jnp.concatenate([grad_three[0], grad_three[1], grad_three[2]], axis=1)
    grad_w_qkv = dot_tn(dealt, grad_qkv).astype(jnp.bfloat16)
    grad_dealt = (dot_nt(grad_qkv, w_qkv) + grad_hidden_one).astype(jnp.bfloat16)

    back = jnp.concatenate([grad_dealt, embedded], axis=1)
    back = dot_tn(chosen, back).astype(jnp.bfloat16)
    returned = lax.all_to_all(back, AXIS, split_axis=0, concat_axis=0, tiled=True)
    shards, small = scatter_grads(
        [grad_w_qkv, grad_w_out, grad_w_up, grad_w_down, grad_w_proj],
        [
            grad_b_qv,
            grad_b_out,
            grad_gain_one,
            grad_bias_one,
            grad_b_up,
            grad_b_down,
            grad_gain_two,
            grad_bias_two,
        ],
        ring,
        devices,
    )
    return (
        returned[:, model_width:],
        returned[:, :model_width],
        shards[0],
        small[0],
        shards[1],
        small[1],
        small[2],
        small[3],
        shards[2],
        small[4],
        shards[3],
        small[5],
        small[6],
        small[7],
        shards[4],
    )


def solution(mesh):
    matrix, vector = P(AXIS, None), P(AXIS)
    params = "mvmvvvmvmvvvm"
    in_kinds = "mmvv" + params
    out_kinds = "mm" + params
    specs = {"m": matrix, "v": vector}
    return jax.shard_map(
        local,
        mesh=mesh,
        in_specs=tuple(specs[kind] for kind in in_kinds),
        out_specs=tuple(specs[kind] for kind in out_kinds),
        check_vma=False,
    )
```

```python
from functools import partial

import jax
import jax.numpy as jnp
from jax import lax
from jax.experimental import pallas as pl
from jax.experimental.pallas import tpu as pltpu
from jax.sharding import PartitionSpec as P


HEAD_DIM = 64
AXIS = "fsdp"
MESH_ID = pl.DeviceIdType.MESH
VMEM_SPEC = pl.BlockSpec(memory_space=pltpu.VMEM)
ANY_SPEC = pl.BlockSpec(memory_space=pl.ANY)
VMEM_LIMIT = 60 * 1024 * 1024


def chain_edges(node, ring, lean_up):
    up_count = ring // 2 if lean_up else (ring - 1) // 2
    edges = []
    here = node
    for _ in range(up_count):
        there = ((here[0] + 1) % ring,) + here[1:]
        edges.append((here, there, "up"))
        here = there
    here = node
    for _ in range(ring - 1 - up_count):
        there = ((here[0] - 1) % ring,) + here[1:]
        edges.append((here, there, "down"))
        here = there
    return edges


def plane_edges(node, x_first):
    z = node[0]
    own, by_x, by_y, both = (z, 0, 0, 0), (z, 0, 1, 0), (z, 1, 0, 0), (z, 1, 1, 0)
    edges = [(own, by_x, "x"), (own, by_y, "y")]
    edges.append((by_x, both, "y") if x_first else (by_y, both, "x"))
    return edges


def make_tree(ring, ring_first, flip):
    root = (0, 0, 0, 0)
    edges = []
    if ring_first:
        edges += chain_edges(root, ring, flip)
        nodes = [root] + [edge[1] for edge in edges]
        for place, node in enumerate(nodes):
            edges += plane_edges(node, (place % 2 == 0) != flip)
    else:
        edges += plane_edges(root, flip)
        nodes = [root] + [edge[1] for edge in edges]
        for place, node in enumerate(nodes):
            edges += chain_edges(node, ring, (place % 2 == 0) != flip)
    nodes = [root] + [edge[1] for edge in edges]
    edges += [(node, node[:3] + (1,), "core") for node in nodes]
    depth = {root: 0}
    for parent, child, _ in edges:
        depth[child] = depth[parent] + 1
    order = sorted(range(len(edges)), key=lambda index: depth[edges[index][1]])
    return [edges[index] + (depth[edges[index][1]],) for index in order]


class Place:
    def __init__(self, ring):
        me = lax.axis_index(AXIS)
        self.ring = ring
        self.me = me
        self.core = lax.rem(me, 2)
        self.x = lax.rem(me // 2, 2)
        self.y = lax.rem(me // 4, 2)
        self.z = me // 8

    @staticmethod
    def flip(value, amount):
        return 1 - value if amount else value

    def chip_of(self, offset):
        z = lax.rem(self.z + (self.ring - offset[0]) % self.ring, self.ring)
        return (z * 2 + self.flip(self.y, offset[1])) * 2 + self.flip(self.x, offset[2])

    def unit_of(self, offset):
        return self.chip_of(offset) * 2 + self.flip(self.core, offset[3])

    def neighbour(self, way, back=False):
        step = {"up": (1, 0, 0, 0), "down": (-1, 0, 0, 0), "x": (0, 0, 1, 0)}
        step.update({"y": (0, 1, 0, 0), "core": (0, 0, 0, 1)})
        offset = step[way]
        dz = offset[0] if back else -offset[0]
        return self.unit_of((dz % self.ring,) + offset[1:])


def enter(place):
    barrier = pltpu.get_barrier_semaphore()
    for way in ("up", "down", "x", "y", "core"):
        pl.semaphore_signal(
            barrier, inc=1, device_id=(place.neighbour(way),), device_id_type=MESH_ID
        )
    pl.semaphore_wait(barrier, 5)


def gather_kernel(ring, plan, *refs):
    arrays = len(plan["shapes"])
    shards, outs = refs[:arrays], refs[arrays : 2 * arrays]
    recv_sem, send_sem, local_sem = refs[2 * arrays :]
    place = Place(ring)
    parts = plan["parts"]

    def window(ref, part):
        _, first, count, _ = parts[part]
        return ref if count is None else ref.at[:, pl.ds(first, count)]

    def copy(part, index):
        array, _, _, tree = parts[part]
        parent, _, way, _ = tree[index]
        unit = place.unit_of(parent)
        source = shards[array] if parent == (0, 0, 0, 0) else outs[array].at[unit]
        return pltpu.make_async_remote_copy(
            src_ref=window(source, part),
            dst_ref=window(outs[array].at[unit], part),
            send_sem=send_sem.at[part],
            recv_sem=recv_sem.at[part, index],
            device_id=(place.neighbour(way),),
            device_id_type=MESH_ID,
        )

    def arrived(part, index):
        array, _, _, tree = parts[part]
        _, child, way, _ = tree[index]
        landed = window(outs[array].at[place.unit_of(child)], part)
        pltpu.make_async_remote_copy(
            src_ref=landed,
            dst_ref=landed,
            send_sem=send_sem.at[part],
            recv_sem=recv_sem.at[part, index],
            device_id=(place.neighbour(way),),
            device_id_type=MESH_ID,
        ).wait_recv()

    def send_from(part, node):
        for index, edge in enumerate(parts[part][3]):
            if edge[0] == node:
                copy(part, index).start()

    own_copies = [
        pltpu.make_async_copy(shards[array], outs[array].at[place.me], local_sem.at[array])
        for array in range(arrays)
    ]
    for own_copy in own_copies:
        own_copy.start()
    enter(place)
    for part in range(len(parts)):
        send_from(part, (0, 0, 0, 0))
    deepest = max(edge[3] for part in parts for edge in part[3])
    for depth in range(1, deepest + 1):
        for part in range(len(parts)):
            for index, edge in enumerate(parts[part][3]):
                if edge[3] == depth and edge[2] != "core":
                    arrived(part, index)
                    send_from(part, edge[1])
    for part in range(len(parts)):
        for index, edge in enumerate(parts[part][3]):
            if edge[2] == "core":
                arrived(part, index)
    for own_copy in own_copies:
        own_copy.wait()
    for part, (array, first, count, tree) in enumerate(parts):
        whole = outs[array].at[pl.ds(0, len(tree))]
        if count is not None:
            whole = whole.at[:, :, pl.ds(first, count)]
        pltpu.make_async_copy(whole, whole, send_sem.at[part]).wait()


def gather_units(shards, plan, ring):
    devices = ring * 8
    edges = devices - 1
    return pl.pallas_call(
        partial(gather_kernel, ring, plan),
        out_shape=[
            jax.ShapeDtypeStruct((devices,) + shard.shape, shard.dtype) for shard in shards
        ],
        in_specs=[VMEM_SPEC] * len(shards),
        out_specs=[ANY_SPEC] * len(shards),
        scratch_shapes=[
            pltpu.SemaphoreType.DMA((len(plan["parts"]), edges)),
            pltpu.SemaphoreType.DMA((len(plan["parts"]),)),
            pltpu.SemaphoreType.DMA((len(shards),)),
        ],
        compiler_params=pltpu.CompilerParams(collective_id=0, has_side_effects=True),
        name="gather_units",
    )(*shards)


def scatter_kernel(ring, plan, *refs):
    shapes = plan["shapes"]
    arrays = len(shapes)
    parts = plan["parts"]
    grads, outs = refs[:arrays], refs[arrays : 2 * arrays]
    owns = refs[2 * arrays : 3 * arrays]
    lands = refs[3 * arrays : 3 * arrays + len(parts)]
    recv_sem, send_sem, local_sem = refs[3 * arrays + len(parts) :]
    place = Place(ring)

    def window(ref, part):
        _, first, count, _ = parts[part]
        return ref if count is None else ref.at[:, pl.ds(first, count)]

    def copy(part, index, source):
        way = parts[part][3][index][2]
        return pltpu.make_async_remote_copy(
            src_ref=source,
            dst_ref=lands[part].at[index],
            send_sem=send_sem.at[part],
            recv_sem=recv_sem.at[part, index],
            device_id=(place.neighbour(way, back=True),),
            device_id_type=MESH_ID,
        )

    own_copies = [
        pltpu.make_async_copy(grads[array].at[:, place.core], owns[array], local_sem.at[array])
        for array in range(arrays)
    ]
    for own_copy in own_copies:
        own_copy.start()
    enter(place)
    deepest = max(edge[3] for part in parts for edge in part[3])
    for depth in range(deepest, 0, -1):
        for part, (array, _, _, tree) in enumerate(parts):
            for index, (_, child, way, level) in enumerate(tree):
                if way == "core" and level == depth:
                    chip = place.chip_of(child)
                    source = grads[array].at[chip, place.flip(place.core, 1)]
                    copy(part, index, window(source, part)).start()
    for own_copy in own_copies:
        own_copy.wait()

    def add_up(part, node, target):
        array, first, count, tree = parts[part]
        children = [index for index, edge in enumerate(tree) if edge[0] == node]
        for index in children:
            copy(part, index, lands[part].at[index]).wait_recv()
        chip = place.chip_of(node)
        rows, columns = shapes[array]
        if count is not None:
            columns = count
        step = columns
        while rows * step > 24 * 768 and step % 256 == 0:
            step //= 2
        own = owns[array]

        def body(block, carry):
            here = pl.ds(pl.multiple_of(block * step, 128), step)
            where = pl.ds(pl.multiple_of(first + block * step, 128), step)
            total = own[chip, :, where].astype(jnp.float32)
            for index in children:
                total = total + lands[part][index, :, here].astype(jnp.float32)
            if target is None:
                own[chip, :, where] = total.astype(own.dtype)
            else:
                target[:, where] = total
            return carry

        lax.fori_loop(0, columns // step, body, 0)
        return window(own.at[chip], part)

    waiting = None
    for depth in range(deepest, 0, -1):
        for part in range(len(parts)):
            for index, (_, child, way, level) in enumerate(parts[part][3]):
                if way != "core" and level == depth:
                    ready = copy(part, index, add_up(part, child, None))
                    if waiting is not None:
                        waiting.start()
                    waiting = ready
    waiting.start()
    for part in range(len(parts)):
        add_up(part, (0, 0, 0, 0), outs[parts[part][0]])
    for part in range(len(parts)):
        pltpu.make_async_copy(lands[part], lands[part], send_sem.at[part]).wait()


def scatter_units(grads, plan, ring):
    devices = ring * 8
    edges = devices - 1
    shapes = plan["shapes"]
    lands = []
    for array, _, count, _ in plan["parts"]:
        rows, columns = shapes[array]
        lands.append(
            pltpu.VMEM((edges, rows, columns if count is None else count), jnp.bfloat16)
        )
    return pl.pallas_call(
        partial(scatter_kernel, ring, plan),
        out_shape=[jax.ShapeDtypeStruct(shape, jnp.float32) for shape in shapes],
        in_specs=[ANY_SPEC] * len(shapes),
        out_specs=[VMEM_SPEC] * len(shapes),
        scratch_shapes=[pltpu.VMEM((devices // 2,) + shape, jnp.bfloat16) for shape in shapes]
        + lands
        + [
            pltpu.SemaphoreType.DMA((len(plan["parts"]), edges)),
            pltpu.SemaphoreType.DMA((len(plan["parts"]),)),
            pltpu.SemaphoreType.DMA((len(shapes),)),
        ],
        compiler_params=pltpu.CompilerParams(
            collective_id=1, has_side_effects=True, vmem_limit_bytes=VMEM_LIMIT
        ),
        name="scatter_units",
    )(*[grad.reshape((devices // 2, 2) + shape) for grad, shape in zip(grads, shapes)])


def make_plan(shapes, ring, mixed):
    trees = [make_tree(ring, first, flip) for first in (True, False) for flip in (False, True)]
    parts = []
    for array, (_, columns) in enumerate(shapes):
        flip = array % 2
        late = columns // 512 * 128 if columns > 768 else 0
        if shapes[array][0] > 32:
            late = columns // 3
        if late and mixed:
            parts.append((array, 0, columns - late, trees[flip]))
            parts.append((array, columns - late, late, trees[2 + flip]))
        else:
            parts.append((array, 0, None, trees[flip]))
    return {"shapes": shapes, "parts": parts}


def dot_nt(left, right):
    return lax.dot_general(
        left, right, (((1,), (1,)), ((), ())), preferred_element_type=jnp.float32
    )


def dot_tn(left, right):
    return lax.dot_general(
        left, right, (((0,), (0,)), ((), ())), preferred_element_type=jnp.float32
    )


def dot_nn(left, right):
    return jnp.dot(left, right, preferred_element_type=jnp.float32)


def attend_kernel(lengths_ref, q_ref, k_ref, v_ref, context_ref, log_ref):
    rows, width = q_ref.shape
    length = lengths_ref[pl.program_id(0)]
    lane = lax.broadcasted_iota(jnp.int32, (rows, width), 1)
    inside = lax.broadcasted_iota(jnp.int32, (rows, width), 0) < length
    bias = jnp.where(lax.broadcasted_iota(jnp.int32, (1, rows), 1) < length, 0.0, -1e30)
    queries, keys, values = q_ref[...] * 0.125, k_ref[...], v_ref[...]
    context = jnp.zeros((rows, width), jnp.float32)
    logs = context
    for head in range(width // HEAD_DIM):
        mine = lane // HEAD_DIM == head
        scores = dot_nt(jnp.where(mine, queries, jnp.zeros_like(queries)), keys) + bias
        top = jnp.max(scores, axis=-1, keepdims=True)
        weights = jnp.exp(scores - top).astype(jnp.bfloat16)
        sums = dot_nn(weights, jnp.where(mine, values, jnp.ones_like(values)))
        other = (width - 1) if head == 0 else 0
        total = sums[:, other : other + 1]
        context = jnp.where(mine, sums * (1.0 / total), context)
        logs = jnp.where(mine, top + jnp.log(total), logs)
    context_ref[...] = jnp.where(inside, context, values.astype(jnp.float32)).astype(
        context_ref.dtype
    )
    log_ref[...] = logs


def attend(qkv, lengths):
    rows, width3 = qkv.shape
    width = width3 // 3
    halves = lengths.shape[0]
    half = rows // halves
    pairs = width // 128

    def columns(which):
        return pl.BlockSpec((half, 128), lambda i, j, l: (i, which * pairs + j))

    return pl.pallas_call(
        attend_kernel,
        out_shape=[
            jax.ShapeDtypeStruct((rows, width), jnp.bfloat16),
            jax.ShapeDtypeStruct((rows, width), jnp.float32),
        ],
        grid_spec=pltpu.PrefetchScalarGridSpec(
            num_scalar_prefetch=1,
            grid=(halves, pairs),
            in_specs=[columns(0), columns(1), columns(2)],
            out_specs=[columns(0), columns(0)],
        ),
        compiler_params=pltpu.CompilerParams(vmem_limit_bytes=VMEM_LIMIT),
        name="attend",
    )(lengths, qkv, qkv, qkv)


def attend_back_kernel(
    lengths_ref, q_ref, k_ref, v_ref, context_ref, log_ref, g_ref, grad_ref, sums_ref
):
    rows, width = q_ref.shape
    heads = width // HEAD_DIM
    length = lengths_ref[pl.program_id(0)]
    lane = lax.broadcasted_iota(jnp.int32, (rows, width), 1)
    inside = lax.broadcasted_iota(jnp.int32, (rows, width), 0) < length
    bias = jnp.where(lax.broadcasted_iota(jnp.int32, (rows, 1), 0) < length, 0.0, -1e30)
    queries, keys, values = q_ref[...] * 0.125, k_ref[...], v_ref[...]
    keys_scaled = keys * 0.125
    zero = jnp.zeros_like(queries)
    grads = jnp.where(inside, g_ref[...], zero)
    product = grads.astype(jnp.float32) * context_ref[...].astype(jnp.float32)
    table = jnp.zeros((rows, width), jnp.float32)
    for head in range(heads):
        mine = lane // HEAD_DIM == head
        along = jnp.sum(jnp.where(mine, product, 0.0), axis=-1, keepdims=True)
        first = head * HEAD_DIM
        table = jnp.where(lane == head, log_ref[:, first : first + 1], table)
        table = jnp.where(lane == heads + head, along, table)
    table = jnp.transpose(table)
    grad_q = jnp.zeros((rows, width), jnp.float32)
    grad_k = grad_q
    grad_v = jnp.where(inside, 0.0, g_ref[...].astype(jnp.float32))
    for head in range(heads):
        mine = lane // HEAD_DIM == head
        queries_head = jnp.where(mine, queries, zero)
        grads_head = jnp.where(mine, grads, zero)
        scores = dot_nt(keys, queries_head) + bias
        probs = jnp.exp(scores - table[head : head + 1])
        grad_v = grad_v + dot_nn(probs.astype(jnp.bfloat16), grads_head)
        grad_probs = dot_nt(values, grads_head)
        grad_scores = (probs * (grad_probs - table[heads + head : heads + head + 1])).astype(
            jnp.bfloat16
        )
        grad_k = grad_k + dot_nn(grad_scores, queries_head)
        grad_q = grad_q + dot_tn(grad_scores, jnp.where(mine, keys_scaled, zero))
    for place, grad in enumerate((grad_q, grad_k, grad_v)):
        grad_ref[place] = grad.astype(grad_ref.dtype)
        sums_ref[0, place] = jnp.sum(grad, axis=0, keepdims=True)


def attend_back(qkv, context, logs, grad_context, lengths):
    rows, width3 = qkv.shape
    width = width3 // 3
    halves = lengths.shape[0]
    half = rows // halves
    pairs = width // 128

    def columns(which):
        return pl.BlockSpec((half, 128), lambda i, j, l: (i, which * pairs + j))

    return pl.pallas_call(
        attend_back_kernel,
        out_shape=[
            jax.ShapeDtypeStruct((3, rows, width), jnp.bfloat16),
            jax.ShapeDtypeStruct((halves, 3, 1, width), jnp.float32),
        ],
        grid_spec=pltpu.PrefetchScalarGridSpec(
            num_scalar_prefetch=1,
            grid=(halves, pairs),
            in_specs=[columns(0), columns(1), columns(2)] + [columns(0)] * 3,
            out_specs=[
                pl.BlockSpec((3, half, 128), lambda i, j, l: (0, i, j)),
                pl.BlockSpec((1, 3, 1, 128), lambda i, j, l: (i, 0, 0, j)),
            ],
        ),
        compiler_params=pltpu.CompilerParams(vmem_limit_bytes=VMEM_LIMIT),
        name="attend_back",
    )(lengths, qkv, qkv, qkv, context, logs, grad_context)


LOG2_E = 1.4426950408889634


def gelu_parts(u):
    under = 1.0 + jnp.abs(u) * (0.3275911 * 0.7071067811865476)
    t = pl.reciprocal(under, approx=True)
    t = t * (2.0 - under * t)
    decay = jnp.exp2(u * u * (-0.5 * LOG2_E))
    poly = 0.5 * 1.061405429
    for term in (-1.453152027, 1.421413741, -0.284496736, 0.254829592):
        poly = poly * t + 0.5 * term
    tail = poly * t * decay
    cdf = jnp.where(u < 0, tail, 1.0 - tail)
    return u * cdf, cdf + u * (decay * 0.3989422804014327)


def up_kernel(first_ref, w_ref, b_ref, active_ref, slope_ref):
    rows = first_ref.shape[0]
    step = 128
    for start in range(0, rows, step):
        where = pl.ds(start, step)
        u = dot_nn(first_ref[where, :], w_ref[...]) + b_ref[...]
        value, slope = gelu_parts(u)
        active_ref[where, :] = value.astype(active_ref.dtype)
        slope_ref[where, :] = slope.astype(slope_ref.dtype)


def up_project(first_low, w_up, b_up):
    rows, width = first_low.shape
    hidden = w_up.shape[1]
    block = 512
    return pl.pallas_call(
        up_kernel,
        out_shape=[jax.ShapeDtypeStruct((rows, hidden), jnp.bfloat16)] * 2,
        grid=(hidden // block,),
        in_specs=[
            pl.BlockSpec((rows, width), lambda j: (0, 0)),
            pl.BlockSpec((width, block), lambda j: (0, j)),
            pl.BlockSpec((1, block), lambda j: (0, j)),
        ],
        out_specs=[pl.BlockSpec((rows, block), lambda j: (0, j))] * 2,
        compiler_params=pltpu.CompilerParams(vmem_limit_bytes=VMEM_LIMIT),
        name="up_project",
    )(first_low, w_up, b_up.reshape(1, hidden))


def norm_parts(hidden):
    center = hidden - jnp.mean(hidden, axis=-1, keepdims=True)
    inverse = lax.rsqrt(jnp.mean(center * center, axis=-1, keepdims=True) + 1e-12)
    return (center * inverse, inverse)


def norm_back(grad_out, normed, inverse, gain):
    scaled = grad_out * gain
    centered = scaled - jnp.mean(scaled, axis=-1, keepdims=True)
    return inverse * (centered - normed * jnp.mean(scaled * normed, axis=-1, keepdims=True))


def order_rows(slots, lengths):
    count = slots.shape[0]
    half = count // 2
    row = jnp.arange(count, dtype=jnp.int32)
    first, second = lengths[0], lengths[1]
    twice = jnp.concatenate([slots, slots])
    hole = lax.dynamic_slice_in_dim(twice, second, count)
    later = lax.dynamic_slice_in_dim(twice, first + half, count)
    in_first, in_second = row < first, row - half < second
    inside = jnp.where(row < half, in_first, in_second)
    placed = jnp.where(
        row < half, jnp.where(in_first, slots, hole), jnp.where(in_second, later, slots)
    )
    return placed, inside


def gather_params(params, ring):
    (w_qkv, b_qv, w_out, b_out, g1, c1, w_up, b_up, w_down, b_down, g2, c2, w_proj) = params
    small = [b_qv, b_up, b_out, g1, c1, b_down, g2, c2]
    packed = jnp.concatenate(small)
    if ring is None:
        whole = [lax.all_gather(w, AXIS, axis=0, tiled=True) for w in (w_qkv, w_out, w_up, w_down)]
        proj = lax.all_gather(w_proj, AXIS, axis=0, tiled=True)
        few = lax.all_gather(packed, AXIS, axis=0)
    else:
        filled = jnp.pad(packed, (0, 1024 - packed.shape[0])).reshape(8, 128)
        shards = [w_qkv, w_out, w_up, jnp.concatenate([w_proj, filled], axis=0)]
        plan = make_plan([shard.shape for shard in shards], ring, False)
        units = gather_units(shards, plan, ring)
        w_down, units = lax.optimization_barrier((w_down, units))
        whole = [unit.reshape(-1, unit.shape[2]) for unit in units[:3]]
        whole.append(lax.all_gather(w_down, AXIS, axis=0, tiled=True))
        rows = w_proj.shape[0]
        proj = units[3][:, :rows].reshape(-1, w_proj.shape[1])
        few = units[3][:, rows:].reshape(units[3].shape[0], -1)
    vectors = []
    start = 0
    for entry in small:
        size = entry.shape[0]
        vectors.append(few[:, start : start + size].reshape(-1).astype(jnp.float32))
        start += size
    return whole + [proj], vectors


def scatter_grads(weights, vectors, ring, devices):
    few = [vector.reshape(devices, -1) for vector in vectors]
    sizes = [entry.shape[1] for entry in few]
    few = jnp.concatenate(few, axis=1)

    def native(w):
        return lax.psum_scatter(w, AXIS, scatter_dimension=0, tiled=True).astype(jnp.float32)

    if ring is None:
        shards = [native(w) for w in weights]
        small = lax.psum_scatter(few.reshape(-1), AXIS, scatter_dimension=0, tiled=True)
    else:
        few = jnp.pad(few, ((0, 0), (0, 1024 - few.shape[1]))).astype(jnp.bfloat16)
        down = native(weights[3])
        units = [w.reshape(devices, -1, w.shape[1]) for w in weights[:3] + weights[4:]]
        rows = units[3].shape[1]
        units[3] = jnp.concatenate([units[3], few.reshape(devices, 8, 128)], axis=1)
        plan = make_plan([unit.shape[1:] for unit in units], ring, True)
        shards = list(scatter_units(units, plan, ring))
        small = shards[3][rows:].reshape(-1)
        shards = shards[:3] + [down, shards[3][:rows]]
    pieces = []
    start = 0
    for size in sizes:
        pieces.append(small[start : start + size])
        start += size
    return shards, pieces


def local(tokens, cotangent, slot_row, lengths, *params):
    devices = lax.axis_size(AXIS)
    row_count, model_width = tokens.shape
    peer_rows = row_count // devices
    ring = devices // 8 if params[0].shape[0] % 8 == 0 and devices % 8 == 0 else None
    (w_qkv, w_out, w_up, w_down, w_proj), vectors = gather_params(params, ring)
    b_qv, b_up, b_out, gain_one, bias_one, b_down, gain_two, bias_two = vectors

    local_row, inside = order_rows(
        slot_row // row_count * peer_rows + slot_row % peer_rows, lengths
    )
    both = jnp.concatenate([tokens, cotangent], axis=1)
    arrived = lax.all_to_all(both, AXIS, split_axis=0, concat_axis=0, tiled=True)
    chosen = local_row[:, None] == jnp.arange(row_count, dtype=jnp.int32)[None, :]
    chosen = chosen.astype(jnp.bfloat16)
    dealt = dot_nn(chosen, arrived[:, :model_width]).astype(jnp.bfloat16)
    dealt_cot = dot_nn(chosen, arrived[:, model_width:]).astype(jnp.bfloat16)
    valid = inside[:, None].astype(jnp.float32)

    bias_all = jnp.concatenate(
        [b_qv[:model_width], jnp.zeros((model_width,), jnp.float32), b_qv[model_width:]]
    )
    qkv = (dot_nn(dealt, w_qkv) + bias_all).astype(jnp.bfloat16)
    context, logs = attend(qkv, lengths)
    hidden_one = dealt.astype(jnp.float32) + dot_nn(context, w_out) + b_out
    normed_one, inverse_one = norm_parts(hidden_one)
    first_low = (normed_one * gain_one + bias_one).astype(jnp.bfloat16)
    active, slope = up_project(first_low, w_up, b_up)
    hidden_two = first_low.astype(jnp.float32) + dot_nn(active, w_down) + b_down
    normed_two, inverse_two = norm_parts(hidden_two)
    second_low = (normed_two * gain_two + bias_two).astype(jnp.bfloat16)
    project = dot_nn(second_low, w_proj)
    inv_norm = lax.rsqrt(jnp.sum(project * project, axis=-1, keepdims=True) + 1e-06)
    embedded = (project * inv_norm * valid).astype(jnp.bfloat16)

    grad_emb = dealt_cot.astype(jnp.float32) * valid
    along = jnp.sum(project * grad_emb, axis=-1, keepdims=True)
    grad_project = (inv_norm * grad_emb - inv_norm * inv_norm * inv_norm * along * project).astype(
        jnp.bfloat16
    )
    grad_w_proj = dot_tn(second_low, grad_project).astype(jnp.bfloat16)
    grad_second = dot_nt(grad_project, w_proj)
    grad_gain_two = jnp.sum(grad_second * normed_two, axis=0)
    grad_bias_two = jnp.sum(grad_second, axis=0)
    grad_hidden_two = norm_back(grad_second, normed_two, inverse_two, gain_two)
    grad_b_down = jnp.sum(grad_hidden_two, axis=0)
    down_low = grad_hidden_two.astype(jnp.bfloat16)
    grad_w_down = dot_tn(active, down_low).astype(jnp.bfloat16)
    grad_up = dot_nt(down_low, w_down) * slope.astype(jnp.float32)
    grad_b_up = jnp.sum(grad_up, axis=0)
    up_low = grad_up.astype(jnp.bfloat16)
    grad_w_up = dot_tn(first_low, up_low).astype(jnp.bfloat16)
    grad_first = grad_hidden_two + dot_nt(up_low, w_up)
    grad_gain_one = jnp.sum(grad_first * normed_one, axis=0)
    grad_bias_one = jnp.sum(grad_first, axis=0)
    grad_hidden_one = norm_back(grad_first, normed_one, inverse_one, gain_one)
    grad_b_out = jnp.sum(grad_hidden_one, axis=0)
    out_low = grad_hidden_one.astype(jnp.bfloat16)
    grad_w_out = dot_tn(context, out_low).astype(jnp.bfloat16)
    grad_context = dot_nt(out_low, w_out).astype(jnp.bfloat16)
    grad_three, sums = attend_back(qkv, context, logs, grad_context, lengths)
    sums = jnp.sum(sums, axis=0)[:, 0]
    grad_b_qv = jnp.concatenate([sums[0], sums[2]])
    grad_qkv = jnp.concatenate([grad_three[0], grad_three[1], grad_three[2]], axis=1)
    grad_w_qkv = dot_tn(dealt, grad_qkv).astype(jnp.bfloat16)
    grad_dealt = (dot_nt(grad_qkv, w_qkv) + grad_hidden_one).astype(jnp.bfloat16)

    back = jnp.concatenate([grad_dealt, embedded], axis=1)
    back = dot_tn(chosen, back).astype(jnp.bfloat16)
    returned = lax.all_to_all(back, AXIS, split_axis=0, concat_axis=0, tiled=True)
    shards, small = scatter_grads(
        [grad_w_qkv, grad_w_out, grad_w_up, grad_w_down, grad_w_proj],
        [
            grad_b_qv,
            grad_b_up,
            grad_b_out,
            grad_gain_one,
            grad_bias_one,
            grad_b_down,
            grad_gain_two,
            grad_bias_two,
        ],
        ring,
        devices,
    )
    return (
        returned[:, model_width:],
        returned[:, :model_width],
        shards[0],
        small[0],
        shards[1],
        small[2],
        small[3],
        small[4],
        shards[2],
        small[1],
        shards[3],
        small[5],
        small[6],
        small[7],
        shards[4],
    )


def solution(mesh):
    matrix, vector = P(AXIS, None), P(AXIS)
    params = "mvmvvvmvmvvvm"
    in_kinds = "mmvv" + params
    out_kinds = "mm" + params
    specs = {"m": matrix, "v": vector}

    return jax.shard_map(
        local,
        mesh=mesh,
        in_specs=tuple(specs[kind] for kind in in_kinds),
        out_specs=tuple(specs[kind] for kind in out_kinds),
        check_vma=False,
    )
```

```python
from functools import partial

import jax
import jax.numpy as jnp
from jax import lax
from jax.experimental import pallas as pl
from jax.experimental.pallas import tpu as pltpu
from jax.sharding import PartitionSpec as P


HEAD_DIM = 64
AXIS = "fsdp"
MESH_ID = pl.DeviceIdType.MESH
VMEM_SPEC = pl.BlockSpec(memory_space=pltpu.VMEM)
ANY_SPEC = pl.BlockSpec(memory_space=pl.ANY)
VMEM_LIMIT = 60 * 1024 * 1024


def chain_edges(node, ring, lean_up):
    up_count = ring // 2 if lean_up else (ring - 1) // 2
    edges = []
    here = node
    for _ in range(up_count):
        there = ((here[0] + 1) % ring,) + here[1:]
        edges.append((here, there, "up"))
        here = there
    here = node
    for _ in range(ring - 1 - up_count):
        there = ((here[0] - 1) % ring,) + here[1:]
        edges.append((here, there, "down"))
        here = there
    return edges


def plane_edges(node, x_first):
    z = node[0]
    own, by_x, by_y, both = (z, 0, 0, 0), (z, 0, 1, 0), (z, 1, 0, 0), (z, 1, 1, 0)
    edges = [(own, by_x, "x"), (own, by_y, "y")]
    edges.append((by_x, both, "y") if x_first else (by_y, both, "x"))
    return edges


def make_tree(ring, ring_first, flip):
    root = (0, 0, 0, 0)
    edges = []
    if ring_first:
        edges += chain_edges(root, ring, flip)
        nodes = [root] + [edge[1] for edge in edges]
        for place, node in enumerate(nodes):
            edges += plane_edges(node, (place % 2 == 0) != flip)
    else:
        edges += plane_edges(root, flip)
        nodes = [root] + [edge[1] for edge in edges]
        for place, node in enumerate(nodes):
            edges += chain_edges(node, ring, (place % 2 == 0) != flip)
    nodes = [root] + [edge[1] for edge in edges]
    edges += [(node, node[:3] + (1,), "core") for node in nodes]
    depth = {root: 0}
    for parent, child, _ in edges:
        depth[child] = depth[parent] + 1
    order = sorted(range(len(edges)), key=lambda index: depth[edges[index][1]])
    return [edges[index] + (depth[edges[index][1]],) for index in order]


class Place:
    def __init__(self, ring):
        me = lax.axis_index(AXIS)
        self.ring = ring
        self.me = me
        self.core = lax.rem(me, 2)
        self.x = lax.rem(me // 2, 2)
        self.y = lax.rem(me // 4, 2)
        self.z = me // 8

    @staticmethod
    def flip(value, amount):
        return 1 - value if amount else value

    def chip_of(self, offset):
        z = lax.rem(self.z + (self.ring - offset[0]) % self.ring, self.ring)
        return (z * 2 + self.flip(self.y, offset[1])) * 2 + self.flip(self.x, offset[2])

    def unit_of(self, offset):
        return self.chip_of(offset) * 2 + self.flip(self.core, offset[3])

    def neighbour(self, way, back=False):
        step = {"up": (1, 0, 0, 0), "down": (-1, 0, 0, 0), "x": (0, 0, 1, 0)}
        step.update({"y": (0, 1, 0, 0), "core": (0, 0, 0, 1)})
        offset = step[way]
        dz = offset[0] if back else -offset[0]
        return self.unit_of((dz % self.ring,) + offset[1:])


def enter(place):
    barrier = pltpu.get_barrier_semaphore()
    for way in ("up", "down", "x", "y", "core"):
        pl.semaphore_signal(
            barrier, inc=1, device_id=(place.neighbour(way),), device_id_type=MESH_ID
        )
    pl.semaphore_wait(barrier, 5)


def gather_steps(ring, plan, shards, outs, recv_sem, send_sem, local_sem):
    arrays = len(shards)
    place = Place(ring)
    parts = plan["parts"]

    def window(ref, part):
        _, first, count, _ = parts[part]
        return ref if count is None else ref.at[:, pl.ds(first, count)]

    def copy(part, index):
        array, _, _, tree = parts[part]
        parent, _, way, _ = tree[index]
        unit = place.unit_of(parent)
        source = shards[array] if parent == (0, 0, 0, 0) else outs[array].at[unit]
        return pltpu.make_async_remote_copy(
            src_ref=window(source, part),
            dst_ref=window(outs[array].at[unit], part),
            send_sem=send_sem.at[part],
            recv_sem=recv_sem.at[part, index],
            device_id=(place.neighbour(way),),
            device_id_type=MESH_ID,
        )

    def arrived(part, index):
        array, _, _, tree = parts[part]
        _, child, way, _ = tree[index]
        landed = window(outs[array].at[place.unit_of(child)], part)
        pltpu.make_async_remote_copy(
            src_ref=landed,
            dst_ref=landed,
            send_sem=send_sem.at[part],
            recv_sem=recv_sem.at[part, index],
            device_id=(place.neighbour(way),),
            device_id_type=MESH_ID,
        ).wait_recv()

    def send_from(part, node):
        for index, edge in enumerate(parts[part][3]):
            if edge[0] == node:
                copy(part, index).start()

    def own_copy(array):
        return pltpu.make_async_copy(shards[array], outs[array].at[place.me], local_sem.at[array])

    def begin():
        for array in range(arrays):
            own_copy(array).start()
        enter(place)
        for part in range(len(parts)):
            send_from(part, (0, 0, 0, 0))

    def pass_on(part, index):
        arrived(part, index)
        send_from(part, parts[part][3][index][1])

    events = []
    deepest = max(edge[3] for part in parts for edge in part[3])
    for depth in range(1, deepest + 1):
        for part in range(len(parts)):
            for index, edge in enumerate(parts[part][3]):
                if edge[3] == depth and edge[2] != "core":
                    events.append(partial(pass_on, part, index))

    def finish():
        for part in range(len(parts)):
            for index, edge in enumerate(parts[part][3]):
                if edge[2] == "core":
                    arrived(part, index)
        for array in range(arrays):
            own_copy(array).wait()
        for part, (array, first, count, tree) in enumerate(parts):
            whole = outs[array].at[pl.ds(0, len(tree))]
            if count is not None:
                whole = whole.at[:, :, pl.ds(first, count)]
            pltpu.make_async_copy(whole, whole, send_sem.at[part]).wait()

    return begin, events, finish


def gather_scratch(plan, edges):
    return [
        pltpu.SemaphoreType.DMA((len(plan["parts"]), edges)),
        pltpu.SemaphoreType.DMA((len(plan["parts"]),)),
        pltpu.SemaphoreType.DMA((len(plan["shapes"]),)),
    ]


def run_steps(begin, events, finish):
    begin()
    for event in events:
        event()
    finish()


def spread_steps(step, steps, lag, pace, begin, events, finish):
    def at(number):
        return max(0, min(len(events), (number - lag + 1) * pace))

    def handle(number):
        for event in events[at(number - 1) : at(number)]:
            event()

    def before():
        pl.when(step == 0)(begin)
        for number in range(1, steps):
            if at(number) > at(number - 1):
                pl.when(step == number)(partial(handle, number))

    def after():
        @pl.when(step == steps - 1)
        def _():
            for event in events[at(steps - 1) :]:
                event()
            finish()

    return before, after


def gather_kernel(ring, plan, *refs):
    arrays = len(plan["shapes"])
    run_steps(*gather_steps(ring, plan, refs[:arrays], refs[arrays : 2 * arrays], *refs[2 * arrays :]))


def gather_units(shards, plan, ring):
    devices = ring * 8
    return pl.pallas_call(
        partial(gather_kernel, ring, plan),
        out_shape=[
            jax.ShapeDtypeStruct((devices,) + shard.shape, shard.dtype) for shard in shards
        ],
        in_specs=[VMEM_SPEC] * len(shards),
        out_specs=[ANY_SPEC] * len(shards),
        scratch_shapes=gather_scratch(plan, devices - 1),
        compiler_params=pltpu.CompilerParams(collective_id=0, has_side_effects=True),
        name="gather_units",
    )(*shards)


def scatter_steps(ring, plan, grads, outs, scratch):
    shapes = plan["shapes"]
    arrays = len(shapes)
    parts = plan["parts"]
    owns = scratch[:arrays]
    lands = scratch[arrays : arrays + len(parts)]
    recv_sem, send_sem, local_sem = scratch[arrays + len(parts) :]
    place = Place(ring)

    def window(ref, part):
        _, first, count, _ = parts[part]
        return ref if count is None else ref.at[:, pl.ds(first, count)]

    def copy(part, index, source):
        way = parts[part][3][index][2]
        return pltpu.make_async_remote_copy(
            src_ref=source,
            dst_ref=lands[part].at[index],
            send_sem=send_sem.at[part],
            recv_sem=recv_sem.at[part, index],
            device_id=(place.neighbour(way, back=True),),
            device_id_type=MESH_ID,
        )

    def own_copy(array):
        return pltpu.make_async_copy(
            grads[array].at[:, place.core], owns[array], local_sem.at[array]
        )

    deepest = max(edge[3] for part in parts for edge in part[3])

    def begin():
        for array in range(arrays):
            own_copy(array).start()
        enter(place)
        for depth in range(deepest, 0, -1):
            for part, (array, _, _, tree) in enumerate(parts):
                for index, (_, child, way, level) in enumerate(tree):
                    if way == "core" and level == depth:
                        chip = place.chip_of(child)
                        source = grads[array].at[chip, place.flip(place.core, 1)]
                        copy(part, index, window(source, part)).start()
        for array in range(arrays):
            own_copy(array).wait()

    def add_up(part, node, target):
        array, first, count, tree = parts[part]
        children = [index for index, edge in enumerate(tree) if edge[0] == node]
        for index in children:
            copy(part, index, lands[part].at[index]).wait_recv()
        chip = place.chip_of(node)
        rows, columns = shapes[array]
        if count is not None:
            columns = count
        step = columns
        while rows * step > 24 * 768 and step % 256 == 0:
            step //= 2
        own = owns[array]

        def body(block, carry):
            here = pl.ds(pl.multiple_of(block * step, 128), step)
            where = pl.ds(pl.multiple_of(first + block * step, 128), step)
            total = own[chip, :, where].astype(jnp.float32)
            for index in children:
                total = total + lands[part][index, :, here].astype(jnp.float32)
            if target is None:
                own[chip, :, where] = total.astype(own.dtype)
            else:
                target[:, where] = total
            return carry

        lax.fori_loop(0, columns // step, body, 0)

    inner = [
        (part, index)
        for depth in range(deepest, 0, -1)
        for part in range(len(parts))
        for index, edge in enumerate(parts[part][3])
        if edge[2] != "core" and edge[3] == depth
    ]

    def send(part, index):
        array, _, _, tree = parts[part]
        own = owns[array].at[place.chip_of(tree[index][1])]
        copy(part, index, window(own, part)).start()

    def add_then_send(number):
        part, index = inner[number]
        add_up(part, parts[part][3][index][1], None)
        if number:
            send(*inner[number - 1])

    events = [partial(add_then_send, number) for number in range(len(inner))]

    def finish():
        send(*inner[-1])
        for part in range(len(parts)):
            add_up(part, (0, 0, 0, 0), outs[parts[part][0]])
        for part in range(len(parts)):
            pltpu.make_async_copy(lands[part], lands[part], send_sem.at[part]).wait()

    return begin, events, finish


def scatter_scratch(plan, devices):
    shapes = plan["shapes"]
    edges = devices - 1
    lands = []
    for array, _, count, _ in plan["parts"]:
        rows, columns = shapes[array]
        lands.append(
            pltpu.VMEM((edges, rows, columns if count is None else count), jnp.bfloat16)
        )
    owns = [pltpu.VMEM((devices // 2,) + shape, jnp.bfloat16) for shape in shapes]
    return owns + lands + gather_scratch(plan, edges)


def scatter_kernel(ring, plan, *refs):
    arrays = len(plan["shapes"])
    run_steps(
        *scatter_steps(ring, plan, refs[:arrays], refs[arrays : 2 * arrays], refs[2 * arrays :])
    )


def by_owner(grads, shapes, devices):
    return [grad.reshape((devices // 2, 2) + shape) for grad, shape in zip(grads, shapes)]


def scatter_units(grads, plan, ring):
    devices = ring * 8
    shapes = plan["shapes"]
    return pl.pallas_call(
        partial(scatter_kernel, ring, plan),
        out_shape=[jax.ShapeDtypeStruct(shape, jnp.float32) for shape in shapes],
        in_specs=[ANY_SPEC] * len(shapes),
        out_specs=[VMEM_SPEC] * len(shapes),
        scratch_shapes=scatter_scratch(plan, devices),
        compiler_params=pltpu.CompilerParams(
            collective_id=1, has_side_effects=True, vmem_limit_bytes=VMEM_LIMIT
        ),
        name="scatter_units",
    )(*by_owner(grads, shapes, devices))


def make_plan(shapes, ring, mixed):
    trees = [make_tree(ring, first, flip) for first in (True, False) for flip in (False, True)]
    parts = []
    for array, (_, columns) in enumerate(shapes):
        flip = array % 2
        late = columns // 512 * 128 if columns > 768 else 0
        if shapes[array][0] > 32:
            late = columns // 3
        if late and mixed:
            parts.append((array, 0, columns - late, trees[flip]))
            parts.append((array, columns - late, late, trees[2 + flip]))
        else:
            parts.append((array, 0, None, trees[flip]))
    return {"shapes": shapes, "parts": parts}


def dot_nt(left, right):
    return lax.dot_general(
        left, right, (((1,), (1,)), ((), ())), preferred_element_type=jnp.float32
    )


def dot_tn(left, right):
    return lax.dot_general(
        left, right, (((0,), (0,)), ((), ())), preferred_element_type=jnp.float32
    )


def dot_nn(left, right):
    return jnp.dot(left, right, preferred_element_type=jnp.float32)


def attend_kernel(lengths_ref, q_ref, k_ref, v_ref, context_ref, log_ref):
    rows, width = q_ref.shape
    length = lengths_ref[pl.program_id(0)]
    lane = lax.broadcasted_iota(jnp.int32, (rows, width), 1)
    inside = lax.broadcasted_iota(jnp.int32, (rows, width), 0) < length
    bias = jnp.where(lax.broadcasted_iota(jnp.int32, (1, rows), 1) < length, 0.0, -1e30)
    queries, keys, values = q_ref[...] * 0.125, k_ref[...], v_ref[...]
    context = jnp.zeros((rows, width), jnp.float32)
    logs = context
    for head in range(width // HEAD_DIM):
        mine = lane // HEAD_DIM == head
        scores = dot_nt(jnp.where(mine, queries, jnp.zeros_like(queries)), keys) + bias
        top = jnp.max(scores, axis=-1, keepdims=True)
        weights = jnp.exp(scores - top).astype(jnp.bfloat16)
        sums = dot_nn(weights, jnp.where(mine, values, jnp.ones_like(values)))
        other = (width - 1) if head == 0 else 0
        total = sums[:, other : other + 1]
        context = jnp.where(mine, sums * (1.0 / total), context)
        logs = jnp.where(mine, top + jnp.log(total), logs)
    context_ref[...] = jnp.where(inside, context, values.astype(jnp.float32)).astype(
        context_ref.dtype
    )
    log_ref[...] = logs


def grid_step():
    return pl.program_id(0) * pl.num_programs(1) + pl.program_id(1)


def attend_gather_kernel(ring, plan, steps, lengths_ref, q_ref, k_ref, v_ref, *refs):
    arrays = len(plan["shapes"])
    shards = refs[:arrays]
    context_ref, log_ref = refs[arrays : arrays + 2]
    outs = refs[arrays + 2 : 2 * arrays + 2]
    moves = gather_steps(ring, plan, shards, outs, *refs[2 * arrays + 2 :])
    before, after = spread_steps(grid_step(), steps, 3, 3, *moves)
    before()
    attend_kernel(lengths_ref, q_ref, k_ref, v_ref, context_ref, log_ref)
    after()


def attend(qkv, lengths, shards, ring):
    rows, width3 = qkv.shape
    width = width3 // 3
    halves = lengths.shape[0]
    half = rows // halves
    pairs = width // 128

    def columns(which):
        return pl.BlockSpec((half, 128), lambda i, j, l: (i, which * pairs + j))

    params = {"vmem_limit_bytes": VMEM_LIMIT}
    kernel, scratch, more = attend_kernel, [], []
    if shards:
        devices = ring * 8
        plan = make_plan([shard.shape for shard in shards], ring, True)
        kernel = partial(attend_gather_kernel, ring, plan, halves * pairs)
        scratch = gather_scratch(plan, devices - 1)
        more = [jax.ShapeDtypeStruct((devices,) + shard.shape, shard.dtype) for shard in shards]
        params.update(collective_id=2, has_side_effects=True)
    return pl.pallas_call(
        kernel,
        out_shape=[
            jax.ShapeDtypeStruct((rows, width), jnp.bfloat16),
            jax.ShapeDtypeStruct((rows, width), jnp.float32),
        ]
        + more,
        grid_spec=pltpu.PrefetchScalarGridSpec(
            num_scalar_prefetch=1,
            grid=(halves, pairs),
            in_specs=[columns(0), columns(1), columns(2)] + [VMEM_SPEC] * len(shards),
            out_specs=[columns(0), columns(0)] + [ANY_SPEC] * len(shards),
            scratch_shapes=scratch,
        ),
        compiler_params=pltpu.CompilerParams(**params),
        name="attend",
    )(lengths, qkv, qkv, qkv, *shards)


def attend_back_kernel(
    lengths_ref, q_ref, k_ref, v_ref, context_ref, log_ref, g_ref, grad_ref, sums_ref
):
    rows, width = q_ref.shape
    heads = width // HEAD_DIM
    length = lengths_ref[pl.program_id(0)]
    lane = lax.broadcasted_iota(jnp.int32, (rows, width), 1)
    inside = lax.broadcasted_iota(jnp.int32, (rows, width), 0) < length
    bias = jnp.where(lax.broadcasted_iota(jnp.int32, (rows, 1), 0) < length, 0.0, -1e30)
    queries, keys, values = q_ref[...] * 0.125, k_ref[...], v_ref[...]
    keys_scaled = keys * 0.125
    zero = jnp.zeros_like(queries)
    grads = jnp.where(inside, g_ref[...], zero)
    product = grads.astype(jnp.float32) * context_ref[...].astype(jnp.float32)
    table = jnp.zeros((rows, width), jnp.float32)
    for head in range(heads):
        mine = lane // HEAD_DIM == head
        along = jnp.sum(jnp.where(mine, product, 0.0), axis=-1, keepdims=True)
        first = head * HEAD_DIM
        table = jnp.where(lane == head, log_ref[:, first : first + 1], table)
        table = jnp.where(lane == heads + head, along, table)
    table = jnp.transpose(table)
    grad_q = jnp.zeros((rows, width), jnp.float32)
    grad_k = grad_q
    grad_v = jnp.where(inside, 0.0, g_ref[...].astype(jnp.float32))
    for head in range(heads):
        mine = lane // HEAD_DIM == head
        queries_head = jnp.where(mine, queries, zero)
        grads_head = jnp.where(mine, grads, zero)
        scores = dot_nt(keys, queries_head) + bias
        probs = jnp.exp(scores - table[head : head + 1])
        grad_v = grad_v + dot_nn(probs.astype(jnp.bfloat16), grads_head)
        grad_probs = dot_nt(values, grads_head)
        grad_scores = (probs * (grad_probs - table[heads + head : heads + head + 1])).astype(
            jnp.bfloat16
        )
        grad_k = grad_k + dot_nn(grad_scores, queries_head)
        grad_q = grad_q + dot_tn(grad_scores, jnp.where(mine, keys_scaled, zero))
    for place, grad in enumerate((grad_q, grad_k, grad_v)):
        grad_ref[place] = grad.astype(grad_ref.dtype)
        sums_ref[0, place] = jnp.sum(grad, axis=0, keepdims=True)


def attend_scatter_kernel(ring, plan, steps, lengths_ref, *refs):
    arrays = len(plan["shapes"])
    grads = refs[6 : 6 + arrays]
    outs = refs[8 + arrays : 8 + 2 * arrays]
    moves = scatter_steps(ring, plan, grads, outs, refs[8 + 2 * arrays :])
    before, after = spread_steps(grid_step(), steps, 1, 5, *moves)
    before()
    attend_back_kernel(lengths_ref, *refs[:6], *refs[6 + arrays : 8 + arrays])
    after()


def attend_back(qkv, context, logs, grad_context, lengths, grads, ring):
    rows, width3 = qkv.shape
    width = width3 // 3
    halves = lengths.shape[0]
    half = rows // halves
    pairs = width // 128

    def columns(which):
        return pl.BlockSpec((half, 128), lambda i, j, l: (i, which * pairs + j))

    params = {"vmem_limit_bytes": VMEM_LIMIT}
    kernel, scratch, more = attend_back_kernel, [], []
    if grads:
        devices = ring * 8
        shapes = [(grad.shape[0] // devices, grad.shape[1]) for grad in grads]
        plan = make_plan(shapes, ring, True)
        kernel = partial(attend_scatter_kernel, ring, plan, halves * pairs)
        scratch = scatter_scratch(plan, devices)
        more = [jax.ShapeDtypeStruct(shape, jnp.float32) for shape in shapes]
        params.update(collective_id=3, has_side_effects=True)
        grads = by_owner(grads, shapes, devices)
    return pl.pallas_call(
        kernel,
        out_shape=[
            jax.ShapeDtypeStruct((3, rows, width), jnp.bfloat16),
            jax.ShapeDtypeStruct((halves, 3, 1, width), jnp.float32),
        ]
        + more,
        grid_spec=pltpu.PrefetchScalarGridSpec(
            num_scalar_prefetch=1,
            grid=(halves, pairs),
            in_specs=[columns(0), columns(1), columns(2)]
            + [columns(0)] * 3
            + [ANY_SPEC] * len(grads),
            out_specs=[
                pl.BlockSpec((3, half, 128), lambda i, j, l: (0, i, j)),
                pl.BlockSpec((1, 3, 1, 128), lambda i, j, l: (i, 0, 0, j)),
            ]
            + [VMEM_SPEC] * len(more),
            scratch_shapes=scratch,
        ),
        compiler_params=pltpu.CompilerParams(**params),
        name="attend_back",
    )(lengths, qkv, qkv, qkv, context, logs, grad_context, *grads)


LOG2_E = 1.4426950408889634


def gelu_parts(u):
    under = 1.0 + jnp.abs(u) * (0.3275911 * 0.7071067811865476)
    t = pl.reciprocal(under, approx=True)
    t = t * (2.0 - under * t)
    decay = jnp.exp2(u * u * (-0.5 * LOG2_E))
    poly = 0.5 * 1.061405429
    for term in (-1.453152027, 1.421413741, -0.284496736, 0.254829592):
        poly = poly * t + 0.5 * term
    tail = poly * t * decay
    cdf = jnp.where(u < 0, tail, 1.0 - tail)
    return u * cdf, cdf + u * (decay * 0.3989422804014327)


def up_kernel(first_ref, w_ref, b_ref, active_ref, slope_ref):
    rows = first_ref.shape[0]
    step = 128
    for start in range(0, rows, step):
        where = pl.ds(start, step)
        u = dot_nn(first_ref[where, :], w_ref[...]) + b_ref[...]
        value, slope = gelu_parts(u)
        active_ref[where, :] = value.astype(active_ref.dtype)
        slope_ref[where, :] = slope.astype(slope_ref.dtype)


def up_project(first_low, w_up, b_up):
    rows, width = first_low.shape
    hidden = w_up.shape[1]
    block = 512
    return pl.pallas_call(
        up_kernel,
        out_shape=[jax.ShapeDtypeStruct((rows, hidden), jnp.bfloat16)] * 2,
        grid=(hidden // block,),
        in_specs=[
            pl.BlockSpec((rows, width), lambda j: (0, 0)),
            pl.BlockSpec((width, block), lambda j: (0, j)),
            pl.BlockSpec((1, block), lambda j: (0, j)),
        ],
        out_specs=[pl.BlockSpec((rows, block), lambda j: (0, j))] * 2,
        compiler_params=pltpu.CompilerParams(vmem_limit_bytes=VMEM_LIMIT),
        name="up_project",
    )(first_low, w_up, b_up.reshape(1, hidden))


def norm_parts(hidden):
    center = hidden - jnp.mean(hidden, axis=-1, keepdims=True)
    inverse = lax.rsqrt(jnp.mean(center * center, axis=-1, keepdims=True) + 1e-12)
    return (center * inverse, inverse)


def norm_back(grad_out, normed, inverse, gain):
    scaled = grad_out * gain
    centered = scaled - jnp.mean(scaled, axis=-1, keepdims=True)
    return inverse * (centered - normed * jnp.mean(scaled * normed, axis=-1, keepdims=True))


def order_rows(slots, lengths):
    count = slots.shape[0]
    half = count // 2
    row = jnp.arange(count, dtype=jnp.int32)
    first, second = lengths[0], lengths[1]
    twice = jnp.concatenate([slots, slots])
    hole = lax.dynamic_slice_in_dim(twice, second, count)
    later = lax.dynamic_slice_in_dim(twice, first + half, count)
    in_first, in_second = row < first, row - half < second
    inside = jnp.where(row < half, in_first, in_second)
    placed = jnp.where(
        row < half, jnp.where(in_first, slots, hole), jnp.where(in_second, later, slots)
    )
    return placed, inside


def gather_params(params, ring):
    (w_qkv, b_qv, w_out, b_out, g1, c1, w_up, b_up, w_down, b_down, g2, c2, w_proj) = params
    small = [b_qv, b_up, b_out, g1, c1, b_down, g2, c2]
    packed = jnp.concatenate(small)
    if ring is None:
        whole = [lax.all_gather(w, AXIS, axis=0, tiled=True) for w in (w_qkv, w_out, w_up, w_down)]
        proj = lax.all_gather(w_proj, AXIS, axis=0, tiled=True)
        few = lax.all_gather(packed, AXIS, axis=0)
    else:
        filled = jnp.pad(packed, (0, 1024 - packed.shape[0])).reshape(8, 128)
        shards = [w_qkv, w_out, jnp.concatenate([w_proj, filled], axis=0)]
        plan = make_plan([shard.shape for shard in shards], ring, False)
        units = gather_units(shards, plan, ring)
        whole = [unit.reshape(-1, unit.shape[2]) for unit in units[:2]] + [w_up, w_down]
        rows = w_proj.shape[0]
        proj = units[2][:, :rows].reshape(-1, w_proj.shape[1])
        few = units[2][:, rows:].reshape(units[2].shape[0], -1)
    vectors = []
    start = 0
    for entry in small:
        size = entry.shape[0]
        vectors.append(few[:, start : start + size].reshape(-1).astype(jnp.float32))
        start += size
    return whole + [proj], vectors


def scatter_grads(weights, vectors, ring, devices):
    few = [vector.reshape(devices, -1) for vector in vectors]
    sizes = [entry.shape[1] for entry in few]
    few = jnp.concatenate(few, axis=1)

    def native(w):
        return lax.psum_scatter(w, AXIS, scatter_dimension=0, tiled=True).astype(jnp.float32)

    if ring is None:
        shards = [native(w) for w in weights]
        small = lax.psum_scatter(few.reshape(-1), AXIS, scatter_dimension=0, tiled=True)
    else:
        few = jnp.pad(few, ((0, 0), (0, 1024 - few.shape[1]))).astype(jnp.bfloat16)
        units = [w.reshape(devices, -1, w.shape[1]) for w in weights[:2] + weights[4:]]
        rows = units[2].shape[1]
        units[2] = jnp.concatenate([units[2], few.reshape(devices, 8, 128)], axis=1)
        plan = make_plan([unit.shape[1:] for unit in units], ring, False)
        shards = list(scatter_units(units, plan, ring))
        small = shards[2][rows:].reshape(-1)
        shards = shards[:2] + weights[2:4] + [shards[2][:rows]]
    pieces = []
    start = 0
    for size in sizes:
        pieces.append(small[start : start + size])
        start += size
    return shards, pieces


def local(tokens, cotangent, slot_row, lengths, *params):
    devices = lax.axis_size(AXIS)
    row_count, model_width = tokens.shape
    peer_rows = row_count // devices
    ring = devices // 8 if params[0].shape[0] % 8 == 0 and devices % 8 == 0 else None
    (w_qkv, w_out, w_up, w_down, w_proj), vectors = gather_params(params, ring)
    b_qv, b_up, b_out, gain_one, bias_one, b_down, gain_two, bias_two = vectors

    local_row, inside = order_rows(
        slot_row // row_count * peer_rows + slot_row % peer_rows, lengths
    )
    both = jnp.concatenate([tokens, cotangent], axis=1)
    arrived = lax.all_to_all(both, AXIS, split_axis=0, concat_axis=0, tiled=True)
    chosen = local_row[:, None] == jnp.arange(row_count, dtype=jnp.int32)[None, :]
    chosen = chosen.astype(jnp.bfloat16)
    dealt = dot_nn(chosen, arrived[:, :model_width]).astype(jnp.bfloat16)
    dealt_cot = dot_nn(chosen, arrived[:, model_width:]).astype(jnp.bfloat16)
    valid = inside[:, None].astype(jnp.float32)

    bias_all = jnp.concatenate(
        [b_qv[:model_width], jnp.zeros((model_width,), jnp.float32), b_qv[model_width:]]
    )
    qkv = (dot_nn(dealt, w_qkv) + bias_all).astype(jnp.bfloat16)
    context, logs, *units = attend(qkv, lengths, [w_up, w_down] if ring else [], ring)
    if ring:
        w_up, w_down = [unit.reshape(-1, unit.shape[2]) for unit in units]
    hidden_one = dealt.astype(jnp.float32) + dot_nn(context, w_out) + b_out
    normed_one, inverse_one = norm_parts(hidden_one)
    first_low = (normed_one * gain_one + bias_one).astype(jnp.bfloat16)
    active, slope = up_project(first_low, w_up, b_up)
    hidden_two = first_low.astype(jnp.float32) + dot_nn(active, w_down) + b_down
    normed_two, inverse_two = norm_parts(hidden_two)
    second_low = (normed_two * gain_two + bias_two).astype(jnp.bfloat16)
    project = dot_nn(second_low, w_proj)
    inv_norm = lax.rsqrt(jnp.sum(project * project, axis=-1, keepdims=True) + 1e-06)
    embedded = (project * inv_norm * valid).astype(jnp.bfloat16)

    grad_emb = dealt_cot.astype(jnp.float32) * valid
    along = jnp.sum(project * grad_emb, axis=-1, keepdims=True)
    grad_project = (inv_norm * grad_emb - inv_norm * inv_norm * inv_norm * along * project).astype(
        jnp.bfloat16
    )
    grad_w_proj = dot_tn(second_low, grad_project).astype(jnp.bfloat16)
    grad_second = dot_nt(grad_project, w_proj)
    grad_gain_two = jnp.sum(grad_second * normed_two, axis=0)
    grad_bias_two = jnp.sum(grad_second, axis=0)
    grad_hidden_two = norm_back(grad_second, normed_two, inverse_two, gain_two)
    grad_b_down = jnp.sum(grad_hidden_two, axis=0)
    down_low = grad_hidden_two.astype(jnp.bfloat16)
    grad_w_down = dot_tn(active, down_low).astype(jnp.bfloat16)
    grad_up = dot_nt(down_low, w_down) * slope.astype(jnp.float32)
    grad_b_up = jnp.sum(grad_up, axis=0)
    up_low = grad_up.astype(jnp.bfloat16)
    grad_w_up = dot_tn(first_low, up_low).astype(jnp.bfloat16)
    grad_first = grad_hidden_two + dot_nt(up_low, w_up)
    grad_gain_one = jnp.sum(grad_first * normed_one, axis=0)
    grad_bias_one = jnp.sum(grad_first, axis=0)
    grad_hidden_one = norm_back(grad_first, normed_one, inverse_one, gain_one)
    grad_b_out = jnp.sum(grad_hidden_one, axis=0)
    out_low = grad_hidden_one.astype(jnp.bfloat16)
    grad_w_out = dot_tn(context, out_low).astype(jnp.bfloat16)
    grad_context = dot_nt(out_low, w_out).astype(jnp.bfloat16)
    large = [grad_w_up, grad_w_down] if ring else []
    grad_three, sums, *large = attend_back(
        qkv, context, logs, grad_context, lengths, large, ring
    )
    if ring:
        grad_w_up, grad_w_down = large
    sums = jnp.sum(sums, axis=0)[:, 0]
    grad_b_qv = jnp.concatenate([sums[0], sums[2]])
    grad_qkv = jnp.concatenate([grad_three[0], grad_three[1], grad_three[2]], axis=1)
    grad_w_qkv = dot_tn(dealt, grad_qkv).astype(jnp.bfloat16)
    grad_dealt = (dot_nt(grad_qkv, w_qkv) + grad_hidden_one).astype(jnp.bfloat16)

    back = jnp.concatenate([grad_dealt, embedded], axis=1)
    back = dot_tn(chosen, back).astype(jnp.bfloat16)
    returned = lax.all_to_all(back, AXIS, split_axis=0, concat_axis=0, tiled=True)
    shards, small = scatter_grads(
        [grad_w_qkv, grad_w_out, grad_w_up, grad_w_down, grad_w_proj],
        [
            grad_b_qv,
            grad_b_up,
            grad_b_out,
            grad_gain_one,
            grad_bias_one,
            grad_b_down,
            grad_gain_two,
            grad_bias_two,
        ],
        ring,
        devices,
    )
    return (
        returned[:, model_width:],
        returned[:, :model_width],
        shards[0],
        small[0],
        shards[1],
        small[2],
        small[3],
        small[4],
        shards[2],
        small[1],
        shards[3],
        small[5],
        small[6],
        small[7],
        shards[4],
    )


def solution(mesh):
    matrix, vector = P(AXIS, None), P(AXIS)
    params = "mvmvvvmvmvvvm"
    in_kinds = "mmvv" + params
    out_kinds = "mm" + params
    specs = {"m": matrix, "v": vector}

    return jax.shard_map(
        local,
        mesh=mesh,
        in_specs=tuple(specs[kind] for kind in in_kinds),
        out_specs=tuple(specs[kind] for kind in out_kinds),
        check_vma=False,
    )
```

```python
from functools import partial

import jax
import jax.numpy as jnp
from jax import lax
from jax.experimental import pallas as pl
from jax.experimental.pallas import tpu as pltpu
from jax.sharding import PartitionSpec as P


HEAD_DIM = 64
AXIS = "fsdp"
MESH_ID = pl.DeviceIdType.MESH
VMEM_SPEC = pl.BlockSpec(memory_space=pltpu.VMEM)
ANY_SPEC = pl.BlockSpec(memory_space=pl.ANY)
VMEM_LIMIT = 60 * 1024 * 1024


def chain_edges(node, ring, lean_up):
    up_count = ring // 2 if lean_up else (ring - 1) // 2
    edges = []
    here = node
    for _ in range(up_count):
        there = ((here[0] + 1) % ring,) + here[1:]
        edges.append((here, there, "up"))
        here = there
    here = node
    for _ in range(ring - 1 - up_count):
        there = ((here[0] - 1) % ring,) + here[1:]
        edges.append((here, there, "down"))
        here = there
    return edges


def plane_edges(node, x_first):
    z = node[0]
    own, by_x, by_y, both = (z, 0, 0, 0), (z, 0, 1, 0), (z, 1, 0, 0), (z, 1, 1, 0)
    edges = [(own, by_x, "x"), (own, by_y, "y")]
    edges.append((by_x, both, "y") if x_first else (by_y, both, "x"))
    return edges


def make_tree(ring, ring_first, flip):
    root = (0, 0, 0, 0)
    edges = []
    if ring_first:
        edges += chain_edges(root, ring, flip)
        nodes = [root] + [edge[1] for edge in edges]
        for place, node in enumerate(nodes):
            edges += plane_edges(node, (place % 2 == 0) != flip)
    else:
        edges += plane_edges(root, flip)
        nodes = [root] + [edge[1] for edge in edges]
        for place, node in enumerate(nodes):
            edges += chain_edges(node, ring, (place % 2 == 0) != flip)
    nodes = [root] + [edge[1] for edge in edges]
    edges += [(node, node[:3] + (1,), "core") for node in nodes]
    depth = {root: 0}
    for parent, child, _ in edges:
        depth[child] = depth[parent] + 1
    order = sorted(range(len(edges)), key=lambda index: depth[edges[index][1]])
    return [edges[index] + (depth[edges[index][1]],) for index in order]


class Place:
    def __init__(self, ring):
        me = lax.axis_index(AXIS)
        self.ring = ring
        self.me = me
        self.core = lax.rem(me, 2)
        self.x = lax.rem(me // 2, 2)
        self.y = lax.rem(me // 4, 2)
        self.z = me // 8

    @staticmethod
    def flip(value, amount):
        return 1 - value if amount else value

    def chip_of(self, offset):
        z = lax.rem(self.z + (self.ring - offset[0]) % self.ring, self.ring)
        return (z * 2 + self.flip(self.y, offset[1])) * 2 + self.flip(self.x, offset[2])

    def unit_of(self, offset):
        return self.chip_of(offset) * 2 + self.flip(self.core, offset[3])

    def neighbour(self, way, back=False):
        step = {"up": (1, 0, 0, 0), "down": (-1, 0, 0, 0), "x": (0, 0, 1, 0)}
        step.update({"y": (0, 1, 0, 0), "core": (0, 0, 0, 1)})
        offset = step[way]
        dz = offset[0] if back else -offset[0]
        return self.unit_of((dz % self.ring,) + offset[1:])


def enter(place):
    barrier = pltpu.get_barrier_semaphore()
    for way in ("up", "down", "x", "y", "core"):
        pl.semaphore_signal(
            barrier, inc=1, device_id=(place.neighbour(way),), device_id_type=MESH_ID
        )
    pl.semaphore_wait(barrier, 5)


def gather_steps(ring, plan, shards, outs, recv_sem, send_sem, local_sem):
    arrays = len(shards)
    place = Place(ring)
    parts = plan["parts"]

    def window(ref, part):
        _, first, count, _ = parts[part]
        return ref if count is None else ref.at[:, pl.ds(first, count)]

    def copy(part, index):
        array, _, _, tree = parts[part]
        parent, _, way, _ = tree[index]
        unit = place.unit_of(parent)
        source = shards[array] if parent == (0, 0, 0, 0) else outs[array].at[unit]
        return pltpu.make_async_remote_copy(
            src_ref=window(source, part),
            dst_ref=window(outs[array].at[unit], part),
            send_sem=send_sem.at[part],
            recv_sem=recv_sem.at[part, index],
            device_id=(place.neighbour(way),),
            device_id_type=MESH_ID,
        )

    def arrived(part, index):
        array, _, _, tree = parts[part]
        _, child, way, _ = tree[index]
        landed = window(outs[array].at[place.unit_of(child)], part)
        pltpu.make_async_remote_copy(
            src_ref=landed,
            dst_ref=landed,
            send_sem=send_sem.at[part],
            recv_sem=recv_sem.at[part, index],
            device_id=(place.neighbour(way),),
            device_id_type=MESH_ID,
        ).wait_recv()

    def send_from(part, node):
        for index, edge in enumerate(parts[part][3]):
            if edge[0] == node:
                copy(part, index).start()

    def own_copy(array):
        return pltpu.make_async_copy(shards[array], outs[array].at[place.me], local_sem.at[array])

    def begin():
        for array in range(arrays):
            own_copy(array).start()
        enter(place)
        for part in range(len(parts)):
            send_from(part, (0, 0, 0, 0))

    def pass_on(part, index):
        arrived(part, index)
        send_from(part, parts[part][3][index][1])

    events = []
    deepest = max(edge[3] for part in parts for edge in part[3])
    for depth in range(1, deepest + 1):
        for part in range(len(parts)):
            for index, edge in enumerate(parts[part][3]):
                if edge[3] == depth and edge[2] != "core":
                    events.append(partial(pass_on, part, index))

    def finish():
        for part in range(len(parts)):
            for index, edge in enumerate(parts[part][3]):
                if edge[2] == "core":
                    arrived(part, index)
        for array in range(arrays):
            own_copy(array).wait()
        for part, (array, first, count, tree) in enumerate(parts):
            whole = outs[array].at[pl.ds(0, len(tree))]
            if count is not None:
                whole = whole.at[:, :, pl.ds(first, count)]
            pltpu.make_async_copy(whole, whole, send_sem.at[part]).wait()

    return begin, events, finish


def gather_scratch(plan, edges):
    return [
        pltpu.SemaphoreType.DMA((len(plan["parts"]), edges)),
        pltpu.SemaphoreType.DMA((len(plan["parts"]),)),
        pltpu.SemaphoreType.DMA((len(plan["shapes"]),)),
    ]


def run_steps(begin, events, finish):
    begin()
    for event in events:
        event()
    finish()


def spread_steps(step, steps, lag, pace, begin, events, finish):
    def at(number):
        return max(0, min(len(events), (number - lag + 1) * pace))

    def handle(number):
        for event in events[at(number - 1) : at(number)]:
            event()

    def before():
        pl.when(step == 0)(begin)
        for number in range(1, steps):
            if at(number) > at(number - 1):
                pl.when(step == number)(partial(handle, number))

    def after():
        @pl.when(step == steps - 1)
        def _():
            for event in events[at(steps - 1) :]:
                event()
            finish()

    return before, after


def gather_kernel(ring, plan, *refs):
    arrays = len(plan["shapes"])
    run_steps(*gather_steps(ring, plan, refs[:arrays], refs[arrays : 2 * arrays], *refs[2 * arrays :]))


def gather_units(shards, plan, ring):
    devices = ring * 8
    return pl.pallas_call(
        partial(gather_kernel, ring, plan),
        out_shape=[
            jax.ShapeDtypeStruct((devices,) + shard.shape, shard.dtype) for shard in shards
        ],
        in_specs=[VMEM_SPEC] * len(shards),
        out_specs=[ANY_SPEC] * len(shards),
        scratch_shapes=gather_scratch(plan, devices - 1),
        compiler_params=pltpu.CompilerParams(collective_id=0, has_side_effects=True),
        name="gather_units",
    )(*shards)


def scatter_steps(ring, plan, grads, outs, scratch):
    shapes = plan["shapes"]
    arrays = len(shapes)
    parts = plan["parts"]
    owns = scratch[:arrays]
    lands = scratch[arrays : arrays + len(parts)]
    recv_sem, send_sem, local_sem = scratch[arrays + len(parts) :]
    place = Place(ring)

    def window(ref, part):
        _, first, count, _ = parts[part]
        return ref if count is None else ref.at[:, pl.ds(first, count)]

    def copy(part, index, source):
        way = parts[part][3][index][2]
        return pltpu.make_async_remote_copy(
            src_ref=source,
            dst_ref=lands[part].at[index],
            send_sem=send_sem.at[part],
            recv_sem=recv_sem.at[part, index],
            device_id=(place.neighbour(way, back=True),),
            device_id_type=MESH_ID,
        )

    def own_copy(array):
        return pltpu.make_async_copy(
            grads[array].at[:, place.core], owns[array], local_sem.at[array]
        )

    deepest = max(edge[3] for part in parts for edge in part[3])

    def begin():
        for array in range(arrays):
            own_copy(array).start()
        enter(place)
        for depth in range(deepest, 0, -1):
            for part, (array, _, _, tree) in enumerate(parts):
                for index, (_, child, way, level) in enumerate(tree):
                    if way == "core" and level == depth:
                        chip = place.chip_of(child)
                        source = grads[array].at[chip, place.flip(place.core, 1)]
                        copy(part, index, window(source, part)).start()
        for array in range(arrays):
            own_copy(array).wait()

    def add_up(part, node, target):
        array, first, count, tree = parts[part]
        children = [index for index, edge in enumerate(tree) if edge[0] == node]
        for index in children:
            copy(part, index, lands[part].at[index]).wait_recv()
        chip = place.chip_of(node)
        rows, columns = shapes[array]
        if count is not None:
            columns = count
        step = columns
        while rows * step > 24 * 768 and step % 256 == 0:
            step //= 2
        own = owns[array]

        def body(block, carry):
            here = pl.ds(pl.multiple_of(block * step, 128), step)
            where = pl.ds(pl.multiple_of(first + block * step, 128), step)
            kind = own.dtype if target is None else jnp.float32
            total = own[chip, :, where].astype(kind)
            for index in children:
                total = total + lands[part][index, :, here].astype(kind)
            if target is None:
                own[chip, :, where] = total
            else:
                target[:, where] = total
            return carry

        lax.fori_loop(0, columns // step, body, 0)

    inner = [
        (part, index)
        for depth in range(deepest, 0, -1)
        for part in range(len(parts))
        for index, edge in enumerate(parts[part][3])
        if edge[2] != "core" and edge[3] == depth
    ]

    def send(part, index):
        array, _, _, tree = parts[part]
        own = owns[array].at[place.chip_of(tree[index][1])]
        copy(part, index, window(own, part)).start()

    def add_then_send(number):
        part, index = inner[number]
        add_up(part, parts[part][3][index][1], None)
        if number:
            send(*inner[number - 1])

    events = [partial(add_then_send, number) for number in range(len(inner))]

    def finish():
        send(*inner[-1])
        for part in range(len(parts)):
            add_up(part, (0, 0, 0, 0), outs[parts[part][0]])
        for part in range(len(parts)):
            pltpu.make_async_copy(lands[part], lands[part], send_sem.at[part]).wait()

    return begin, events, finish


def scatter_scratch(plan, devices):
    shapes = plan["shapes"]
    edges = devices - 1
    lands = []
    for array, _, count, _ in plan["parts"]:
        rows, columns = shapes[array]
        lands.append(
            pltpu.VMEM((edges, rows, columns if count is None else count), jnp.bfloat16)
        )
    owns = [pltpu.VMEM((devices // 2,) + shape, jnp.bfloat16) for shape in shapes]
    return owns + lands + gather_scratch(plan, edges)


def scatter_kernel(ring, plan, *refs):
    arrays = len(plan["shapes"])
    run_steps(
        *scatter_steps(ring, plan, refs[:arrays], refs[arrays : 2 * arrays], refs[2 * arrays :])
    )


def by_owner(grads, shapes, devices):
    return [grad.reshape((devices // 2, 2) + shape) for grad, shape in zip(grads, shapes)]


def scatter_units(grads, plan, ring):
    devices = ring * 8
    shapes = plan["shapes"]
    return pl.pallas_call(
        partial(scatter_kernel, ring, plan),
        out_shape=[jax.ShapeDtypeStruct(shape, jnp.float32) for shape in shapes],
        in_specs=[ANY_SPEC] * len(shapes),
        out_specs=[VMEM_SPEC] * len(shapes),
        scratch_shapes=scatter_scratch(plan, devices),
        compiler_params=pltpu.CompilerParams(
            collective_id=1, has_side_effects=True, vmem_limit_bytes=VMEM_LIMIT
        ),
        name="scatter_units",
    )(*by_owner(grads, shapes, devices))


def make_plan(shapes, ring, mixed):
    trees = [make_tree(ring, first, flip) for first in (True, False) for flip in (False, True)]
    parts = []
    for array, (_, columns) in enumerate(shapes):
        flip = array % 2
        late = columns // 512 * 128 if columns > 768 else 0
        if shapes[array][0] > 32:
            late = columns // 3
        if late and mixed:
            parts.append((array, 0, columns - late, trees[flip]))
            parts.append((array, columns - late, late, trees[2 + flip]))
        else:
            parts.append((array, 0, None, trees[flip]))
    return {"shapes": shapes, "parts": parts}


def dot_nt(left, right):
    return lax.dot_general(
        left, right, (((1,), (1,)), ((), ())), preferred_element_type=jnp.float32
    )


def dot_tn(left, right):
    return lax.dot_general(
        left, right, (((0,), (0,)), ((), ())), preferred_element_type=jnp.float32
    )


def dot_nn(left, right):
    return jnp.dot(left, right, preferred_element_type=jnp.float32)


def attend_kernel(lengths_ref, q_ref, k_ref, v_ref, context_ref, log_ref):
    rows, width = q_ref.shape
    length = lengths_ref[pl.program_id(0)]
    lane = lax.broadcasted_iota(jnp.int32, (rows, width), 1)
    inside = lax.broadcasted_iota(jnp.int32, (rows, width), 0) < length
    bias = jnp.where(lax.broadcasted_iota(jnp.int32, (1, rows), 1) < length, 0.0, -1e30)
    queries, keys, values = q_ref[...] * 0.125, k_ref[...], v_ref[...]
    context = jnp.zeros((rows, width), jnp.float32)
    logs = context
    for head in range(width // HEAD_DIM):
        mine = lane // HEAD_DIM == head
        scores = dot_nt(jnp.where(mine, queries, jnp.zeros_like(queries)), keys) + bias
        top = jnp.max(scores, axis=-1, keepdims=True)
        weights = jnp.exp(scores - top).astype(jnp.bfloat16)
        sums = dot_nn(weights, jnp.where(mine, values, jnp.ones_like(values)))
        other = (width - 1) if head == 0 else 0
        total = sums[:, other : other + 1]
        context = jnp.where(mine, sums * (1.0 / total), context)
        logs = jnp.where(mine, top + jnp.log(total), logs)
    context_ref[...] = jnp.where(inside, context, values.astype(jnp.float32)).astype(
        context_ref.dtype
    )
    log_ref[...] = logs


def grid_step():
    return pl.program_id(0) * pl.num_programs(1) + pl.program_id(1)


def attend_gather_kernel(ring, plan, steps, lengths_ref, q_ref, k_ref, v_ref, *refs):
    arrays = len(plan["shapes"])
    shards = refs[:arrays]
    context_ref, log_ref = refs[arrays : arrays + 2]
    outs = refs[arrays + 2 : 2 * arrays + 2]
    moves = gather_steps(ring, plan, shards, outs, *refs[2 * arrays + 2 :])
    before, after = spread_steps(grid_step(), steps, 1, 6, *moves)
    before()
    attend_kernel(lengths_ref, q_ref, k_ref, v_ref, context_ref, log_ref)
    after()


def attend(qkv, lengths, shards, ring):
    rows, width3 = qkv.shape
    width = width3 // 3
    halves = lengths.shape[0]
    half = rows // halves
    pairs = width // 128

    def columns(which):
        return pl.BlockSpec((half, 128), lambda i, j, l: (i, which * pairs + j))

    params = {"vmem_limit_bytes": VMEM_LIMIT}
    kernel, scratch, more = attend_kernel, [], []
    if shards:
        devices = ring * 8
        plan = make_plan([shard.shape for shard in shards], ring, True)
        kernel = partial(attend_gather_kernel, ring, plan, halves * pairs)
        scratch = gather_scratch(plan, devices - 1)
        more = [jax.ShapeDtypeStruct((devices,) + shard.shape, shard.dtype) for shard in shards]
        params.update(collective_id=2, has_side_effects=True)
    return pl.pallas_call(
        kernel,
        out_shape=[
            jax.ShapeDtypeStruct((rows, width), jnp.bfloat16),
            jax.ShapeDtypeStruct((rows, width), jnp.float32),
        ]
        + more,
        grid_spec=pltpu.PrefetchScalarGridSpec(
            num_scalar_prefetch=1,
            grid=(halves, pairs),
            in_specs=[columns(0), columns(1), columns(2)] + [VMEM_SPEC] * len(shards),
            out_specs=[columns(0), columns(0)] + [ANY_SPEC] * len(shards),
            scratch_shapes=scratch,
        ),
        compiler_params=pltpu.CompilerParams(**params),
        name="attend",
    )(lengths, qkv, qkv, qkv, *shards)


def attend_back_kernel(
    lengths_ref, q_ref, k_ref, v_ref, context_ref, log_ref, g_ref, grad_ref, sums_ref
):
    rows, width = q_ref.shape
    heads = width // HEAD_DIM
    length = lengths_ref[pl.program_id(0)]
    lane = lax.broadcasted_iota(jnp.int32, (rows, width), 1)
    inside = lax.broadcasted_iota(jnp.int32, (rows, width), 0) < length
    bias = jnp.where(lax.broadcasted_iota(jnp.int32, (rows, 1), 0) < length, 0.0, -1e30)
    queries, keys, values = q_ref[...] * 0.125, k_ref[...], v_ref[...]
    keys_scaled = keys * 0.125
    zero = jnp.zeros_like(queries)
    grads = jnp.where(inside, g_ref[...], zero)
    product = grads.astype(jnp.float32) * context_ref[...].astype(jnp.float32)
    table = jnp.zeros((rows, width), jnp.float32)
    for head in range(heads):
        mine = lane // HEAD_DIM == head
        along = jnp.sum(jnp.where(mine, product, 0.0), axis=-1, keepdims=True)
        first = head * HEAD_DIM
        table = jnp.where(lane == head, log_ref[:, first : first + 1], table)
        table = jnp.where(lane == heads + head, along, table)
    table = jnp.transpose(table)
    grad_q = jnp.zeros((rows, width), jnp.float32)
    grad_k = grad_q
    grad_v = jnp.where(inside, 0.0, g_ref[...].astype(jnp.float32))
    for head in range(heads):
        mine = lane // HEAD_DIM == head
        queries_head = jnp.where(mine, queries, zero)
        grads_head = jnp.where(mine, grads, zero)
        scores = dot_nt(keys, queries_head) + bias
        probs = jnp.exp(scores - table[head : head + 1])
        grad_v = grad_v + dot_nn(probs.astype(jnp.bfloat16), grads_head)
        grad_probs = dot_nt(values, grads_head)
        grad_scores = (probs * (grad_probs - table[heads + head : heads + head + 1])).astype(
            jnp.bfloat16
        )
        grad_k = grad_k + dot_nn(grad_scores, queries_head)
        grad_q = grad_q + dot_tn(grad_scores, jnp.where(mine, keys_scaled, zero))
    for place, grad in enumerate((grad_q, grad_k, grad_v)):
        grad_ref[place] = grad.astype(grad_ref.dtype)
        sums_ref[0, place] = jnp.sum(grad, axis=0, keepdims=True)


def attend_scatter_kernel(ring, plan, steps, lengths_ref, *refs):
    arrays = len(plan["shapes"])
    grads = refs[6 : 6 + arrays]
    outs = refs[8 + arrays : 8 + 2 * arrays]
    moves = scatter_steps(ring, plan, grads, outs, refs[8 + 2 * arrays :])
    before, after = spread_steps(grid_step(), steps, 1, 5, *moves)
    before()
    attend_back_kernel(lengths_ref, *refs[:6], *refs[6 + arrays : 8 + arrays])
    after()


def attend_back(qkv, context, logs, grad_context, lengths, grads, ring):
    rows, width3 = qkv.shape
    width = width3 // 3
    halves = lengths.shape[0]
    half = rows // halves
    pairs = width // 128

    def columns(which):
        return pl.BlockSpec((half, 128), lambda i, j, l: (i, which * pairs + j))

    params = {"vmem_limit_bytes": VMEM_LIMIT}
    kernel, scratch, more = attend_back_kernel, [], []
    if grads:
        devices = ring * 8
        shapes = [(grad.shape[0] // devices, grad.shape[1]) for grad in grads]
        plan = make_plan(shapes, ring, True)
        kernel = partial(attend_scatter_kernel, ring, plan, halves * pairs)
        scratch = scatter_scratch(plan, devices)
        more = [jax.ShapeDtypeStruct(shape, jnp.float32) for shape in shapes]
        params.update(collective_id=3, has_side_effects=True)
        grads = by_owner(grads, shapes, devices)
    return pl.pallas_call(
        kernel,
        out_shape=[
            jax.ShapeDtypeStruct((3, rows, width), jnp.bfloat16),
            jax.ShapeDtypeStruct((halves, 3, 1, width), jnp.float32),
        ]
        + more,
        grid_spec=pltpu.PrefetchScalarGridSpec(
            num_scalar_prefetch=1,
            grid=(halves, pairs),
            in_specs=[columns(0), columns(1), columns(2)]
            + [columns(0)] * 3
            + [ANY_SPEC] * len(grads),
            out_specs=[
                pl.BlockSpec((3, half, 128), lambda i, j, l: (0, i, j)),
                pl.BlockSpec((1, 3, 1, 128), lambda i, j, l: (i, 0, 0, j)),
            ]
            + [VMEM_SPEC] * len(more),
            scratch_shapes=scratch,
        ),
        compiler_params=pltpu.CompilerParams(**params),
        name="attend_back",
    )(lengths, qkv, qkv, qkv, context, logs, grad_context, *grads)


LOG2_E = 1.4426950408889634


def gelu_parts(u):
    under = 1.0 + jnp.abs(u) * (0.3275911 * 0.7071067811865476)
    t = pl.reciprocal(under, approx=True)
    t = t * (2.0 - under * t)
    decay = jnp.exp2(u * u * (-0.5 * LOG2_E))
    poly = 0.5 * 1.061405429
    for term in (-1.453152027, 1.421413741, -0.284496736, 0.254829592):
        poly = poly * t + 0.5 * term
    tail = poly * t * decay
    cdf = jnp.where(u < 0, tail, 1.0 - tail)
    return u * cdf, cdf + u * (decay * 0.3989422804014327)


def up_kernel(first_ref, w_ref, b_ref, active_ref, slope_ref):
    rows = first_ref.shape[0]
    step = 128
    for start in range(0, rows, step):
        where = pl.ds(start, step)
        u = dot_nn(first_ref[where, :], w_ref[...]) + b_ref[...]
        value, slope = gelu_parts(u)
        active_ref[where, :] = value.astype(active_ref.dtype)
        slope_ref[where, :] = slope.astype(slope_ref.dtype)


def up_project(first_low, w_up, b_up):
    rows, width = first_low.shape
    hidden = w_up.shape[1]
    block = 512
    return pl.pallas_call(
        up_kernel,
        out_shape=[jax.ShapeDtypeStruct((rows, hidden), jnp.bfloat16)] * 2,
        grid=(hidden // block,),
        in_specs=[
            pl.BlockSpec((rows, width), lambda j: (0, 0)),
            pl.BlockSpec((width, block), lambda j: (0, j)),
            pl.BlockSpec((1, block), lambda j: (0, j)),
        ],
        out_specs=[pl.BlockSpec((rows, block), lambda j: (0, j))] * 2,
        compiler_params=pltpu.CompilerParams(vmem_limit_bytes=VMEM_LIMIT),
        name="up_project",
    )(first_low, w_up, b_up.reshape(1, hidden))


def norm_parts(hidden):
    center = hidden - jnp.mean(hidden, axis=-1, keepdims=True)
    inverse = lax.rsqrt(jnp.mean(center * center, axis=-1, keepdims=True) + 1e-12)
    return (center * inverse, inverse)


def norm_back(grad_out, normed, inverse, gain):
    scaled = grad_out * gain
    centered = scaled - jnp.mean(scaled, axis=-1, keepdims=True)
    return inverse * (centered - normed * jnp.mean(scaled * normed, axis=-1, keepdims=True))


def order_rows(slots, lengths):
    count = slots.shape[0]
    half = count // 2
    row = jnp.arange(count, dtype=jnp.int32)
    first, second = lengths[0], lengths[1]
    twice = jnp.concatenate([slots, slots])
    hole = lax.dynamic_slice_in_dim(twice, second, count)
    later = lax.dynamic_slice_in_dim(twice, first + half, count)
    in_first, in_second = row < first, row - half < second
    inside = jnp.where(row < half, in_first, in_second)
    placed = jnp.where(
        row < half, jnp.where(in_first, slots, hole), jnp.where(in_second, later, slots)
    )
    return placed, inside


def tile_layout(wide, wider, size):
    return [
        (1, 0, wide),
        (0, 0, wider),
        (1, wide, size),
        (1, wide + size, size),
        (1, wide + 2 * size, size),
        (0, wider, size),
        (2, 0, size),
        (2, size, size),
    ]


def fill_tile(shards):
    rows = [[shards[1], shards[5]], [shards[0]] + shards[2:5], shards[6:]]
    filled = []
    for row in rows:
        row = jnp.concatenate(row, axis=-1)
        room = [(0, 0)] * (row.ndim - 1) + [(0, 128 - row.shape[-1])]
        filled.append(jnp.pad(row, room))
    tile = jnp.stack(filled, axis=-2)
    return jnp.pad(tile, [(0, 0)] * (tile.ndim - 2) + [(0, 5), (0, 0)])


def split_kernel(layout, tiles_ref, *vector_refs):
    for device in range(tiles_ref.shape[0]):
        for vector_ref, (row, first, size) in zip(vector_refs, layout):
            piece = tiles_ref[device, row : row + 1, first : first + size]
            vector_ref[:, device * size : (device + 1) * size] = piece.astype(jnp.float32)


def split_tiles(tiles, layout):
    devices = tiles.shape[0]
    return pl.pallas_call(
        partial(split_kernel, layout),
        out_shape=[jax.ShapeDtypeStruct((1, devices * size), jnp.float32) for _, _, size in layout],
        in_specs=[VMEM_SPEC],
        out_specs=[VMEM_SPEC] * len(layout),
        name="split_tiles",
    )(tiles.astype(jnp.float32))


def gather_params(params, ring):
    (w_qkv, b_qv, w_out, b_out, g1, c1, w_up, b_up, w_down, b_down, g2, c2, w_proj) = params
    small = [b_qv, b_up, b_out, g1, c1, b_down, g2, c2]
    if ring is None:
        whole = [lax.all_gather(w, AXIS, axis=0, tiled=True) for w in (w_qkv, w_out, w_up, w_down)]
        proj = lax.all_gather(w_proj, AXIS, axis=0, tiled=True)
        few = lax.all_gather(jnp.concatenate(small), AXIS, axis=0).astype(jnp.float32)
        vectors = []
        start = 0
        for entry in small:
            size = entry.shape[0]
            vectors.append(few[:, start : start + size].reshape(-1))
            start += size
    else:
        shards = [w_qkv, w_out, jnp.concatenate([w_proj, fill_tile(small)], axis=0)]
        plan = make_plan([shard.shape for shard in shards], ring, False)
        units = gather_units(shards, plan, ring)
        whole = [unit.reshape(-1, unit.shape[2]) for unit in units[:2]] + [w_up, w_down]
        rows = w_proj.shape[0]
        proj = units[2][:, :rows].reshape(-1, w_proj.shape[1])
        layout = tile_layout(b_qv.shape[0], b_up.shape[0], b_out.shape[0])
        vectors = [row.reshape(-1) for row in split_tiles(units[2][:, rows:], layout)]
    return whole + [proj], vectors


def join_kernel(layout, *refs):
    vector_refs, tiles_ref = refs[:-1], refs[-1]
    tiles_ref[...] = jnp.zeros_like(tiles_ref)
    for device in range(tiles_ref.shape[0]):
        for vector_ref, (row, first, size) in zip(vector_refs, layout):
            piece = vector_ref[:, device * size : (device + 1) * size]
            tiles_ref[device, row : row + 1, first : first + size] = piece


def join_tiles(vectors, layout, devices):
    return pl.pallas_call(
        partial(join_kernel, layout),
        out_shape=jax.ShapeDtypeStruct((devices, 8, 128), jnp.float32),
        in_specs=[VMEM_SPEC] * len(layout),
        out_specs=VMEM_SPEC,
        name="join_tiles",
    )(*[vector.reshape(1, -1) for vector in vectors])


def scatter_grads(weights, vectors, ring, devices):
    sizes = [vector.shape[0] // devices for vector in vectors]
    if ring is None:
        few = jnp.concatenate([vector.reshape(devices, -1) for vector in vectors], axis=1)
        shards = [
            lax.psum_scatter(w, AXIS, scatter_dimension=0, tiled=True).astype(jnp.float32)
            for w in weights
        ]
        small = lax.psum_scatter(few.reshape(-1), AXIS, scatter_dimension=0, tiled=True)
        pieces = []
        start = 0
        for size in sizes:
            pieces.append(small[start : start + size])
            start += size
    else:
        layout = tile_layout(sizes[0], sizes[1], sizes[2])
        tiles = join_tiles(vectors, layout, devices).astype(jnp.bfloat16)
        units = [w.reshape(devices, -1, w.shape[1]) for w in weights[:2] + weights[4:]]
        rows = units[2].shape[1]
        units[2] = jnp.concatenate([units[2], tiles], axis=1)
        plan = make_plan([unit.shape[1:] for unit in units], ring, False)
        shards = list(scatter_units(units, plan, ring))
        tile = shards[2][rows:]
        pieces = [tile[row, first : first + size] for row, first, size in layout]
        shards = shards[:2] + weights[2:4] + [shards[2][:rows]]
    return shards, pieces


def local(tokens, cotangent, slot_row, lengths, *params):
    devices = lax.axis_size(AXIS)
    row_count, model_width = tokens.shape
    peer_rows = row_count // devices
    ring = devices // 8 if params[0].shape[0] % 8 == 0 and devices % 8 == 0 else None
    (w_qkv, w_out, w_up, w_down, w_proj), vectors = gather_params(params, ring)
    b_qv, b_up, b_out, gain_one, bias_one, b_down, gain_two, bias_two = vectors

    local_row, inside = order_rows(
        slot_row // row_count * peer_rows + slot_row % peer_rows, lengths
    )
    both = jnp.concatenate([tokens, cotangent], axis=1)
    arrived = lax.all_to_all(both, AXIS, split_axis=0, concat_axis=0, tiled=True)
    chosen = local_row[:, None] == jnp.arange(row_count, dtype=jnp.int32)[None, :]
    chosen = chosen.astype(jnp.bfloat16)
    dealt = dot_nn(chosen, arrived[:, :model_width]).astype(jnp.bfloat16)
    dealt_cot = dot_nn(chosen, arrived[:, model_width:]).astype(jnp.bfloat16)
    valid = inside[:, None].astype(jnp.float32)

    bias_all = jnp.concatenate(
        [b_qv[:model_width], jnp.zeros((model_width,), jnp.float32), b_qv[model_width:]]
    )
    qkv = (dot_nn(dealt, w_qkv) + bias_all).astype(jnp.bfloat16)
    context, logs, *units = attend(qkv, lengths, [w_up, w_down] if ring else [], ring)
    if ring:
        w_up, w_down = [unit.reshape(-1, unit.shape[2]) for unit in units]
    hidden_one = dealt.astype(jnp.float32) + dot_nn(context, w_out) + b_out
    normed_one, inverse_one = norm_parts(hidden_one)
    first_low = (normed_one * gain_one + bias_one).astype(jnp.bfloat16)
    active, slope = up_project(first_low, w_up, b_up)
    hidden_two = first_low.astype(jnp.float32) + dot_nn(active, w_down) + b_down
    normed_two, inverse_two = norm_parts(hidden_two)
    second_low = (normed_two * gain_two + bias_two).astype(jnp.bfloat16)
    project = dot_nn(second_low, w_proj)
    inv_norm = lax.rsqrt(jnp.sum(project * project, axis=-1, keepdims=True) + 1e-06)
    embedded = (project * inv_norm * valid).astype(jnp.bfloat16)

    grad_emb = dealt_cot.astype(jnp.float32) * valid
    along = jnp.sum(project * grad_emb, axis=-1, keepdims=True)
    grad_project = (inv_norm * grad_emb - inv_norm * inv_norm * inv_norm * along * project).astype(
        jnp.bfloat16
    )
    grad_w_proj = dot_tn(second_low, grad_project).astype(jnp.bfloat16)
    grad_second = dot_nt(grad_project, w_proj)
    grad_gain_two = jnp.sum(grad_second * normed_two, axis=0)
    grad_bias_two = jnp.sum(grad_second, axis=0)
    grad_hidden_two = norm_back(grad_second, normed_two, inverse_two, gain_two)
    grad_b_down = jnp.sum(grad_hidden_two, axis=0)
    down_low = grad_hidden_two.astype(jnp.bfloat16)
    grad_w_down = dot_tn(active, down_low).astype(jnp.bfloat16)
    grad_up = dot_nt(down_low, w_down) * slope.astype(jnp.float32)
    grad_b_up = jnp.sum(grad_up, axis=0)
    up_low = grad_up.astype(jnp.bfloat16)
    grad_w_up = dot_tn(first_low, up_low).astype(jnp.bfloat16)
    grad_first = grad_hidden_two + dot_nt(up_low, w_up)
    grad_gain_one = jnp.sum(grad_first * normed_one, axis=0)
    grad_bias_one = jnp.sum(grad_first, axis=0)
    grad_hidden_one = norm_back(grad_first, normed_one, inverse_one, gain_one)
    grad_b_out = jnp.sum(grad_hidden_one, axis=0)
    out_low = grad_hidden_one.astype(jnp.bfloat16)
    grad_w_out = dot_tn(context, out_low).astype(jnp.bfloat16)
    grad_context = dot_nt(out_low, w_out).astype(jnp.bfloat16)
    large = [grad_w_up, grad_w_down] if ring else []
    grad_three, sums, *large = attend_back(
        qkv, context, logs, grad_context, lengths, large, ring
    )
    if ring:
        grad_w_up, grad_w_down = large
    sums = jnp.sum(sums, axis=0)[:, 0]
    grad_b_qv = jnp.concatenate([sums[0], sums[2]])
    grad_qkv = jnp.concatenate([grad_three[0], grad_three[1], grad_three[2]], axis=1)
    grad_w_qkv = dot_tn(dealt, grad_qkv).astype(jnp.bfloat16)
    grad_dealt = (dot_nt(grad_qkv, w_qkv) + grad_hidden_one).astype(jnp.bfloat16)

    back = jnp.concatenate([grad_dealt, embedded], axis=1)
    back = dot_tn(chosen, back).astype(jnp.bfloat16)
    returned = lax.all_to_all(back, AXIS, split_axis=0, concat_axis=0, tiled=True)
    shards, small = scatter_grads(
        [grad_w_qkv, grad_w_out, grad_w_up, grad_w_down, grad_w_proj],
        [
            grad_b_qv,
            grad_b_up,
            grad_b_out,
            grad_gain_one,
            grad_bias_one,
            grad_b_down,
            grad_gain_two,
            grad_bias_two,
        ],
        ring,
        devices,
    )
    return (
        returned[:, model_width:],
        returned[:, :model_width],
        shards[0],
        small[0],
        shards[1],
        small[2],
        small[3],
        small[4],
        shards[2],
        small[1],
        shards[3],
        small[5],
        small[6],
        small[7],
        shards[4],
    )


def solution(mesh):
    matrix, vector = P(AXIS, None), P(AXIS)
    params = "mvmvvvmvmvvvm"
    in_kinds = "mmvv" + params
    out_kinds = "mm" + params
    specs = {"m": matrix, "v": vector}

    return jax.shard_map(
        local,
        mesh=mesh,
        in_specs=tuple(specs[kind] for kind in in_kinds),
        out_specs=tuple(specs[kind] for kind in out_kinds),
        check_vma=False,
    )
```

```python
from functools import partial

import jax
import jax.numpy as jnp
from jax import lax
from jax.experimental import pallas as pl
from jax.experimental.pallas import tpu as pltpu
from jax.sharding import PartitionSpec as P


HEAD_DIM = 64
AXIS = "fsdp"
MESH_ID = pl.DeviceIdType.MESH
VMEM_SPEC = pl.BlockSpec(memory_space=pltpu.VMEM)
ANY_SPEC = pl.BlockSpec(memory_space=pl.ANY)
VMEM_LIMIT = 60 * 1024 * 1024


def chain_edges(node, ring, lean_up):
    up_count = ring // 2 if lean_up else (ring - 1) // 2
    edges = []
    here = node
    for _ in range(up_count):
        there = ((here[0] + 1) % ring,) + here[1:]
        edges.append((here, there, "up"))
        here = there
    here = node
    for _ in range(ring - 1 - up_count):
        there = ((here[0] - 1) % ring,) + here[1:]
        edges.append((here, there, "down"))
        here = there
    return edges


def plane_edges(node, x_first):
    z = node[0]
    own, by_x, by_y, both = (z, 0, 0, 0), (z, 0, 1, 0), (z, 1, 0, 0), (z, 1, 1, 0)
    edges = [(own, by_x, "x"), (own, by_y, "y")]
    edges.append((by_x, both, "y") if x_first else (by_y, both, "x"))
    return edges


def make_tree(ring, ring_first, flip):
    root = (0, 0, 0, 0)
    edges = []
    if ring_first:
        edges += chain_edges(root, ring, flip)
        nodes = [root] + [edge[1] for edge in edges]
        for place, node in enumerate(nodes):
            edges += plane_edges(node, (place % 2 == 0) != flip)
    else:
        edges += plane_edges(root, flip)
        nodes = [root] + [edge[1] for edge in edges]
        for place, node in enumerate(nodes):
            edges += chain_edges(node, ring, (place % 2 == 0) != flip)
    nodes = [root] + [edge[1] for edge in edges]
    edges += [(node, node[:3] + (1,), "core") for node in nodes]
    depth = {root: 0}
    for parent, child, _ in edges:
        depth[child] = depth[parent] + 1
    order = sorted(range(len(edges)), key=lambda index: depth[edges[index][1]])
    return [edges[index] + (depth[edges[index][1]],) for index in order]


class Place:
    def __init__(self, ring):
        me = lax.axis_index(AXIS)
        self.ring = ring
        self.me = me
        self.core = lax.rem(me, 2)
        self.x = lax.rem(me // 2, 2)
        self.y = lax.rem(me // 4, 2)
        self.z = me // 8

    @staticmethod
    def flip(value, amount):
        return 1 - value if amount else value

    def chip_of(self, offset):
        z = lax.rem(self.z + (self.ring - offset[0]) % self.ring, self.ring)
        return (z * 2 + self.flip(self.y, offset[1])) * 2 + self.flip(self.x, offset[2])

    def unit_of(self, offset):
        return self.chip_of(offset) * 2 + self.flip(self.core, offset[3])

    def neighbour(self, way, back=False):
        step = {"up": (1, 0, 0, 0), "down": (-1, 0, 0, 0), "x": (0, 0, 1, 0)}
        step.update({"y": (0, 1, 0, 0), "core": (0, 0, 0, 1)})
        offset = step[way]
        dz = offset[0] if back else -offset[0]
        return self.unit_of((dz % self.ring,) + offset[1:])


def enter(place):
    barrier = pltpu.get_barrier_semaphore()
    for way in ("up", "down", "x", "y", "core"):
        pl.semaphore_signal(
            barrier, inc=1, device_id=(place.neighbour(way),), device_id_type=MESH_ID
        )
    pl.semaphore_wait(barrier, 5)


def gather_steps(ring, plan, shards, outs, recv_sem, send_sem, local_sem):
    arrays = len(shards)
    place = Place(ring)
    parts = plan["parts"]

    def window(ref, part):
        _, first, count, _ = parts[part]
        return ref if count is None else ref.at[:, pl.ds(first, count)]

    def copy(part, index):
        array, _, _, tree = parts[part]
        parent, _, way, _ = tree[index]
        unit = place.unit_of(parent)
        source = shards[array] if parent == (0, 0, 0, 0) else outs[array].at[unit]
        return pltpu.make_async_remote_copy(
            src_ref=window(source, part),
            dst_ref=window(outs[array].at[unit], part),
            send_sem=send_sem.at[part],
            recv_sem=recv_sem.at[part, index],
            device_id=(place.neighbour(way),),
            device_id_type=MESH_ID,
        )

    def arrived(part, index):
        array, _, _, tree = parts[part]
        _, child, way, _ = tree[index]
        landed = window(outs[array].at[place.unit_of(child)], part)
        pltpu.make_async_remote_copy(
            src_ref=landed,
            dst_ref=landed,
            send_sem=send_sem.at[part],
            recv_sem=recv_sem.at[part, index],
            device_id=(place.neighbour(way),),
            device_id_type=MESH_ID,
        ).wait_recv()

    def send_from(part, node):
        for index, edge in enumerate(parts[part][3]):
            if edge[0] == node:
                copy(part, index).start()

    def own_copy(array):
        return pltpu.make_async_copy(shards[array], outs[array].at[place.me], local_sem.at[array])

    def begin():
        for array in range(arrays):
            own_copy(array).start()
        enter(place)
        for part in range(len(parts)):
            send_from(part, (0, 0, 0, 0))

    def pass_on(part, index):
        arrived(part, index)
        send_from(part, parts[part][3][index][1])

    events = []
    deepest = max(edge[3] for part in parts for edge in part[3])
    for depth in range(1, deepest + 1):
        for part in range(len(parts)):
            for index, edge in enumerate(parts[part][3]):
                if edge[3] == depth and edge[2] != "core":
                    events.append(partial(pass_on, part, index))

    def finish():
        for part in range(len(parts)):
            for index, edge in enumerate(parts[part][3]):
                if edge[2] == "core":
                    arrived(part, index)
        for array in range(arrays):
            own_copy(array).wait()
        for part, (array, first, count, tree) in enumerate(parts):
            whole = outs[array].at[pl.ds(0, len(tree))]
            if count is not None:
                whole = whole.at[:, :, pl.ds(first, count)]
            pltpu.make_async_copy(whole, whole, send_sem.at[part]).wait()

    return begin, events, finish


def gather_scratch(plan, edges):
    return [
        pltpu.SemaphoreType.DMA((len(plan["parts"]), edges)),
        pltpu.SemaphoreType.DMA((len(plan["parts"]),)),
        pltpu.SemaphoreType.DMA((len(plan["shapes"]),)),
    ]


def run_steps(begin, events, finish):
    begin()
    for event in events:
        event()
    finish()


def spread_steps(step, steps, lag, pace, begin, events, finish):
    def at(number):
        return max(0, min(len(events), (number - lag + 1) * pace))

    def handle(number):
        for event in events[at(number - 1) : at(number)]:
            event()

    def before():
        pl.when(step == 0)(begin)
        for number in range(1, steps):
            if at(number) > at(number - 1):
                pl.when(step == number)(partial(handle, number))

    def after():
        @pl.when(step == steps - 1)
        def _():
            for event in events[at(steps - 1) :]:
                event()
            finish()

    return before, after


def gather_kernel(ring, plan, *refs):
    arrays = len(plan["shapes"])
    run_steps(*gather_steps(ring, plan, refs[:arrays], refs[arrays : 2 * arrays], *refs[2 * arrays :]))


def gather_units(shards, plan, ring):
    devices = ring * 8
    return pl.pallas_call(
        partial(gather_kernel, ring, plan),
        out_shape=[
            jax.ShapeDtypeStruct((devices,) + shard.shape, shard.dtype) for shard in shards
        ],
        in_specs=[VMEM_SPEC] * len(shards),
        out_specs=[ANY_SPEC] * len(shards),
        scratch_shapes=gather_scratch(plan, devices - 1),
        compiler_params=pltpu.CompilerParams(collective_id=0, has_side_effects=True),
        name="gather_units",
    )(*shards)


def scatter_steps(ring, plan, grads, outs, scratch):
    shapes = plan["shapes"]
    arrays = len(shapes)
    parts = plan["parts"]
    owns = scratch[:arrays]
    lands = scratch[arrays : arrays + len(parts)]
    recv_sem, send_sem, local_sem = scratch[arrays + len(parts) :]
    place = Place(ring)

    def window(ref, part):
        _, first, count, _ = parts[part]
        return ref if count is None else ref.at[:, pl.ds(first, count)]

    def copy(part, index, source):
        way = parts[part][3][index][2]
        return pltpu.make_async_remote_copy(
            src_ref=source,
            dst_ref=lands[part].at[index],
            send_sem=send_sem.at[part],
            recv_sem=recv_sem.at[part, index],
            device_id=(place.neighbour(way, back=True),),
            device_id_type=MESH_ID,
        )

    def own_copy(array):
        return pltpu.make_async_copy(
            grads[array].at[:, place.core], owns[array], local_sem.at[array]
        )

    deepest = max(edge[3] for part in parts for edge in part[3])

    def begin():
        for array in range(arrays):
            own_copy(array).start()
        enter(place)
        for depth in range(deepest, 0, -1):
            for part, (array, _, _, tree) in enumerate(parts):
                for index, (_, child, way, level) in enumerate(tree):
                    if way == "core" and level == depth:
                        chip = place.chip_of(child)
                        source = grads[array].at[chip, place.flip(place.core, 1)]
                        copy(part, index, window(source, part)).start()
        for array in range(arrays):
            own_copy(array).wait()

    def add_up(part, node, target):
        array, first, count, tree = parts[part]
        children = [index for index, edge in enumerate(tree) if edge[0] == node]
        for index in children:
            copy(part, index, lands[part].at[index]).wait_recv()
        chip = place.chip_of(node)
        rows, columns = shapes[array]
        if count is not None:
            columns = count
        step = columns
        while rows * step > 24 * 768 and step % 256 == 0:
            step //= 2
        own = owns[array]

        def body(block, carry):
            here = pl.ds(pl.multiple_of(block * step, 128), step)
            where = pl.ds(pl.multiple_of(first + block * step, 128), step)
            kind = own.dtype if target is None else jnp.float32
            total = own[chip, :, where].astype(kind)
            for index in children:
                total = total + lands[part][index, :, here].astype(kind)
            if target is None:
                own[chip, :, where] = total
            else:
                target[:, where] = total
            return carry

        lax.fori_loop(0, columns // step, body, 0)

    inner = [
        (part, index)
        for depth in range(deepest, 0, -1)
        for part in range(len(parts))
        for index, edge in enumerate(parts[part][3])
        if edge[2] != "core" and edge[3] == depth
    ]

    def send(part, index):
        array, _, _, tree = parts[part]
        own = owns[array].at[place.chip_of(tree[index][1])]
        copy(part, index, window(own, part)).start()

    def add_then_send(number):
        part, index = inner[number]
        add_up(part, parts[part][3][index][1], None)
        if number:
            send(*inner[number - 1])

    events = [partial(add_then_send, number) for number in range(len(inner))]

    def finish():
        send(*inner[-1])
        for part in range(len(parts)):
            add_up(part, (0, 0, 0, 0), outs[parts[part][0]])
        for part in range(len(parts)):
            pltpu.make_async_copy(lands[part], lands[part], send_sem.at[part]).wait()

    return begin, events, finish


def scatter_scratch(plan, devices):
    shapes = plan["shapes"]
    edges = devices - 1
    lands = []
    for array, _, count, _ in plan["parts"]:
        rows, columns = shapes[array]
        lands.append(
            pltpu.VMEM((edges, rows, columns if count is None else count), jnp.bfloat16)
        )
    owns = [pltpu.VMEM((devices // 2,) + shape, jnp.bfloat16) for shape in shapes]
    return owns + lands + gather_scratch(plan, edges)


def scatter_kernel(ring, plan, *refs):
    arrays = len(plan["shapes"])
    run_steps(
        *scatter_steps(ring, plan, refs[:arrays], refs[arrays : 2 * arrays], refs[2 * arrays :])
    )


def by_owner(grads, shapes, devices):
    return [grad.reshape((devices // 2, 2) + shape) for grad, shape in zip(grads, shapes)]


def scatter_units(grads, plan, ring):
    devices = ring * 8
    shapes = plan["shapes"]
    return pl.pallas_call(
        partial(scatter_kernel, ring, plan),
        out_shape=[jax.ShapeDtypeStruct(shape, jnp.float32) for shape in shapes],
        in_specs=[ANY_SPEC] * len(shapes),
        out_specs=[VMEM_SPEC] * len(shapes),
        scratch_shapes=scatter_scratch(plan, devices),
        compiler_params=pltpu.CompilerParams(
            collective_id=1, has_side_effects=True, vmem_limit_bytes=VMEM_LIMIT
        ),
        name="scatter_units",
    )(*by_owner(grads, shapes, devices))


def make_plan(shapes, ring, mixed):
    trees = [make_tree(ring, first, flip) for first in (True, False) for flip in (False, True)]
    parts = []
    for array, (_, columns) in enumerate(shapes):
        flip = array % 2
        late = columns // 512 * 128 if columns > 768 and mixed == 2 else 0
        if shapes[array][0] > 32 and mixed:
            late = columns // 3
        if late:
            parts.append((array, 0, columns - late, trees[flip]))
            parts.append((array, columns - late, late, trees[2 + flip]))
        else:
            parts.append((array, 0, None, trees[flip]))
    return {"shapes": shapes, "parts": parts}


def dot_nt(left, right):
    return lax.dot_general(
        left, right, (((1,), (1,)), ((), ())), preferred_element_type=jnp.float32
    )


def dot_tn(left, right):
    return lax.dot_general(
        left, right, (((0,), (0,)), ((), ())), preferred_element_type=jnp.float32
    )


def dot_nn(left, right):
    return jnp.dot(left, right, preferred_element_type=jnp.float32)


def attend_kernel(lengths_ref, q_ref, k_ref, v_ref, context_ref, log_ref):
    rows, width = q_ref.shape
    length = lengths_ref[pl.program_id(0)]
    lane = lax.broadcasted_iota(jnp.int32, (rows, width), 1)
    inside = lax.broadcasted_iota(jnp.int32, (rows, width), 0) < length
    bias = jnp.where(lax.broadcasted_iota(jnp.int32, (1, rows), 1) < length, 0.0, -1e30)
    queries, keys, values = q_ref[...] * 0.125, k_ref[...], v_ref[...]
    context = jnp.zeros((rows, width), jnp.float32)
    logs = context
    for head in range(width // HEAD_DIM):
        mine = lane // HEAD_DIM == head
        scores = dot_nt(jnp.where(mine, queries, jnp.zeros_like(queries)), keys) + bias
        top = jnp.max(scores, axis=-1, keepdims=True)
        weights = jnp.exp(scores - top).astype(jnp.bfloat16)
        sums = dot_nn(weights, jnp.where(mine, values, jnp.ones_like(values)))
        other = (width - 1) if head == 0 else 0
        total = sums[:, other : other + 1]
        context = jnp.where(mine, sums * (1.0 / total), context)
        logs = jnp.where(mine, top + jnp.log(total), logs)
    context_ref[...] = jnp.where(inside, context, values.astype(jnp.float32)).astype(
        context_ref.dtype
    )
    log_ref[...] = logs


def grid_step():
    return pl.program_id(0) * pl.num_programs(1) + pl.program_id(1)


def attend(qkv, lengths):
    rows, width3 = qkv.shape
    width = width3 // 3
    halves = lengths.shape[0]
    half = rows // halves
    pairs = width // 128

    def columns(which):
        return pl.BlockSpec((half, 128), lambda i, j, l: (i, which * pairs + j))

    return pl.pallas_call(
        attend_kernel,
        out_shape=[
            jax.ShapeDtypeStruct((rows, width), jnp.bfloat16),
            jax.ShapeDtypeStruct((rows, width), jnp.float32),
        ],
        grid_spec=pltpu.PrefetchScalarGridSpec(
            num_scalar_prefetch=1,
            grid=(halves, pairs),
            in_specs=[columns(0), columns(1), columns(2)],
            out_specs=[columns(0), columns(0)],
        ),
        compiler_params=pltpu.CompilerParams(vmem_limit_bytes=VMEM_LIMIT),
        name="attend",
    )(lengths, qkv, qkv, qkv)


def attend_back_kernel(
    lengths_ref, q_ref, k_ref, v_ref, context_ref, log_ref, g_ref, grad_ref, sums_ref
):
    rows, width = q_ref.shape
    heads = width // HEAD_DIM
    length = lengths_ref[pl.program_id(0)]
    lane = lax.broadcasted_iota(jnp.int32, (rows, width), 1)
    inside = lax.broadcasted_iota(jnp.int32, (rows, width), 0) < length
    bias = jnp.where(lax.broadcasted_iota(jnp.int32, (rows, 1), 0) < length, 0.0, -1e30)
    queries, keys, values = q_ref[...] * 0.125, k_ref[...], v_ref[...]
    keys_scaled = keys * 0.125
    zero = jnp.zeros_like(queries)
    grads = jnp.where(inside, g_ref[...], zero)
    product = grads.astype(jnp.float32) * context_ref[...].astype(jnp.float32)
    table = jnp.zeros((rows, width), jnp.float32)
    for head in range(heads):
        mine = lane // HEAD_DIM == head
        along = jnp.sum(jnp.where(mine, product, 0.0), axis=-1, keepdims=True)
        first = head * HEAD_DIM
        table = jnp.where(lane == head, log_ref[:, first : first + 1], table)
        table = jnp.where(lane == heads + head, along, table)
    table = jnp.transpose(table)
    grad_q = jnp.zeros((rows, width), jnp.float32)
    grad_k = grad_q
    grad_v = jnp.where(inside, 0.0, g_ref[...].astype(jnp.float32))
    for head in range(heads):
        mine = lane // HEAD_DIM == head
        queries_head = jnp.where(mine, queries, zero)
        grads_head = jnp.where(mine, grads, zero)
        scores = dot_nt(keys, queries_head) + bias
        probs = jnp.exp(scores - table[head : head + 1])
        grad_v = grad_v + dot_nn(probs.astype(jnp.bfloat16), grads_head)
        grad_probs = dot_nt(values, grads_head)
        grad_scores = (probs * (grad_probs - table[heads + head : heads + head + 1])).astype(
            jnp.bfloat16
        )
        grad_k = grad_k + dot_nn(grad_scores, queries_head)
        grad_q = grad_q + dot_tn(grad_scores, jnp.where(mine, keys_scaled, zero))
    for place, grad in enumerate((grad_q, grad_k, grad_v)):
        grad_ref[place] = grad.astype(grad_ref.dtype)
        sums_ref[0, place] = jnp.sum(grad, axis=0, keepdims=True)


def attend_scatter_kernel(ring, plan, steps, lengths_ref, *refs):
    arrays = len(plan["shapes"])
    grads = refs[6 : 6 + arrays]
    outs = refs[8 + arrays : 8 + 2 * arrays]
    moves = scatter_steps(ring, plan, grads, outs, refs[8 + 2 * arrays :])
    before, after = spread_steps(grid_step(), steps, 1, 5, *moves)
    before()
    attend_back_kernel(lengths_ref, *refs[:6], *refs[6 + arrays : 8 + arrays])
    after()


def attend_back(qkv, context, logs, grad_context, lengths, grads, ring):
    rows, width3 = qkv.shape
    width = width3 // 3
    halves = lengths.shape[0]
    half = rows // halves
    pairs = width // 128

    def columns(which):
        return pl.BlockSpec((half, 128), lambda i, j, l: (i, which * pairs + j))

    params = {"vmem_limit_bytes": VMEM_LIMIT}
    kernel, scratch, more = attend_back_kernel, [], []
    if grads:
        devices = ring * 8
        shapes = [(grad.shape[0] // devices, grad.shape[1]) for grad in grads]
        plan = make_plan(shapes, ring, 2)
        kernel = partial(attend_scatter_kernel, ring, plan, halves * pairs)
        scratch = scatter_scratch(plan, devices)
        more = [jax.ShapeDtypeStruct(shape, jnp.float32) for shape in shapes]
        params.update(collective_id=3, has_side_effects=True)
        grads = by_owner(grads, shapes, devices)
    return pl.pallas_call(
        kernel,
        out_shape=[
            jax.ShapeDtypeStruct((3, rows, width), jnp.bfloat16),
            jax.ShapeDtypeStruct((halves, 3, 1, width), jnp.float32),
        ]
        + more,
        grid_spec=pltpu.PrefetchScalarGridSpec(
            num_scalar_prefetch=1,
            grid=(halves, pairs),
            in_specs=[columns(0), columns(1), columns(2)]
            + [columns(0)] * 3
            + [ANY_SPEC] * len(grads),
            out_specs=[
                pl.BlockSpec((3, half, 128), lambda i, j, l: (0, i, j)),
                pl.BlockSpec((1, 3, 1, 128), lambda i, j, l: (i, 0, 0, j)),
            ]
            + [VMEM_SPEC] * len(more),
            scratch_shapes=scratch,
        ),
        compiler_params=pltpu.CompilerParams(**params),
        name="attend_back",
    )(lengths, qkv, qkv, qkv, context, logs, grad_context, *grads)


LOG2_E = 1.4426950408889634


def gelu_parts(u):
    under = 1.0 + jnp.abs(u) * (0.3275911 * 0.7071067811865476)
    t = pl.reciprocal(under, approx=True)
    t = t * (2.0 - under * t)
    decay = jnp.exp2(u * u * (-0.5 * LOG2_E))
    poly = 0.5 * 1.061405429
    for term in (-1.453152027, 1.421413741, -0.284496736, 0.254829592):
        poly = poly * t + 0.5 * term
    tail = poly * t * decay
    cdf = jnp.where(u < 0, tail, 1.0 - tail)
    return u * cdf, cdf + u * (decay * 0.3989422804014327)


def up_kernel(first_ref, w_ref, b_ref, active_ref, slope_ref):
    rows = first_ref.shape[0]
    step = 128
    for start in range(0, rows, step):
        where = pl.ds(start, step)
        u = dot_nn(first_ref[where, :], w_ref[...]) + b_ref[...]
        value, slope = gelu_parts(u)
        active_ref[where, :] = value.astype(active_ref.dtype)
        slope_ref[where, :] = slope.astype(slope_ref.dtype)


def up_project(first_low, w_up, b_up):
    rows, width = first_low.shape
    hidden = w_up.shape[1]
    block = 512
    return pl.pallas_call(
        up_kernel,
        out_shape=[jax.ShapeDtypeStruct((rows, hidden), jnp.bfloat16)] * 2,
        grid=(hidden // block,),
        in_specs=[
            pl.BlockSpec((rows, width), lambda j: (0, 0)),
            pl.BlockSpec((width, block), lambda j: (0, j)),
            pl.BlockSpec((1, block), lambda j: (0, j)),
        ],
        out_specs=[pl.BlockSpec((rows, block), lambda j: (0, j))] * 2,
        compiler_params=pltpu.CompilerParams(vmem_limit_bytes=VMEM_LIMIT),
        name="up_project",
    )(first_low, w_up, b_up.reshape(1, hidden))


def norm_parts(hidden):
    center = hidden - jnp.mean(hidden, axis=-1, keepdims=True)
    inverse = lax.rsqrt(jnp.mean(center * center, axis=-1, keepdims=True) + 1e-12)
    return (center * inverse, inverse)


def norm_back(grad_out, normed, inverse, gain):
    scaled = grad_out * gain
    centered = scaled - jnp.mean(scaled, axis=-1, keepdims=True)
    return inverse * (centered - normed * jnp.mean(scaled * normed, axis=-1, keepdims=True))


def order_rows(slots, lengths):
    count = slots.shape[0]
    half = count // 2
    row = jnp.arange(count, dtype=jnp.int32)
    first, second = lengths[0], lengths[1]
    twice = jnp.concatenate([slots, slots])
    hole = lax.dynamic_slice_in_dim(twice, second, count)
    later = lax.dynamic_slice_in_dim(twice, first + half, count)
    in_first, in_second = row < first, row - half < second
    inside = jnp.where(row < half, in_first, in_second)
    placed = jnp.where(
        row < half, jnp.where(in_first, slots, hole), jnp.where(in_second, later, slots)
    )
    return placed, inside


def gather_params(params, ring):
    (w_qkv, b_qv, w_out, b_out, g1, c1, w_up, b_up, w_down, b_down, g2, c2, w_proj) = params
    small = [b_qv, b_up, b_out, g1, c1, b_down, g2, c2]
    packed = jnp.concatenate(small)
    if ring is None:
        whole = [lax.all_gather(w, AXIS, axis=0, tiled=True) for w in (w_qkv, w_out, w_up, w_down)]
        proj = lax.all_gather(w_proj, AXIS, axis=0, tiled=True)
        few = lax.all_gather(packed, AXIS, axis=0)
    else:
        filled = jnp.pad(packed, (0, 1024 - packed.shape[0])).reshape(8, 128)
        shards = [w_qkv, w_out, w_up, w_down, jnp.concatenate([w_proj, filled], axis=0)]
        plan = make_plan([shard.shape for shard in shards], ring, 1)
        units = gather_units(shards, plan, ring)
        whole = [unit.reshape(-1, unit.shape[2]) for unit in units[:4]]
        rows = w_proj.shape[0]
        proj = units[4][:, :rows].reshape(-1, w_proj.shape[1])
        few = units[4][:, rows:].reshape(units[4].shape[0], -1)
    vectors = []
    start = 0
    for entry in small:
        size = entry.shape[0]
        vectors.append(few[:, start : start + size].reshape(-1).astype(jnp.float32))
        start += size
    return whole + [proj], vectors


def scatter_grads(weights, vectors, ring, devices):
    few = [vector.reshape(devices, -1) for vector in vectors]
    sizes = [entry.shape[1] for entry in few]
    few = jnp.concatenate(few, axis=1)

    def native(w):
        return lax.psum_scatter(w, AXIS, scatter_dimension=0, tiled=True).astype(jnp.float32)

    if ring is None:
        shards = [native(w) for w in weights]
        small = lax.psum_scatter(few.reshape(-1), AXIS, scatter_dimension=0, tiled=True)
    else:
        few = jnp.pad(few, ((0, 0), (0, 1024 - few.shape[1]))).astype(jnp.bfloat16)
        units = [w.reshape(devices, -1, w.shape[1]) for w in weights[:2] + weights[4:]]
        rows = units[2].shape[1]
        units[2] = jnp.concatenate([units[2], few.reshape(devices, 8, 128)], axis=1)
        plan = make_plan([unit.shape[1:] for unit in units], ring, 0)
        shards = list(scatter_units(units, plan, ring))
        small = shards[2][rows:].reshape(-1)
        shards = shards[:2] + weights[2:4] + [shards[2][:rows]]
    pieces = []
    start = 0
    for size in sizes:
        pieces.append(small[start : start + size])
        start += size
    return shards, pieces


def local(tokens, cotangent, slot_row, lengths, *params):
    devices = lax.axis_size(AXIS)
    row_count, model_width = tokens.shape
    peer_rows = row_count // devices
    ring = devices // 8 if params[0].shape[0] % 8 == 0 and devices % 8 == 0 else None
    (w_qkv, w_out, w_up, w_down, w_proj), vectors = gather_params(params, ring)
    b_qv, b_up, b_out, gain_one, bias_one, b_down, gain_two, bias_two = vectors

    local_row, inside = order_rows(
        slot_row // row_count * peer_rows + slot_row % peer_rows, lengths
    )
    both = jnp.concatenate([tokens, cotangent], axis=1)
    arrived = lax.all_to_all(both, AXIS, split_axis=0, concat_axis=0, tiled=True)
    chosen = local_row[:, None] == jnp.arange(row_count, dtype=jnp.int32)[None, :]
    chosen = chosen.astype(jnp.bfloat16)
    dealt = dot_nn(chosen, arrived[:, :model_width]).astype(jnp.bfloat16)
    dealt_cot = dot_nn(chosen, arrived[:, model_width:]).astype(jnp.bfloat16)
    valid = inside[:, None].astype(jnp.float32)

    bias_all = jnp.concatenate(
        [b_qv[:model_width], jnp.zeros((model_width,), jnp.float32), b_qv[model_width:]]
    )
    qkv = (dot_nn(dealt, w_qkv) + bias_all).astype(jnp.bfloat16)
    context, logs = attend(qkv, lengths)
    hidden_one = dealt.astype(jnp.float32) + dot_nn(context, w_out) + b_out
    normed_one, inverse_one = norm_parts(hidden_one)
    first_low = (normed_one * gain_one + bias_one).astype(jnp.bfloat16)
    active, slope = up_project(first_low, w_up, b_up)
    hidden_two = first_low.astype(jnp.float32) + dot_nn(active, w_down) + b_down
    normed_two, inverse_two = norm_parts(hidden_two)
    second_low = (normed_two * gain_two + bias_two).astype(jnp.bfloat16)
    project = dot_nn(second_low, w_proj)
    inv_norm = lax.rsqrt(jnp.sum(project * project, axis=-1, keepdims=True) + 1e-06)
    embedded = (project * inv_norm * valid).astype(jnp.bfloat16)

    grad_emb = dealt_cot.astype(jnp.float32) * valid
    along = jnp.sum(project * grad_emb, axis=-1, keepdims=True)
    grad_project = (inv_norm * grad_emb - inv_norm * inv_norm * inv_norm * along * project).astype(
        jnp.bfloat16
    )
    grad_w_proj = dot_tn(second_low, grad_project).astype(jnp.bfloat16)
    grad_second = dot_nt(grad_project, w_proj)
    grad_gain_two = jnp.sum(grad_second * normed_two, axis=0)
    grad_bias_two = jnp.sum(grad_second, axis=0)
    grad_hidden_two = norm_back(grad_second, normed_two, inverse_two, gain_two)
    grad_b_down = jnp.sum(grad_hidden_two, axis=0)
    down_low = grad_hidden_two.astype(jnp.bfloat16)
    grad_w_down = dot_tn(active, down_low).astype(jnp.bfloat16)
    grad_up = dot_nt(down_low, w_down) * slope.astype(jnp.float32)
    grad_b_up = jnp.sum(grad_up, axis=0)
    up_low = grad_up.astype(jnp.bfloat16)
    grad_w_up = dot_tn(first_low, up_low).astype(jnp.bfloat16)
    grad_first = grad_hidden_two + dot_nt(up_low, w_up)
    grad_gain_one = jnp.sum(grad_first * normed_one, axis=0)
    grad_bias_one = jnp.sum(grad_first, axis=0)
    grad_hidden_one = norm_back(grad_first, normed_one, inverse_one, gain_one)
    grad_b_out = jnp.sum(grad_hidden_one, axis=0)
    out_low = grad_hidden_one.astype(jnp.bfloat16)
    grad_w_out = dot_tn(context, out_low).astype(jnp.bfloat16)
    grad_context = dot_nt(out_low, w_out).astype(jnp.bfloat16)
    large = [grad_w_up, grad_w_down] if ring else []
    grad_three, sums, *large = attend_back(
        qkv, context, logs, grad_context, lengths, large, ring
    )
    if ring:
        grad_w_up, grad_w_down = large
    sums = jnp.sum(sums, axis=0)[:, 0]
    grad_b_qv = jnp.concatenate([sums[0], sums[2]])
    grad_qkv = jnp.concatenate([grad_three[0], grad_three[1], grad_three[2]], axis=1)
    grad_w_qkv = dot_tn(dealt, grad_qkv).astype(jnp.bfloat16)
    grad_dealt = (dot_nt(grad_qkv, w_qkv) + grad_hidden_one).astype(jnp.bfloat16)

    back = jnp.concatenate([grad_dealt, embedded], axis=1)
    back = dot_tn(chosen, back).astype(jnp.bfloat16)
    returned = lax.all_to_all(back, AXIS, split_axis=0, concat_axis=0, tiled=True)
    shards, small = scatter_grads(
        [grad_w_qkv, grad_w_out, grad_w_up, grad_w_down, grad_w_proj],
        [
            grad_b_qv,
            grad_b_up,
            grad_b_out,
            grad_gain_one,
            grad_bias_one,
            grad_b_down,
            grad_gain_two,
            grad_bias_two,
        ],
        ring,
        devices,
    )
    return (
        returned[:, model_width:],
        returned[:, :model_width],
        shards[0],
        small[0],
        shards[1],
        small[2],
        small[3],
        small[4],
        shards[2],
        small[1],
        shards[3],
        small[5],
        small[6],
        small[7],
        shards[4],
    )


def solution(mesh):
    matrix, vector = P(AXIS, None), P(AXIS)
    params = "mvmvvvmvmvvvm"
    in_kinds = "mmvv" + params
    out_kinds = "mm" + params
    specs = {"m": matrix, "v": vector}

    return jax.shard_map(
        local,
        mesh=mesh,
        in_specs=tuple(specs[kind] for kind in in_kinds),
        out_specs=tuple(specs[kind] for kind in out_kinds),
        check_vma=False,
    )
```

```python
from functools import partial

import jax
import jax.numpy as jnp
from jax import lax
from jax.experimental import pallas as pl
from jax.experimental.pallas import tpu as pltpu
from jax.sharding import PartitionSpec as P


HEAD_DIM = 64
AXIS = "fsdp"
MESH_ID = pl.DeviceIdType.MESH
VMEM_SPEC = pl.BlockSpec(memory_space=pltpu.VMEM)
ANY_SPEC = pl.BlockSpec(memory_space=pl.ANY)
VMEM_LIMIT = 60 * 1024 * 1024


def chain_edges(node, ring, lean_up):
    up_count = ring // 2 if lean_up else (ring - 1) // 2
    edges = []
    here = node
    for _ in range(up_count):
        there = ((here[0] + 1) % ring,) + here[1:]
        edges.append((here, there, "up"))
        here = there
    here = node
    for _ in range(ring - 1 - up_count):
        there = ((here[0] - 1) % ring,) + here[1:]
        edges.append((here, there, "down"))
        here = there
    return edges


def plane_edges(node, x_first):
    z = node[0]
    own, by_x, by_y, both = (z, 0, 0, 0), (z, 0, 1, 0), (z, 1, 0, 0), (z, 1, 1, 0)
    edges = [(own, by_x, "x"), (own, by_y, "y")]
    edges.append((by_x, both, "y") if x_first else (by_y, both, "x"))
    return edges


def make_tree(ring, ring_first, flip):
    root = (0, 0, 0, 0)
    edges = []
    if ring_first:
        edges += chain_edges(root, ring, flip)
        nodes = [root] + [edge[1] for edge in edges]
        for place, node in enumerate(nodes):
            edges += plane_edges(node, (place % 2 == 0) != flip)
    else:
        edges += plane_edges(root, flip)
        nodes = [root] + [edge[1] for edge in edges]
        for place, node in enumerate(nodes):
            edges += chain_edges(node, ring, (place % 2 == 0) != flip)
    nodes = [root] + [edge[1] for edge in edges]
    edges += [(node, node[:3] + (1,), "core") for node in nodes]
    depth = {root: 0}
    for parent, child, _ in edges:
        depth[child] = depth[parent] + 1
    order = sorted(range(len(edges)), key=lambda index: depth[edges[index][1]])
    return [edges[index] + (depth[edges[index][1]],) for index in order]


class Place:
    def __init__(self, ring):
        me = lax.axis_index(AXIS)
        self.ring = ring
        self.me = me
        self.core = lax.rem(me, 2)
        self.x = lax.rem(me // 2, 2)
        self.y = lax.rem(me // 4, 2)
        self.z = me // 8

    @staticmethod
    def flip(value, amount):
        return 1 - value if amount else value

    def chip_of(self, offset):
        z = lax.rem(self.z + (self.ring - offset[0]) % self.ring, self.ring)
        return (z * 2 + self.flip(self.y, offset[1])) * 2 + self.flip(self.x, offset[2])

    def unit_of(self, offset):
        return self.chip_of(offset) * 2 + self.flip(self.core, offset[3])

    def neighbour(self, way, back=False):
        step = {"up": (1, 0, 0, 0), "down": (-1, 0, 0, 0), "x": (0, 0, 1, 0)}
        step.update({"y": (0, 1, 0, 0), "core": (0, 0, 0, 1)})
        offset = step[way]
        dz = offset[0] if back else -offset[0]
        return self.unit_of((dz % self.ring,) + offset[1:])


def enter(place):
    barrier = pltpu.get_barrier_semaphore()
    for way in ("up", "down", "x", "y", "core"):
        pl.semaphore_signal(
            barrier, inc=1, device_id=(place.neighbour(way),), device_id_type=MESH_ID
        )
    pl.semaphore_wait(barrier, 5)


def gather_steps(ring, plan, shards, outs, recv_sem, send_sem, local_sem):
    arrays = len(shards)
    place = Place(ring)
    parts = plan["parts"]

    def window(ref, part):
        _, first, count, _ = parts[part]
        return ref if count is None else ref.at[:, pl.ds(first, count)]

    def copy(part, index):
        array, _, _, tree = parts[part]
        parent, _, way, _ = tree[index]
        unit = place.unit_of(parent)
        source = shards[array] if parent == (0, 0, 0, 0) else outs[array].at[unit]
        return pltpu.make_async_remote_copy(
            src_ref=window(source, part),
            dst_ref=window(outs[array].at[unit], part),
            send_sem=send_sem.at[part],
            recv_sem=recv_sem.at[part, index],
            device_id=(place.neighbour(way),),
            device_id_type=MESH_ID,
        )

    def arrived(part, index):
        array, _, _, tree = parts[part]
        _, child, way, _ = tree[index]
        landed = window(outs[array].at[place.unit_of(child)], part)
        pltpu.make_async_remote_copy(
            src_ref=landed,
            dst_ref=landed,
            send_sem=send_sem.at[part],
            recv_sem=recv_sem.at[part, index],
            device_id=(place.neighbour(way),),
            device_id_type=MESH_ID,
        ).wait_recv()

    def send_from(part, node):
        for index, edge in enumerate(parts[part][3]):
            if edge[0] == node:
                copy(part, index).start()

    def own_copy(array):
        return pltpu.make_async_copy(shards[array], outs[array].at[place.me], local_sem.at[array])

    def begin():
        for array in range(arrays):
            own_copy(array).start()
        enter(place)
        for part in range(len(parts)):
            send_from(part, (0, 0, 0, 0))

    def pass_on(part, index):
        arrived(part, index)
        send_from(part, parts[part][3][index][1])

    events = []
    deepest = max(edge[3] for part in parts for edge in part[3])
    for depth in range(1, deepest + 1):
        for part in range(len(parts)):
            for index, edge in enumerate(parts[part][3]):
                if edge[3] == depth and edge[2] != "core":
                    events.append(partial(pass_on, part, index))

    def finish():
        for part in range(len(parts)):
            for index, edge in enumerate(parts[part][3]):
                if edge[2] == "core":
                    arrived(part, index)
        for array in range(arrays):
            own_copy(array).wait()
        for part, (array, first, count, tree) in enumerate(parts):
            whole = outs[array].at[pl.ds(0, len(tree))]
            if count is not None:
                whole = whole.at[:, :, pl.ds(first, count)]
            pltpu.make_async_copy(whole, whole, send_sem.at[part]).wait()

    return begin, events, finish


def gather_scratch(plan, edges):
    return [
        pltpu.SemaphoreType.DMA((len(plan["parts"]), edges)),
        pltpu.SemaphoreType.DMA((len(plan["parts"]),)),
        pltpu.SemaphoreType.DMA((len(plan["shapes"]),)),
    ]


def run_steps(begin, events, finish):
    begin()
    for event in events:
        event()
    finish()


def spread_steps(step, steps, lag, pace, begin, events, finish):
    def at(number):
        return max(0, min(len(events), (number - lag + 1) * pace))

    def handle(number):
        for event in events[at(number - 1) : at(number)]:
            event()

    def before():
        pl.when(step == 0)(begin)
        for number in range(1, steps):
            if at(number) > at(number - 1):
                pl.when(step == number)(partial(handle, number))

    def after():
        @pl.when(step == steps - 1)
        def _():
            for event in events[at(steps - 1) :]:
                event()
            finish()

    return before, after


def gather_kernel(ring, plan, *refs):
    arrays = len(plan["shapes"])
    run_steps(*gather_steps(ring, plan, refs[:arrays], refs[arrays : 2 * arrays], *refs[2 * arrays :]))


def gather_units(shards, plan, ring):
    devices = ring * 8
    return pl.pallas_call(
        partial(gather_kernel, ring, plan),
        out_shape=[
            jax.ShapeDtypeStruct((devices,) + shard.shape, shard.dtype) for shard in shards
        ],
        in_specs=[VMEM_SPEC] * len(shards),
        out_specs=[ANY_SPEC] * len(shards),
        scratch_shapes=gather_scratch(plan, devices - 1),
        compiler_params=pltpu.CompilerParams(collective_id=0, has_side_effects=True),
        name="gather_units",
    )(*shards)


def scatter_steps(ring, plan, grads, outs, scratch):
    shapes = plan["shapes"]
    arrays = len(shapes)
    parts = plan["parts"]
    owns = scratch[:arrays]
    lands = scratch[arrays : arrays + len(parts)]
    recv_sem, send_sem, local_sem = scratch[arrays + len(parts) :]
    place = Place(ring)

    def window(ref, part):
        _, first, count, _ = parts[part]
        return ref if count is None else ref.at[:, pl.ds(first, count)]

    def copy(part, index, source):
        way = parts[part][3][index][2]
        return pltpu.make_async_remote_copy(
            src_ref=source,
            dst_ref=lands[part].at[index],
            send_sem=send_sem.at[part],
            recv_sem=recv_sem.at[part, index],
            device_id=(place.neighbour(way, back=True),),
            device_id_type=MESH_ID,
        )

    def own_copy(array):
        return pltpu.make_async_copy(
            grads[array].at[:, place.core], owns[array], local_sem.at[array]
        )

    deepest = max(edge[3] for part in parts for edge in part[3])

    def begin():
        for array in range(arrays):
            own_copy(array).start()
        enter(place)
        for depth in range(deepest, 0, -1):
            for part, (array, _, _, tree) in enumerate(parts):
                for index, (_, child, way, level) in enumerate(tree):
                    if way == "core" and level == depth:
                        chip = place.chip_of(child)
                        source = grads[array].at[chip, place.flip(place.core, 1)]
                        copy(part, index, window(source, part)).start()
        for array in range(arrays):
            own_copy(array).wait()

    def add_up(part, node, target):
        array, first, count, tree = parts[part]
        children = [index for index, edge in enumerate(tree) if edge[0] == node]
        for index in children:
            copy(part, index, lands[part].at[index]).wait_recv()
        chip = place.chip_of(node)
        rows, columns = shapes[array]
        if count is not None:
            columns = count
        step = columns
        while rows * step > 24 * 768 and step % 256 == 0:
            step //= 2
        own = owns[array]

        def body(block, carry):
            here = pl.ds(pl.multiple_of(block * step, 128), step)
            where = pl.ds(pl.multiple_of(first + block * step, 128), step)
            kind = own.dtype if target is None else jnp.float32
            total = own[chip, :, where].astype(kind)
            for index in children:
                total = total + lands[part][index, :, here].astype(kind)
            if target is None:
                own[chip, :, where] = total
            else:
                target[:, where] = total
            return carry

        lax.fori_loop(0, columns // step, body, 0)

    inner = [
        (part, index)
        for depth in range(deepest, 0, -1)
        for part in range(len(parts))
        for index, edge in enumerate(parts[part][3])
        if edge[2] != "core" and edge[3] == depth
    ]

    def send(part, index):
        array, _, _, tree = parts[part]
        own = owns[array].at[place.chip_of(tree[index][1])]
        copy(part, index, window(own, part)).start()

    def add_then_send(number):
        part, index = inner[number]
        add_up(part, parts[part][3][index][1], None)
        if number:
            send(*inner[number - 1])

    events = [partial(add_then_send, number) for number in range(len(inner))]

    def finish():
        send(*inner[-1])
        for part in range(len(parts)):
            add_up(part, (0, 0, 0, 0), outs[parts[part][0]])
        for part in range(len(parts)):
            pltpu.make_async_copy(lands[part], lands[part], send_sem.at[part]).wait()

    return begin, events, finish


def scatter_scratch(plan, devices):
    shapes = plan["shapes"]
    edges = devices - 1
    lands = []
    for array, _, count, _ in plan["parts"]:
        rows, columns = shapes[array]
        lands.append(
            pltpu.VMEM((edges, rows, columns if count is None else count), jnp.bfloat16)
        )
    owns = [pltpu.VMEM((devices // 2,) + shape, jnp.bfloat16) for shape in shapes]
    return owns + lands + gather_scratch(plan, edges)


def scatter_kernel(ring, plan, *refs):
    arrays = len(plan["shapes"])
    run_steps(
        *scatter_steps(ring, plan, refs[:arrays], refs[arrays : 2 * arrays], refs[2 * arrays :])
    )


def by_owner(grads, shapes, devices):
    return [grad.reshape((devices // 2, 2) + shape) for grad, shape in zip(grads, shapes)]


def scatter_units(grads, plan, ring):
    devices = ring * 8
    shapes = plan["shapes"]
    return pl.pallas_call(
        partial(scatter_kernel, ring, plan),
        out_shape=[jax.ShapeDtypeStruct(shape, jnp.float32) for shape in shapes],
        in_specs=[ANY_SPEC] * len(shapes),
        out_specs=[VMEM_SPEC] * len(shapes),
        scratch_shapes=scatter_scratch(plan, devices),
        compiler_params=pltpu.CompilerParams(
            collective_id=1, has_side_effects=True, vmem_limit_bytes=VMEM_LIMIT
        ),
        name="scatter_units",
    )(*by_owner(grads, shapes, devices))


def make_plan(shapes, ring, mixed):
    trees = [make_tree(ring, first, flip) for first in (True, False) for flip in (False, True)]
    parts = []
    for array, (_, columns) in enumerate(shapes):
        flip = array % 2
        late = columns // 512 * 128 if columns > 768 else 0
        if shapes[array][0] > 32:
            late = columns // 3
        if late and mixed:
            parts.append((array, 0, columns - late, trees[flip]))
            parts.append((array, columns - late, late, trees[2 + flip]))
        else:
            parts.append((array, 0, None, trees[flip]))
    return {"shapes": shapes, "parts": parts}


def dot_nt(left, right):
    return lax.dot_general(
        left, right, (((1,), (1,)), ((), ())), preferred_element_type=jnp.float32
    )


def dot_tn(left, right):
    return lax.dot_general(
        left, right, (((0,), (0,)), ((), ())), preferred_element_type=jnp.float32
    )


def dot_nn(left, right):
    return jnp.dot(left, right, preferred_element_type=jnp.float32)


def attend_kernel(lengths_ref, q_ref, k_ref, v_ref, context_ref, log_ref):
    rows, width = q_ref.shape
    length = lengths_ref[pl.program_id(0)]
    lane = lax.broadcasted_iota(jnp.int32, (rows, width), 1)
    inside = lax.broadcasted_iota(jnp.int32, (rows, width), 0) < length
    bias = jnp.where(lax.broadcasted_iota(jnp.int32, (1, rows), 1) < length, 0.0, -1e30)
    queries, keys, values = q_ref[...] * 0.125, k_ref[...], v_ref[...]
    context = jnp.zeros((rows, width), jnp.float32)
    logs = context
    for head in range(width // HEAD_DIM):
        mine = lane // HEAD_DIM == head
        scores = dot_nt(jnp.where(mine, queries, jnp.zeros_like(queries)), keys) + bias
        top = jnp.max(scores, axis=-1, keepdims=True)
        weights = jnp.exp(scores - top).astype(jnp.bfloat16)
        sums = dot_nn(weights, jnp.where(mine, values, jnp.ones_like(values)))
        other = (width - 1) if head == 0 else 0
        total = sums[:, other : other + 1]
        context = jnp.where(mine, sums * (1.0 / total), context)
        logs = jnp.where(mine, top + jnp.log(total), logs)
    context_ref[...] = jnp.where(inside, context, values.astype(jnp.float32)).astype(
        context_ref.dtype
    )
    log_ref[...] = logs


def grid_step():
    return pl.program_id(0) * pl.num_programs(1) + pl.program_id(1)


def attend_gather_kernel(ring, plan, steps, lengths_ref, q_ref, k_ref, v_ref, *refs):
    arrays = len(plan["shapes"])
    shards = refs[:arrays]
    context_ref, log_ref = refs[arrays : arrays + 2]
    outs = refs[arrays + 2 : 2 * arrays + 2]
    moves = gather_steps(ring, plan, shards, outs, *refs[2 * arrays + 2 :])
    before, after = spread_steps(grid_step(), steps, 3, 3, *moves)
    before()
    attend_kernel(lengths_ref, q_ref, k_ref, v_ref, context_ref, log_ref)
    after()


def attend(qkv, lengths, shards, ring):
    rows, width3 = qkv.shape
    width = width3 // 3
    halves = lengths.shape[0]
    half = rows // halves
    pairs = width // 128

    def columns(which):
        return pl.BlockSpec((half, 128), lambda i, j, l: (i, which * pairs + j))

    params = {"vmem_limit_bytes": VMEM_LIMIT}
    kernel, scratch, more = attend_kernel, [], []
    if shards:
        devices = ring * 8
        plan = make_plan([shard.shape for shard in shards], ring, True)
        kernel = partial(attend_gather_kernel, ring, plan, halves * pairs)
        scratch = gather_scratch(plan, devices - 1)
        more = [jax.ShapeDtypeStruct((devices,) + shard.shape, shard.dtype) for shard in shards]
        params.update(collective_id=2, has_side_effects=True)
    return pl.pallas_call(
        kernel,
        out_shape=[
            jax.ShapeDtypeStruct((rows, width), jnp.bfloat16),
            jax.ShapeDtypeStruct((rows, width), jnp.float32),
        ]
        + more,
        grid_spec=pltpu.PrefetchScalarGridSpec(
            num_scalar_prefetch=1,
            grid=(halves, pairs),
            in_specs=[columns(0), columns(1), columns(2)] + [VMEM_SPEC] * len(shards),
            out_specs=[columns(0), columns(0)] + [ANY_SPEC] * len(shards),
            scratch_shapes=scratch,
        ),
        compiler_params=pltpu.CompilerParams(**params),
        name="attend",
    )(lengths, qkv, qkv, qkv, *shards)


def attend_back_kernel(
    lengths_ref, q_ref, k_ref, v_ref, context_ref, log_ref, g_ref, grad_ref, sums_ref
):
    rows, width = q_ref.shape
    heads = width // HEAD_DIM
    length = lengths_ref[pl.program_id(0)]
    lane = lax.broadcasted_iota(jnp.int32, (rows, width), 1)
    inside = lax.broadcasted_iota(jnp.int32, (rows, width), 0) < length
    bias = jnp.where(lax.broadcasted_iota(jnp.int32, (rows, 1), 0) < length, 0.0, -1e30)
    queries, keys, values = q_ref[...] * 0.125, k_ref[...], v_ref[...]
    keys_scaled = keys * 0.125
    zero = jnp.zeros_like(queries)
    grads = jnp.where(inside, g_ref[...], zero)
    product = grads.astype(jnp.float32) * context_ref[...].astype(jnp.float32)
    table = jnp.zeros((rows, width), jnp.float32)
    for head in range(heads):
        mine = lane // HEAD_DIM == head
        along = jnp.sum(jnp.where(mine, product, 0.0), axis=-1, keepdims=True)
        first = head * HEAD_DIM
        table = jnp.where(lane == head, log_ref[:, first : first + 1], table)
        table = jnp.where(lane == heads + head, along, table)
    table = jnp.transpose(table)
    grad_q = jnp.zeros((rows, width), jnp.float32)
    grad_k = grad_q
    grad_v = jnp.where(inside, 0.0, g_ref[...].astype(jnp.float32))
    for head in range(heads):
        mine = lane // HEAD_DIM == head
        queries_head = jnp.where(mine, queries, zero)
        grads_head = jnp.where(mine, grads, zero)
        scores = dot_nt(keys, queries_head) + bias
        probs = jnp.exp(scores - table[head : head + 1])
        grad_v = grad_v + dot_nn(probs.astype(jnp.bfloat16), grads_head)
        grad_probs = dot_nt(values, grads_head)
        grad_scores = (probs * (grad_probs - table[heads + head : heads + head + 1])).astype(
            jnp.bfloat16
        )
        grad_k = grad_k + dot_nn(grad_scores, queries_head)
        grad_q = grad_q + dot_tn(grad_scores, jnp.where(mine, keys_scaled, zero))
    for place, grad in enumerate((grad_q, grad_k, grad_v)):
        grad_ref[place] = grad.astype(grad_ref.dtype)
        sums_ref[0, place] = jnp.sum(grad, axis=0, keepdims=True)


def attend_scatter_kernel(ring, plan, steps, lengths_ref, *refs):
    arrays = len(plan["shapes"])
    grads = refs[6 : 6 + arrays]
    outs = refs[8 + arrays : 8 + 2 * arrays]
    moves = scatter_steps(ring, plan, grads, outs, refs[8 + 2 * arrays :])
    before, after = spread_steps(grid_step(), steps, 1, 5, *moves)
    before()
    attend_back_kernel(lengths_ref, *refs[:6], *refs[6 + arrays : 8 + arrays])
    after()


def attend_back(qkv, context, logs, grad_context, lengths, grads, ring):
    rows, width3 = qkv.shape
    width = width3 // 3
    halves = lengths.shape[0]
    half = rows // halves
    pairs = width // 128

    def columns(which):
        return pl.BlockSpec((half, 128), lambda i, j, l: (i, which * pairs + j))

    params = {"vmem_limit_bytes": VMEM_LIMIT}
    kernel, scratch, more = attend_back_kernel, [], []
    if grads:
        devices = ring * 8
        shapes = [(grad.shape[0] // devices, grad.shape[1]) for grad in grads]
        plan = make_plan(shapes, ring, True)
        kernel = partial(attend_scatter_kernel, ring, plan, halves * pairs)
        scratch = scatter_scratch(plan, devices)
        more = [jax.ShapeDtypeStruct(shape, jnp.float32) for shape in shapes]
        params.update(collective_id=3, has_side_effects=True)
        grads = by_owner(grads, shapes, devices)
    return pl.pallas_call(
        kernel,
        out_shape=[
            jax.ShapeDtypeStruct((3, rows, width), jnp.bfloat16),
            jax.ShapeDtypeStruct((halves, 3, 1, width), jnp.float32),
        ]
        + more,
        grid_spec=pltpu.PrefetchScalarGridSpec(
            num_scalar_prefetch=1,
            grid=(halves, pairs),
            in_specs=[columns(0), columns(1), columns(2)]
            + [columns(0)] * 3
            + [ANY_SPEC] * len(grads),
            out_specs=[
                pl.BlockSpec((3, half, 128), lambda i, j, l: (0, i, j)),
                pl.BlockSpec((1, 3, 1, 128), lambda i, j, l: (i, 0, 0, j)),
            ]
            + [VMEM_SPEC] * len(more),
            scratch_shapes=scratch,
        ),
        compiler_params=pltpu.CompilerParams(**params),
        name="attend_back",
    )(lengths, qkv, qkv, qkv, context, logs, grad_context, *grads)


LOG2_E = 1.4426950408889634


def gelu_parts(u):
    under = 1.0 + jnp.abs(u) * (0.3275911 * 0.7071067811865476)
    t = pl.reciprocal(under, approx=True)
    t = t * (2.0 - under * t)
    decay = jnp.exp2(u * u * (-0.5 * LOG2_E))
    poly = 0.5 * 1.061405429
    for term in (-1.453152027, 1.421413741, -0.284496736, 0.254829592):
        poly = poly * t + 0.5 * term
    tail = poly * t * decay
    cdf = jnp.where(u < 0, tail, 1.0 - tail)
    return u * cdf, cdf + u * (decay * 0.3989422804014327)


def up_kernel(first_ref, w_ref, b_ref, active_ref, slope_ref):
    rows = first_ref.shape[0]
    step = 128
    for start in range(0, rows, step):
        where = pl.ds(start, step)
        u = dot_nn(first_ref[where, :], w_ref[...]) + b_ref[...]
        value, slope = gelu_parts(u)
        active_ref[where, :] = value.astype(active_ref.dtype)
        slope_ref[where, :] = slope.astype(slope_ref.dtype)


def up_project(first_low, w_up, b_up):
    rows, width = first_low.shape
    hidden = w_up.shape[1]
    block = 512
    return pl.pallas_call(
        up_kernel,
        out_shape=[jax.ShapeDtypeStruct((rows, hidden), jnp.bfloat16)] * 2,
        grid=(hidden // block,),
        in_specs=[
            pl.BlockSpec((rows, width), lambda j: (0, 0)),
            pl.BlockSpec((width, block), lambda j: (0, j)),
            pl.BlockSpec((1, block), lambda j: (0, j)),
        ],
        out_specs=[pl.BlockSpec((rows, block), lambda j: (0, j))] * 2,
        compiler_params=pltpu.CompilerParams(vmem_limit_bytes=VMEM_LIMIT),
        name="up_project",
    )(first_low, w_up, b_up.reshape(1, hidden))


def norm_parts(hidden):
    center = hidden - jnp.mean(hidden, axis=-1, keepdims=True)
    inverse = lax.rsqrt(jnp.mean(center * center, axis=-1, keepdims=True) + 1e-12)
    return (center * inverse, inverse)


def norm_back(grad_out, normed, inverse, gain):
    scaled = grad_out * gain
    centered = scaled - jnp.mean(scaled, axis=-1, keepdims=True)
    return inverse * (centered - normed * jnp.mean(scaled * normed, axis=-1, keepdims=True))


def order_rows(slots, lengths):
    count = slots.shape[0]
    half = count // 2
    row = jnp.arange(count, dtype=jnp.int32)
    first, second = lengths[0], lengths[1]
    twice = jnp.concatenate([slots, slots])
    hole = lax.dynamic_slice_in_dim(twice, second, count)
    later = lax.dynamic_slice_in_dim(twice, first + half, count)
    in_first, in_second = row < first, row - half < second
    inside = jnp.where(row < half, in_first, in_second)
    placed = jnp.where(
        row < half, jnp.where(in_first, slots, hole), jnp.where(in_second, later, slots)
    )
    return placed, inside


def gather_params(params, ring):
    (w_qkv, b_qv, w_out, b_out, g1, c1, w_up, b_up, w_down, b_down, g2, c2, w_proj) = params
    small = [b_qv, b_up, b_out, g1, c1, b_down, g2, c2]
    packed = jnp.concatenate(small)
    if ring is None:
        whole = [lax.all_gather(w, AXIS, axis=0, tiled=True) for w in (w_qkv, w_out, w_up, w_down)]
        proj = lax.all_gather(w_proj, AXIS, axis=0, tiled=True)
        few = lax.all_gather(packed, AXIS, axis=0)
    else:
        filled = jnp.pad(packed, (0, 1024 - packed.shape[0])).reshape(8, 128)
        shards = [w_qkv, w_out, jnp.concatenate([w_proj, filled], axis=0)]
        plan = make_plan([shard.shape for shard in shards], ring, False)
        units = gather_units(shards, plan, ring)
        whole = [unit.reshape(-1, unit.shape[2]) for unit in units[:2]] + [w_up, w_down]
        rows = w_proj.shape[0]
        proj = units[2][:, :rows].reshape(-1, w_proj.shape[1])
        few = units[2][:, rows:].reshape(units[2].shape[0], -1)
    vectors = []
    start = 0
    for entry in small:
        size = entry.shape[0]
        vectors.append(few[:, start : start + size].reshape(-1).astype(jnp.float32))
        start += size
    return whole + [proj], vectors


def scatter_grads(weights, vectors, ring, devices):
    few = [vector.reshape(devices, -1) for vector in vectors]
    sizes = [entry.shape[1] for entry in few]
    few = jnp.concatenate(few, axis=1)

    def native(w):
        return lax.psum_scatter(w, AXIS, scatter_dimension=0, tiled=True).astype(jnp.float32)

    if ring is None:
        shards = [native(w) for w in weights]
        small = lax.psum_scatter(few.reshape(-1), AXIS, scatter_dimension=0, tiled=True)
    else:
        few = jnp.pad(few, ((0, 0), (0, 1024 - few.shape[1]))).astype(jnp.bfloat16)
        units = [w.reshape(devices, -1, w.shape[1]) for w in weights[:2] + weights[4:]]
        rows = units[2].shape[1]
        units[2] = jnp.concatenate([units[2], few.reshape(devices, 8, 128)], axis=1)
        plan = make_plan([unit.shape[1:] for unit in units], ring, False)
        shards = list(scatter_units(units, plan, ring))
        small = shards[2][rows:].reshape(-1)
        shards = shards[:2] + weights[2:4] + [shards[2][:rows]]
    pieces = []
    start = 0
    for size in sizes:
        pieces.append(small[start : start + size])
        start += size
    return shards, pieces


def local(tokens, cotangent, slot_row, lengths, *params):
    devices = lax.axis_size(AXIS)
    row_count, model_width = tokens.shape
    peer_rows = row_count // devices
    ring = devices // 8 if params[0].shape[0] % 8 == 0 and devices % 8 == 0 else None
    (w_qkv, w_out, w_up, w_down, w_proj), vectors = gather_params(params, ring)
    b_qv, b_up, b_out, gain_one, bias_one, b_down, gain_two, bias_two = vectors

    local_row, inside = order_rows(
        slot_row // row_count * peer_rows + slot_row % peer_rows, lengths
    )
    both = jnp.concatenate([tokens, cotangent], axis=1)
    arrived = lax.all_to_all(both, AXIS, split_axis=0, concat_axis=0, tiled=True)
    chosen = local_row[:, None] == jnp.arange(row_count, dtype=jnp.int32)[None, :]
    chosen = chosen.astype(jnp.bfloat16)
    dealt = dot_nn(chosen, arrived[:, :model_width]).astype(jnp.bfloat16)
    dealt_cot = dot_nn(chosen, arrived[:, model_width:]).astype(jnp.bfloat16)
    valid = inside[:, None].astype(jnp.float32)

    bias_all = jnp.concatenate(
        [b_qv[:model_width], jnp.zeros((model_width,), jnp.float32), b_qv[model_width:]]
    )
    qkv = (dot_nn(dealt, w_qkv) + bias_all).astype(jnp.bfloat16)
    context, logs, *units = attend(qkv, lengths, [w_up, w_down] if ring else [], ring)
    if ring:
        w_up, w_down = [unit.reshape(-1, unit.shape[2]) for unit in units]
    hidden_one = dealt.astype(jnp.float32) + dot_nn(context, w_out) + b_out
    normed_one, inverse_one = norm_parts(hidden_one)
    first_low = (normed_one * gain_one + bias_one).astype(jnp.bfloat16)
    active, slope = up_project(first_low, w_up, b_up)
    hidden_two = first_low.astype(jnp.float32) + dot_nn(active, w_down) + b_down
    normed_two, inverse_two = norm_parts(hidden_two)
    second_low = (normed_two * gain_two + bias_two).astype(jnp.bfloat16)
    project = dot_nn(second_low, w_proj)
    inv_norm = lax.rsqrt(jnp.sum(project * project, axis=-1, keepdims=True) + 1e-06)
    embedded = (project * inv_norm * valid).astype(jnp.bfloat16)

    grad_emb = dealt_cot.astype(jnp.float32) * valid
    along = jnp.sum(project * grad_emb, axis=-1, keepdims=True)
    grad_project = (inv_norm * grad_emb - inv_norm * inv_norm * inv_norm * along * project).astype(
        jnp.bfloat16
    )
    grad_w_proj = dot_tn(second_low, grad_project).astype(jnp.bfloat16)
    grad_second = dot_nt(grad_project, w_proj)
    grad_gain_two = jnp.sum(grad_second * normed_two, axis=0)
    grad_bias_two = jnp.sum(grad_second, axis=0)
    grad_hidden_two = norm_back(grad_second, normed_two, inverse_two, gain_two)
    grad_b_down = jnp.sum(grad_hidden_two, axis=0)
    down_low = grad_hidden_two.astype(jnp.bfloat16)
    grad_w_down = dot_tn(active, down_low).astype(jnp.bfloat16)
    grad_up = dot_nt(down_low, w_down) * slope.astype(jnp.float32)
    grad_b_up = jnp.sum(grad_up, axis=0)
    up_low = grad_up.astype(jnp.bfloat16)
    grad_w_up = dot_tn(first_low, up_low).astype(jnp.bfloat16)
    grad_first = grad_hidden_two + dot_nt(up_low, w_up)
    grad_gain_one = jnp.sum(grad_first * normed_one, axis=0)
    grad_bias_one = jnp.sum(grad_first, axis=0)
    grad_hidden_one = norm_back(grad_first, normed_one, inverse_one, gain_one)
    grad_b_out = jnp.sum(grad_hidden_one, axis=0)
    out_low = grad_hidden_one.astype(jnp.bfloat16)
    grad_w_out = dot_tn(context, out_low).astype(jnp.bfloat16)
    grad_context = dot_nt(out_low, w_out).astype(jnp.bfloat16)
    large = [grad_w_up, grad_w_down] if ring else []
    grad_three, sums, *large = attend_back(
        qkv, context, logs, grad_context, lengths, large, ring
    )
    if ring:
        grad_w_up, grad_w_down = large
    sums = jnp.sum(sums, axis=0)[:, 0]
    grad_b_qv = jnp.concatenate([sums[0], sums[2]])
    grad_qkv = jnp.concatenate([grad_three[0], grad_three[1], grad_three[2]], axis=1)
    grad_w_qkv = dot_tn(dealt, grad_qkv).astype(jnp.bfloat16)
    grad_dealt = (dot_nt(grad_qkv, w_qkv) + grad_hidden_one).astype(jnp.bfloat16)

    back = jnp.concatenate([grad_dealt, embedded], axis=1)
    back = dot_tn(chosen, back).astype(jnp.bfloat16)
    returned = lax.all_to_all(back, AXIS, split_axis=0, concat_axis=0, tiled=True)
    shards, small = scatter_grads(
        [grad_w_qkv, grad_w_out, grad_w_up, grad_w_down, grad_w_proj],
        [
            grad_b_qv,
            grad_b_up,
            grad_b_out,
            grad_gain_one,
            grad_bias_one,
            grad_b_down,
            grad_gain_two,
            grad_bias_two,
        ],
        ring,
        devices,
    )
    return (
        returned[:, model_width:],
        returned[:, :model_width],
        shards[0],
        small[0],
        shards[1],
        small[2],
        small[3],
        small[4],
        shards[2],
        small[1],
        shards[3],
        small[5],
        small[6],
        small[7],
        shards[4],
    )


def solution(mesh):
    matrix, vector = P(AXIS, None), P(AXIS)
    params = "mvmvvvmvmvvvm"
    in_kinds = "mmvv" + params
    out_kinds = "mm" + params
    specs = {"m": matrix, "v": vector}

    return jax.shard_map(
        local,
        mesh=mesh,
        in_specs=tuple(specs[kind] for kind in in_kinds),
        out_specs=tuple(specs[kind] for kind in out_kinds),
        check_vma=False,
    )
```
